128 devices in a mesh: gx: 16 (over z_lo, x, core), gy: 8 (over y, z_hi).
Axes of the slice: x: 4, y: 4, z: 4 (z_hi: 2, z_lo: 2; z = z_hi * 2 + z_lo), core: 2. Of those that a mesh axis runs over, the one named last changes fastest.
Arguments:
- pair_in: bfloat16 [1024, 1024, 128], P(('gx', 'gy')), may hold values from -6 to 6
- residue_mask: int32 [1024], P(('gx', 'gy')), may hold values 0 or 1
- norm_start: float32 [128], replicated, may hold values from 0.25 to 1.75
- proj_start: bfloat16 [128, 512], replicated, may hold values from -0.5 to 0.5
- gate_bias_start: float32 [128], replicated, may hold values from -4 to 4
- bias_w_start: bfloat16 [128, 4], replicated, may hold values from -1.5 to 1.5
- out_w_start: bfloat16 [128, 128], replicated, may hold values from -1 to 1
- norm_end: float32 [128], replicated, may hold values from 0.25 to 1.75
- proj_end: bfloat16 [128, 512], replicated, may hold values from -0.5 to 0.5
- gate_bias_end: float32 [128], replicated, may hold values from -4 to 4
- bias_w_end: bfloat16 [128, 4], replicated, may hold values from -1.5 to 1.5
- out_w_end: bfloat16 [128, 128], replicated, may hold values from -1 to 1
- norm_trans: float32 [128], replicated, may hold values from 0.25 to 1.75
- trans_in: bfloat16 [128, 512], replicated, may hold values from -0.5 to 0.5
- trans_bias: float32 [512], replicated, may hold values from -4 to 4
- trans_out: bfloat16 [512, 128], replicated, may hold values from -0.375 to 0.375
Outputs:
- pair_out: bfloat16 [1024, 1024, 128], P(('gx', 'gy'))
The draws below stay inside these ranges and needn't reach their ends.
Inputs may be any that keep to these rules, and one draw needn't show every extreme that they name: residue_mask holds only 0 and 1.
All inputs are finite; a program needn't handle non-finite values.
Results may differ from the reference program's by a relative error of at most 0.02.
Values may be sent and summed in bfloat16 or wider, within the bound.
A program may use at most 192 MiB of HBM per device.

```python
import jax
import jax.numpy as jnp
from jax import lax

C = 128
HEADS = 4
HEAD_DIM = 32
FFN = 512
RES = 1024


def with_ends(array, key, smallest, top_value):
    place = [jax.random.randint(jax.random.fold_in(key, axis), (), 0, length) for axis, length in enumerate(array.shape)]
    longest = array.shape.index(max(array.shape))
    next_to = place[:longest] + [(place[longest] + 1) % array.shape[longest]] + place[longest + 1:]
    return array.at[tuple(place)].set(smallest).at[tuple(next_to)].set(top_value)


def block_scale(own_key, shape, split, least, high):
    loudness = 1.0
    for position, shards_of in split:
        steps = jax.random.uniform(jax.random.fold_in(jax.random.fold_in(own_key, 6), position), (shards_of,), jnp.float32, least / len(split), high / len(split))
        loudness = loudness * jnp.repeat(jnp.exp(steps), shape[position] // shards_of).reshape((-1,) + (1,) * (len(shape) - 1 - position))
    return loudness


def scatter_about(own_key, extent, deviation, bound, pieces=(), held_as=jnp.bfloat16):
    values = jax.random.normal(own_key, extent, jnp.float32) * deviation
    if len(pieces) > 0:
        values = block_scale(own_key, extent, pieces, -0.22, 0.18) * values
    return jnp.clip(values, min=-bound, max=bound).astype(held_as)


def setup_inputs(seed: int = 0) -> dict:
    streams_of = jax.random.split(jax.random.key(seed), 17)
    return {
        "pair_in": scatter_about(streams_of[0], (RES, RES, C), 1.0, 6.0, ((0, 128),)),
        "residue_mask": with_ends((jax.random.randint(streams_of[1], (RES,), 0, 8) < 7).astype(jnp.int32), jax.random.fold_in(streams_of[1], 1), 0, 1),
        "norm_start": jnp.clip(1.0 + 0.15 * jax.random.normal(streams_of[2], (C,), jnp.float32), 0.25, 1.75),
        "proj_start": scatter_about(streams_of[3], (C, 4 * C), C ** -0.5, 0.5),
        "gate_bias_start": scatter_about(streams_of[4], (C,), 1.0, 4.0, (), jnp.float32),
        "bias_w_start": scatter_about(streams_of[5], (C, HEADS), (C // 8) ** -0.5, 1.5),
        "out_w_start": scatter_about(streams_of[6], (C, C), (C // 4) ** -0.5, 1.0),
        "norm_end": jnp.clip(1.0 + 0.15 * jax.random.normal(streams_of[7], (C,), jnp.float32), 0.25, 1.75),
        "proj_end": scatter_about(streams_of[8], (C, 4 * C), C ** -0.5, 0.5),
        "gate_bias_end": scatter_about(streams_of[9], (C,), 1.0, 4.0, (), jnp.float32),
        "bias_w_end": scatter_about(streams_of[10], (C, HEADS), (C // 8) ** -0.5, 1.5),
        "out_w_end": scatter_about(streams_of[11], (C, C), (C // 4) ** -0.5, 1.0),
        "norm_trans": jnp.clip(1.0 + 0.15 * jax.random.normal(streams_of[12], (C,), jnp.float32), 0.25, 1.75),
        "trans_in": scatter_about(streams_of[13], (C, FFN), C ** -0.5, 0.5),
        "trans_bias": scatter_about(streams_of[14], (FFN,), 1.0, 4.0, (), jnp.float32),
        "trans_out": scatter_about(streams_of[15], (FFN, C), (FFN // 2) ** -0.5, 0.375),
    }


big_negative = 1000000000.0

def layer_norm(values, norm_gain):
    widened = values.astype(jnp.float32)
    row_mean = lax.optimization_barrier(jnp.mean(widened, axis=-1, keepdims=True))
    row_var = lax.optimization_barrier(jnp.mean(jnp.square(widened - row_mean), axis=-1, keepdims=True))
    return ((widened - row_mean) * lax.rsqrt(row_var + 1e-05) * norm_gain).astype(jnp.bfloat16)

def project(normed, weight):
    flat = normed.reshape(-1, normed.shape[-1])
    result = jnp.dot(flat, weight, preferred_element_type=jnp.float32)
    return result.reshape(normed.shape[:-1] + (weight.shape[1],))

def split_heads(merged):
    return merged.astype(jnp.bfloat16).reshape(merged.shape[:-1] + (HEADS, HEAD_DIM))

def attend_block(query, keys, values, pair_bias, key_bias):
    score_scale = HEAD_DIM ** (-0.5)
    scores = jnp.einsum('jhd,khd->hjk', query.astype(jnp.float32), keys.astype(jnp.float32), precision=lax.Precision.HIGHEST)
    scores = scores * score_scale + pair_bias + key_bias
    attn_weights = jax.nn.softmax(scores, axis=-1)
    mixed = jnp.einsum('hjk,khd->jhd', attn_weights, values.astype(jnp.float32), precision=lax.Precision.HIGHEST)
    return mixed.reshape(query.shape[0], HEADS * HEAD_DIM)

def gated_residual(residual, mixed, gate_logit, gate_bias, out_weight):
    gated = (mixed * jax.nn.sigmoid(gate_logit + gate_bias)).astype(jnp.bfloat16)
    return (residual.astype(jnp.float32) + project(gated, out_weight)).astype(jnp.bfloat16)

def projections(normed, weight, channels):
    projected = project(normed, weight)
    query = split_heads(projected[..., :channels])
    keys = split_heads(projected[..., channels:2 * channels])
    values = split_heads(projected[..., 2 * channels:3 * channels])
    return (query, keys, values, projected[..., 3 * channels:])

def reference(pair_in, residue_mask, norm_start, proj_start, gate_bias_start, bias_w_start, out_w_start, norm_end, proj_end, gate_bias_end, bias_w_end, out_w_end, norm_trans, trans_in, trans_bias, trans_out):
    channels = pair_in.shape[-1]
    key_bias = (residue_mask.astype(jnp.float32) - 1.0) * big_negative
    normed = layer_norm(pair_in, norm_start)
    query, keys, values, gate_logit = projections(normed, proj_start, channels)
    pair_bias = project(normed, bias_w_start).astype(jnp.bfloat16)
    start_bias = jnp.transpose(pair_bias, (2, 0, 1)).astype(jnp.float32)

    def per_row(operands):
        query_row, key_row, value_row = operands
        return attend_block(query_row, key_row, value_row, start_bias, key_bias)
    mixed = lax.map(per_row, (query, keys, values))
    after_start = gated_residual(pair_in, mixed, gate_logit, gate_bias_start, out_w_start)
    normed = layer_norm(after_start, norm_end)
    query, keys, values, gate_logit = projections(normed, proj_end, channels)
    pair_bias = project(normed, bias_w_end).astype(jnp.bfloat16)
    end_bias = jnp.transpose(pair_bias, (2, 1, 0)).astype(jnp.float32)

    def per_column(operands):
        query_col, key_col, value_col = operands
        return attend_block(query_col, key_col, value_col, end_bias, key_bias)
    mixed = lax.map(per_column, (jnp.swapaxes(query, 0, 1), jnp.swapaxes(keys, 0, 1), jnp.swapaxes(values, 0, 1)))
    mixed = jnp.swapaxes(mixed, 0, 1)
    after_end = gated_residual(after_start, mixed, gate_logit, gate_bias_end, out_w_end)
    normed = layer_norm(after_end, norm_trans)
    hidden = jax.nn.relu(project(normed, trans_in) + trans_bias).astype(jnp.bfloat16)
    return (after_end.astype(jnp.float32) + project(hidden, trans_out)).astype(jnp.bfloat16)
```

```python
import functools

import jax
import jax.numpy as jnp
from jax import lax
from jax.experimental import pallas as pl
from jax.experimental.pallas import tpu as pltpu
from jax.sharding import PartitionSpec as P

HEADS = 4
HEAD_DIM = 32
LOG2E = 1.4426950408889634
JB = 256
KB = 128
F32 = jnp.float32
BF16 = jnp.bfloat16
NT = (((1,), (1,)), ((), ()))
TN = (((0,), (0,)), ((), ()))
VMEM = pl.BlockSpec(memory_space=pltpu.VMEM)


def layer_norm(t, gain):
    mean = jnp.mean(t, axis=-1, keepdims=True)
    cent = t - mean
    var = jnp.mean(cent * cent, axis=-1, keepdims=True)
    return (cent * lax.rsqrt(var + 1e-05) * gain).astype(BF16)


def bias_kernel(x_ref, g_ref, bw_ref, o_ref):
    bwt = bw_ref[...].astype(F32).T.astype(BF16)
    gain = g_ref[...]
    for r in range(x_ref.shape[0]):
        a = layer_norm(x_ref[r].astype(F32), gain)
        b = lax.dot_general(bwt, a, NT, preferred_element_type=F32) * LOG2E
        o_ref[:, r, :] = b[:HEADS].astype(BF16)


def pair_bias(x, gain, bias_w):
    rows, res, chan = x.shape
    bw = jnp.pad(bias_w, ((0, 0), (0, 128 - HEADS)))
    return pl.pallas_call(
        bias_kernel,
        out_shape=jax.ShapeDtypeStruct((HEADS, rows, res), BF16),
        in_specs=[VMEM] * 3,
        out_specs=VMEM,
    )(x, gain, bw)


def attn_kernel(trans, *refs):
    (x_ref, g_ref, w_ref, gb_ref, ow_ref, mrow_ref, mcol_ref, b_ref), refs = refs[:8], refs[8:]
    if trans:
        (ng_ref, ti_ref, tb_ref, to_ref), refs = refs[:4], refs[4:]
    o_ref, km, qs, vx, gt, bt, pp, ot, wk, wq, ss = refs
    rows, res, chan = x_ref.shape
    jb = pl.program_id(0)
    groups = rows // 4
    nk = res // KB

    @pl.when(jb == 0)
    def _():
        w = w_ref[...].astype(F32)
        wqt = w[:, :chan].T
        for s in range(4):
            cut = chan - 32 * s
            wk[s] = (pltpu.roll(w[:, chan : 2 * chan], 32 * s, 1) if s else w[:, chan : 2 * chan]).astype(BF16)
            wq[s] = (jnp.concatenate([wqt[cut:], wqt[:cut]], axis=0) if s else wqt).astype(BF16)
        wvt = w[:, 2 * chan : 3 * chan].T.astype(BF16)
        wgt = w[:, 3 * chan :].T.astype(BF16)
        gain = g_ref[...]
        gb = gb_ref[...].T
        mrow = mrow_ref[...]
        lane = lax.broadcasted_iota(jnp.int32, (res, chan), 1) // HEAD_DIM

        def project(r, carry):
            s = lax.rem(r, 4)
            grp = r // 4
            a = layer_norm(x_ref[r].astype(F32), gain)
            kk = jnp.dot(a, wk[s], preferred_element_type=F32)
            qt = (
                lax.dot_general(wq[s], a, NT, preferred_element_type=F32)
                * (HEAD_DIM**-0.5 * LOG2E)
            ).astype(BF16)
            vt = lax.dot_general(wvt, a, NT, preferred_element_type=F32) * mrow
            gt[r] = jax.nn.sigmoid(lax.dot_general(wgt, a, NT, preferred_element_type=F32) + gb)
            for h in range(HEADS):
                slot = lax.rem(h + s, 4)
                km[r, h] = jnp.where(lane == slot, kk, 0.0).astype(BF16)
                vx[r, h, :HEAD_DIM] = vt[HEAD_DIM * h : HEAD_DIM * (h + 1)].astype(BF16)
                vx[r, h, HEAD_DIM:] = jnp.broadcast_to(mrow, (16, res)).astype(BF16)
            for t in range(4):
                hh = lax.rem(t - s + 4, 4)
                qs[grp, hh, pl.ds(32 * t, 32)] = qt[32 * t : 32 * (t + 1)]
            return carry

        lax.fori_loop(0, rows, project, 0)

    for h in range(HEADS):
        for kb in range(nk):
            sl = slice(KB * kb, KB * (kb + 1))
            bt[h, sl] = b_ref[h, :, sl].T

    eye = (
        lax.broadcasted_iota(jnp.int32, (KB, KB), 0) == lax.broadcasted_iota(jnp.int32, (KB, KB), 1)
    ).astype(F32).astype(BF16)
    joff = pl.multiple_of(jb * JB, JB)

    def head_body(it, carry):
        grp = it // HEADS
        h = lax.rem(it, HEADS)
        q = qs[grp, h, :, pl.ds(joff, JB)]
        for kb in range(nk):
            sl = slice(KB * kb, KB * (kb + 1))
            rhs = jnp.concatenate([bt[h, sl], q], axis=0)
            lhs = jnp.concatenate(
                [jnp.concatenate([eye, km[grp * 4 + r, h, sl]], axis=1) for r in range(4)], axis=0
            )
            s4 = jnp.dot(lhs, rhs, preferred_element_type=F32)
            p4 = jnp.exp2(s4).astype(BF16)
            for r in range(4):
                pp[r, sl] = p4[KB * r : KB * (r + 1)]
        good = None
        for r in range(4):
            oe = jnp.dot(vx[grp * 4 + r, h], pp[r], preferred_element_type=F32)
            den = oe[HEAD_DIM : HEAD_DIM + 1]
            fine = (den > 2.0**-60) & (den < 2.0**100)
            good = fine if good is None else good & fine
            ot[grp * 4 + r, pl.ds(pl.multiple_of(HEAD_DIM * h, HEAD_DIM), HEAD_DIM)] = (
                oe[:HEAD_DIM] / den
            )

        @pl.when(jnp.min(good.astype(F32)) < 0.5)
        def _():
            def slow_row(r, carry):
                row = grp * 4 + r

                def scores(kb, carry):
                    ks = pl.ds(pl.multiple_of(kb * KB, KB), KB)
                    rhs = jnp.concatenate([bt[h, ks], q], axis=0)
                    lhs = jnp.concatenate([eye, km[row, h, ks]], axis=1)
                    s1 = jnp.dot(lhs, rhs, preferred_element_type=F32)
                    s1 = jnp.where(mcol_ref[ks] > 0.5, s1, -1e30)
                    ss[ks] = s1
                    return jnp.maximum(carry, jnp.max(s1, axis=0, keepdims=True))

                top = lax.fori_loop(0, nk, scores, jnp.full((1, JB), -1e30, F32))

                def weights(kb, carry):
                    ks = pl.ds(pl.multiple_of(kb * KB, KB), KB)
                    pp[0, ks] = jnp.exp2(ss[ks] - top).astype(BF16)
                    return carry

                lax.fori_loop(0, nk, weights, 0)
                oe = jnp.dot(vx[row, h], pp[0], preferred_element_type=F32)
                ot[row, pl.ds(pl.multiple_of(HEAD_DIM * h, HEAD_DIM), HEAD_DIM)] = (
                    oe[:HEAD_DIM] / oe[HEAD_DIM : HEAD_DIM + 1]
                )
                return carry

            lax.fori_loop(0, 4, slow_row, 0)

        return carry

    lax.fori_loop(0, groups * HEADS, head_body, 0)

    def finish(r, carry):
        gated = (ot[r] * gt[r, :, pl.ds(joff, JB)]).T.astype(BF16)
        z = x_ref[r, pl.ds(joff, JB)].astype(F32) + jnp.dot(
            gated, ow_ref[...], preferred_element_type=F32
        )
        z = z.astype(BF16)
        if trans:
            zf = z.astype(F32)
            a = layer_norm(zf, ng_ref[...])
            hid = jnp.dot(a, ti_ref[...], preferred_element_type=F32) + tb_ref[...]
            hid = jnp.maximum(hid, 0.0).astype(BF16)
            z = (zf + jnp.dot(hid, to_ref[...], preferred_element_type=F32)).astype(BF16)
        o_ref[r] = z
        return carry

    lax.fori_loop(0, rows, finish, 0)


def attention(x, gain, proj, gate_bias, out_w, mrow, mcol, bias, trans=()):
    rows, res, chan = x.shape
    full = lambda a: pl.BlockSpec(a.shape, lambda j, n=a.ndim: (0,) * n)
    ins = [x, gain, proj, gate_bias, out_w, mrow, mcol]
    specs = [full(a) for a in ins] + [pl.BlockSpec((HEADS, JB, res), lambda j: (0, j, 0))]
    ins.append(bias)
    ins += trans
    specs += [full(a) for a in trans]
    return pl.pallas_call(
        functools.partial(attn_kernel, bool(trans)),
        grid=(res // JB,),
        out_shape=jax.ShapeDtypeStruct((rows, res, chan), BF16),
        in_specs=specs,
        out_specs=pl.BlockSpec((rows, JB, chan), lambda j: (0, j, 0)),
        scratch_shapes=[
            pltpu.VMEM((rows, HEADS, res, chan), BF16),
            pltpu.VMEM((rows // 4, HEADS, chan, res), BF16),
            pltpu.VMEM((rows, HEADS, HEAD_DIM + 16, res), BF16),
            pltpu.VMEM((rows, chan, res), F32),
            pltpu.VMEM((HEADS, res, JB), BF16),
            pltpu.VMEM((4, res, JB), BF16),
            pltpu.VMEM((rows, chan, JB), F32),
            pltpu.VMEM((4, chan, chan), BF16),
            pltpu.VMEM((4, chan, chan), BF16),
            pltpu.VMEM((res, JB), F32),
        ],
        compiler_params=pltpu.CompilerParams(
            dimension_semantics=("arbitrary",), vmem_limit_bytes=60 * 1024 * 1024
        ),
    )(*ins)


def local(
    pair_in,
    residue_mask,
    norm_start,
    proj_start,
    gate_bias_start,
    bias_w_start,
    out_w_start,
    norm_end,
    proj_end,
    gate_bias_end,
    bias_w_end,
    out_w_end,
    norm_trans,
    trans_in,
    trans_bias,
    trans_out,
):
    rows, res, chan = pair_in.shape
    axes = ("gx", "gy")
    row = lambda v: v.reshape(1, -1)
    mask = lax.all_gather(residue_mask, axes, axis=0, tiled=True).astype(F32)
    mask = jnp.where(jnp.max(mask) > 0.5, mask, 1.0)
    mrow, mcol = mask.reshape(1, res), mask.reshape(res, 1)

    bias = pair_bias(pair_in, row(norm_start), bias_w_start)
    bias = lax.all_gather(bias, axes, axis=1, tiled=True)
    z1 = attention(
        pair_in, row(norm_start), proj_start, row(gate_bias_start), out_w_start, mrow, mcol, bias
    )
    cols = lax.all_to_all(z1, axes, split_axis=1, concat_axis=0, tiled=True)
    cols = jnp.swapaxes(cols, 0, 1)
    bias = pair_bias(cols, row(norm_end), bias_w_end)
    bias = lax.all_gather(bias, axes, axis=1, tiled=True)
    out = attention(
        cols, row(norm_end), proj_end, row(gate_bias_end), out_w_end, mrow, mcol, bias,
        (row(norm_trans), trans_in, row(trans_bias), trans_out),
    )
    out = lax.all_to_all(jnp.swapaxes(out, 0, 1), axes, split_axis=0, concat_axis=1, tiled=True)
    return out


def solution(mesh):
    spec = P(("gx", "gy"), None, None)
    placed = (spec, P(("gx", "gy"))) + (P(),) * 14
    return jax.shard_map(local, mesh=mesh, in_specs=placed, out_specs=spec, check_vma=False)
```

```python
import functools

import jax
import jax.numpy as jnp
from jax import lax
from jax.experimental import pallas as pl
from jax.experimental.pallas import tpu as pltpu
from jax.sharding import PartitionSpec as P

HEADS = 4
HEAD_DIM = 32
LOG2E = 1.4426950408889634
JB = 256
KB = 128
F32 = jnp.float32
BF16 = jnp.bfloat16
NT = (((1,), (1,)), ((), ()))
TN = (((0,), (0,)), ((), ()))
VMEM = pl.BlockSpec(memory_space=pltpu.VMEM)


def layer_norm(t, gain):
    mean = jnp.mean(t, axis=-1, keepdims=True)
    cent = t - mean
    var = jnp.mean(cent * cent, axis=-1, keepdims=True)
    return (cent * lax.rsqrt(var + 1e-05) * gain).astype(BF16)


def bias_kernel(x_ref, g_ref, bw_ref, o_ref):
    bwt = bw_ref[...].astype(F32).T.astype(BF16)
    gain = g_ref[...]
    for r in range(x_ref.shape[0]):
        a = layer_norm(x_ref[r].astype(F32), gain)
        b = lax.dot_general(bwt, a, NT, preferred_element_type=F32) * LOG2E
        o_ref[:, r, :] = b[:HEADS].astype(BF16)


def pair_bias(x, gain, bias_w):
    rows, res, chan = x.shape
    bw = jnp.pad(bias_w, ((0, 0), (0, 128 - HEADS)))
    return pl.pallas_call(
        bias_kernel,
        out_shape=jax.ShapeDtypeStruct((HEADS, rows, res), BF16),
        in_specs=[VMEM] * 3,
        out_specs=VMEM,
    )(x, gain, bw)


ORDERS = (
    ("xyz", "yzx", "zxy", "xyz", "yzx"),
    ("yzx", "zxy", "xyz", "yzx", "xyz"),
)


def place():
    gx, gy = lax.axis_index("gx"), lax.axis_index("gy")
    return {
        "x": lax.rem(gx // 2, 4),
        "y": gy // 2,
        "z": 2 * lax.rem(gy, 2) + gx // 8,
        "c": lax.rem(gx, 2),
    }


def device(at):
    z_lo, z_hi = lax.rem(at["z"], 2), at["z"] // 2
    return {"gx": (z_lo * 4 + at["x"]) * 2 + at["c"], "gy": at["y"] * 2 + z_hi}


def shift(at, dim, by):
    return {**at, dim: lax.rem(at[dim] + by + 4, 4)}


def part(ref, lead, at, free, tail=()):
    z = "z" in free
    pick = lambda d: slice(None) if d in free else at[d]
    z_lo = slice(None) if z else lax.rem(at["z"], 2)
    z_hi = slice(None) if z else at["z"] // 2
    return ref.at[lead + (z_lo, pick("x"), at["c"], pick("y"), z_hi) + tail]


def gather_kernel(n_out, *refs):
    ins, outs = refs[:n_out], refs[n_out : 2 * n_out]
    ring_send, ring_recv, pair_send, pair_recv, own_sem = refs[2 * n_out :]
    me = place()
    barrier = pltpu.get_barrier_semaphore()
    sib = {**me, "c": 1 - me["c"]}
    partners = [shift(me, d, by) for d in "xyz" for by in (1, -1)] + [sib]
    for at in partners:
        pl.semaphore_signal(barrier, inc=1, device_id=device(at), device_id_type=pl.DeviceIdType.MESH)
    pl.semaphore_wait(barrier, len(partners))

    def items(core):
        half = outs[0].shape[-1] // 2
        got = []
        for h in range(HEADS):
            got.append((h, ins[0].at[h], functools.partial(part, outs[0], (h,)), half))
        if n_out == 2:
            got.append((HEADS, ins[1], functools.partial(part, outs[1], ()), 0))
        return got

    def copy(src, dst, sems, idx, to):
        return pltpu.make_async_remote_copy(
            src_ref=src, dst_ref=dst, send_sem=sems[0].at[idx], recv_sem=sems[1].at[idx],
            device_id=device(to), device_id_type=pl.DeviceIdType.MESH,
        )

    ring, pair = (ring_send, ring_recv), (pair_send, pair_recv)

    def run(core):
        at = {**me, "c": core}
        other = {**me, "c": 1 - core}
        todo = items(core)
        sends = []

        def step0(p, idx, own, sets, half):
            d, free = ORDERS[core][idx][p], ORDERS[core][idx][:p]
            src = sets(at, free)
            for k, by in enumerate((1, -1)):
                c = copy(own if p == 0 else src, src, ring, (idx, p, k), shift(at, d, by))
                c.start()
                sends.append(c)

        def step1(p, idx, own, sets, half):
            d, free = ORDERS[core][idx][p], ORDERS[core][idx][:p]
            for k, by in enumerate((1, -1)):
                got = sets(shift(at, d, -by), free)
                copy(got, got, ring, (idx, p, k), shift(at, d, by)).wait_recv()
                if half:
                    tail = (slice(None), pl.ds(k * half, half))
                    piece = sets(shift(at, d, -by), free, tail)
                elif k == 0:
                    piece = got
                else:
                    continue
                c = copy(piece, piece, ring, (idx, p, 2 + k), shift(at, d, by))
                c.start()
                sends.append(c)

        def step2(p, idx, own, sets, half):
            d, free = ORDERS[core][idx][p], ORDERS[core][idx][:p]
            for k, by in enumerate((1, -1)):
                if half:
                    tail = (slice(None), pl.ds(k * half, half))
                    piece = sets(shift(at, d, 2), free, tail)
                elif k == 0:
                    piece = sets(shift(at, d, 2), free)
                else:
                    continue
                copy(piece, piece, ring, (idx, p, 2 + k), shift(at, d, by)).wait_recv()

        def across(idx, sets, hop):
            d, free = ORDERS[core][idx][2], ORDERS[core][idx][:2]
            piece = sets(shift(at, d, hop), free)
            c = copy(piece, piece, pair, (idx, hop), other)
            c.start()
            sends.append(c)

        own_copies = []
        for idx, own, sets, half in todo:
            step0(0, idx, own, sets, half)
            mine = pltpu.make_async_copy(own, sets(at, ""), own_sem.at[idx])
            mine.start()
            own_copies.append(mine)
        for p in range(3):
            for t in todo:
                step1(p, *t)
                if p == 2:
                    for hop in (1, 3):
                        across(t[0], t[2], hop)
            for i, t in enumerate(todo):
                if p == 0:
                    own_copies[i].wait()
                step2(p, *t)
                if p < 2:
                    step0(p + 1, *t)
                if p == 1:
                    across(t[0], t[2], 0)
                if p == 2:
                    across(t[0], t[2], 2)
        for idx, own, sets, half in todo:
            d, free = ORDERS[1 - core][idx][2], ORDERS[1 - core][idx][:2]
            for hop in range(4):
                piece = sets(shift(other, d, hop), free)
                copy(piece, piece, pair, (idx, hop), other).wait_recv()
        for c in sends:
            c.wait_send()

    for core in range(2):
        pl.when(me["c"] == core)(functools.partial(run, core))


def gather(cid, bias, *mask):
    heads, rows, res = bias.shape
    grid = (2, 4, 2, 4, 2)
    outs = [jax.ShapeDtypeStruct((heads,) + grid + (rows, res), BF16)]
    if mask:
        outs.append(jax.ShapeDtypeStruct(grid + mask[0].shape, F32))
    n = len(outs)
    got = pl.pallas_call(
        functools.partial(gather_kernel, n),
        out_shape=outs,
        in_specs=[VMEM] * n,
        out_specs=[pl.BlockSpec(memory_space=pl.ANY)] * n,
        scratch_shapes=[
            pltpu.SemaphoreType.DMA((5, 3, 4)),
            pltpu.SemaphoreType.DMA((5, 3, 4)),
            pltpu.SemaphoreType.DMA((5, 4)),
            pltpu.SemaphoreType.DMA((5, 4)),
            pltpu.SemaphoreType.DMA((5,)),
        ],
        compiler_params=pltpu.CompilerParams(collective_id=cid, has_side_effects=True),
    )(bias, *mask)
    full = got[0].reshape(heads, -1, res)
    return (full, got[1].reshape((-1,) + mask[0].shape)) if mask else full


def attn_kernel(trans, *refs):
    (x_ref, g_ref, w_ref, gb_ref, ow_ref, mrow_ref, mcol_ref, b_ref), refs = refs[:8], refs[8:]
    if trans:
        (ng_ref, ti_ref, tb_ref, to_ref), refs = refs[:4], refs[4:]
    o_ref, km, qs, vx, gt, bt, pp, ot, wk, wq, ss = refs
    rows, res, chan = x_ref.shape
    jb = pl.program_id(0)
    groups = rows // 4
    nk = res // KB

    @pl.when(jb == 0)
    def _():
        w = w_ref[...].astype(F32)
        wqt = w[:, :chan].T
        for s in range(4):
            cut = chan - 32 * s
            wk[s] = (pltpu.roll(w[:, chan : 2 * chan], 32 * s, 1) if s else w[:, chan : 2 * chan]).astype(BF16)
            wq[s] = (jnp.concatenate([wqt[cut:], wqt[:cut]], axis=0) if s else wqt).astype(BF16)
        wvt = w[:, 2 * chan : 3 * chan].T.astype(BF16)
        wgt = w[:, 3 * chan :].T.astype(BF16)
        gain = g_ref[...]
        gb = gb_ref[...].T
        mrow = mrow_ref[...]
        lane = lax.broadcasted_iota(jnp.int32, (res, chan), 1) // HEAD_DIM

        def project(r, carry):
            s = lax.rem(r, 4)
            grp = r // 4
            a = layer_norm(x_ref[r].astype(F32), gain)
            kk = jnp.dot(a, wk[s], preferred_element_type=F32)
            qt = (
                lax.dot_general(wq[s], a, NT, preferred_element_type=F32)
                * (HEAD_DIM**-0.5 * LOG2E)
            ).astype(BF16)
            vt = lax.dot_general(wvt, a, NT, preferred_element_type=F32) * mrow
            gt[r] = jax.nn.sigmoid(lax.dot_general(wgt, a, NT, preferred_element_type=F32) + gb)
            for h in range(HEADS):
                slot = lax.rem(h + s, 4)
                km[r, h] = jnp.where(lane == slot, kk, 0.0).astype(BF16)
                vx[r, h, :HEAD_DIM] = vt[HEAD_DIM * h : HEAD_DIM * (h + 1)].astype(BF16)
                vx[r, h, HEAD_DIM:] = jnp.broadcast_to(mrow, (16, res)).astype(BF16)
            for t in range(4):
                hh = lax.rem(t - s + 4, 4)
                qs[grp, hh, pl.ds(32 * t, 32)] = qt[32 * t : 32 * (t + 1)]
            return carry

        lax.fori_loop(0, rows, project, 0)

    for h in range(HEADS):
        for kb in range(nk):
            sl = slice(KB * kb, KB * (kb + 1))
            bt[h, sl] = b_ref[h, :, sl].T

    eye = (
        lax.broadcasted_iota(jnp.int32, (KB, KB), 0) == lax.broadcasted_iota(jnp.int32, (KB, KB), 1)
    ).astype(F32).astype(BF16)
    joff = pl.multiple_of(jb * JB, JB)

    def head_body(it, carry):
        grp = it // HEADS
        h = lax.rem(it, HEADS)
        q = qs[grp, h, :, pl.ds(joff, JB)]
        for kb in range(nk):
            sl = slice(KB * kb, KB * (kb + 1))
            rhs = jnp.concatenate([bt[h, sl], q], axis=0)
            lhs = jnp.concatenate(
                [jnp.concatenate([eye, km[grp * 4 + r, h, sl]], axis=1) for r in range(4)], axis=0
            )
            s4 = jnp.dot(lhs, rhs, preferred_element_type=F32)
            p4 = jnp.exp2(s4).astype(BF16)
            for r in range(4):
                pp[r, sl] = p4[KB * r : KB * (r + 1)]
        good = None
        for r in range(4):
            oe = jnp.dot(vx[grp * 4 + r, h], pp[r], preferred_element_type=F32)
            den = oe[HEAD_DIM : HEAD_DIM + 1]
            fine = (den > 2.0**-60) & (den < 2.0**100)
            good = fine if good is None else good & fine
            ot[grp * 4 + r, pl.ds(pl.multiple_of(HEAD_DIM * h, HEAD_DIM), HEAD_DIM)] = (
                oe[:HEAD_DIM] / den
            )

        @pl.when(jnp.min(good.astype(F32)) < 0.5)
        def _():
            def slow_row(r, carry):
                row = grp * 4 + r

                def scores(kb, carry):
                    ks = pl.ds(pl.multiple_of(kb * KB, KB), KB)
                    rhs = jnp.concatenate([bt[h, ks], q], axis=0)
                    lhs = jnp.concatenate([eye, km[row, h, ks]], axis=1)
                    s1 = jnp.dot(lhs, rhs, preferred_element_type=F32)
                    s1 = jnp.where(mcol_ref[ks] > 0.5, s1, -1e30)
                    ss[ks] = s1
                    return jnp.maximum(carry, jnp.max(s1, axis=0, keepdims=True))

                top = lax.fori_loop(0, nk, scores, jnp.full((1, JB), -1e30, F32))

                def weights(kb, carry):
                    ks = pl.ds(pl.multiple_of(kb * KB, KB), KB)
                    pp[0, ks] = jnp.exp2(ss[ks] - top).astype(BF16)
                    return carry

                lax.fori_loop(0, nk, weights, 0)
                oe = jnp.dot(vx[row, h], pp[0], preferred_element_type=F32)
                ot[row, pl.ds(pl.multiple_of(HEAD_DIM * h, HEAD_DIM), HEAD_DIM)] = (
                    oe[:HEAD_DIM] / oe[HEAD_DIM : HEAD_DIM + 1]
                )
                return carry

            lax.fori_loop(0, 4, slow_row, 0)

        return carry

    lax.fori_loop(0, groups * HEADS, head_body, 0)

    def finish(r, carry):
        gated = (ot[r] * gt[r, :, pl.ds(joff, JB)]).T.astype(BF16)
        z = x_ref[r, pl.ds(joff, JB)].astype(F32) + jnp.dot(
            gated, ow_ref[...], preferred_element_type=F32
        )
        z = z.astype(BF16)
        if trans:
            zf = z.astype(F32)
            a = layer_norm(zf, ng_ref[...])
            hid = jnp.dot(a, ti_ref[...], preferred_element_type=F32) + tb_ref[...]
            hid = jnp.maximum(hid, 0.0).astype(BF16)
            z = (zf + jnp.dot(hid, to_ref[...], preferred_element_type=F32)).astype(BF16)
        o_ref[r] = z
        return carry

    lax.fori_loop(0, rows, finish, 0)


def attention(x, gain, proj, gate_bias, out_w, mrow, mcol, bias, trans=()):
    rows, res, chan = x.shape
    full = lambda a: pl.BlockSpec(a.shape, lambda j, n=a.ndim: (0,) * n)
    ins = [x, gain, proj, gate_bias, out_w, mrow, mcol]
    specs = [full(a) for a in ins] + [pl.BlockSpec((HEADS, JB, res), lambda j: (0, j, 0))]
    ins.append(bias)
    ins += trans
    specs += [full(a) for a in trans]
    return pl.pallas_call(
        functools.partial(attn_kernel, bool(trans)),
        grid=(res // JB,),
        out_shape=jax.ShapeDtypeStruct((rows, res, chan), BF16),
        in_specs=specs,
        out_specs=pl.BlockSpec((rows, JB, chan), lambda j: (0, j, 0)),
        scratch_shapes=[
            pltpu.VMEM((rows, HEADS, res, chan), BF16),
            pltpu.VMEM((rows // 4, HEADS, chan, res), BF16),
            pltpu.VMEM((rows, HEADS, HEAD_DIM + 16, res), BF16),
            pltpu.VMEM((rows, chan, res), F32),
            pltpu.VMEM((HEADS, res, JB), BF16),
            pltpu.VMEM((4, res, JB), BF16),
            pltpu.VMEM((rows, chan, JB), F32),
            pltpu.VMEM((4, chan, chan), BF16),
            pltpu.VMEM((4, chan, chan), BF16),
            pltpu.VMEM((res, JB), F32),
        ],
        compiler_params=pltpu.CompilerParams(
            dimension_semantics=("arbitrary",), vmem_limit_bytes=60 * 1024 * 1024
        ),
    )(*ins)


def local(
    pair_in,
    residue_mask,
    norm_start,
    proj_start,
    gate_bias_start,
    bias_w_start,
    out_w_start,
    norm_end,
    proj_end,
    gate_bias_end,
    bias_w_end,
    out_w_end,
    norm_trans,
    trans_in,
    trans_bias,
    trans_out,
):
    rows, res, chan = pair_in.shape
    axes = ("gx", "gy")
    row = lambda v: v.reshape(1, -1)
    mine = jnp.pad(residue_mask.astype(F32).reshape(1, rows), ((0, 7), (0, 128 - rows)))
    bias = pair_bias(pair_in, row(norm_start), bias_w_start)
    bias, mask = gather(0, bias, mine)
    mask = mask[:, 0, :rows].reshape(res)
    mask = jnp.where(jnp.max(mask) > 0.5, mask, 1.0)
    mrow, mcol = mask.reshape(1, res), mask.reshape(res, 1)

    z1 = attention(
        pair_in, row(norm_start), proj_start, row(gate_bias_start), out_w_start, mrow, mcol, bias
    )
    cols = lax.all_to_all(z1, axes, split_axis=1, concat_axis=0, tiled=True)
    cols = jnp.swapaxes(cols, 0, 1)
    bias = pair_bias(cols, row(norm_end), bias_w_end)
    bias = gather(1, bias)
    out = attention(
        cols, row(norm_end), proj_end, row(gate_bias_end), out_w_end, mrow, mcol, bias,
        (row(norm_trans), trans_in, row(trans_bias), trans_out),
    )
    out = lax.all_to_all(jnp.swapaxes(out, 0, 1), axes, split_axis=0, concat_axis=1, tiled=True)
    return out


def solution(mesh):
    spec = P(("gx", "gy"), None, None)
    placed = (spec, P(("gx", "gy"))) + (P(),) * 14
    return jax.shard_map(local, mesh=mesh, in_specs=placed, out_specs=spec, check_vma=False)
```

```python
import functools

import jax
import jax.numpy as jnp
from jax import lax
from jax.experimental import pallas as pl
from jax.experimental.pallas import tpu as pltpu
from jax.sharding import PartitionSpec as P

HEADS = 4
HEAD_DIM = 32
LOG2E = 1.4426950408889634
JB = 256
KB = 128
UNROLL = 4
F32 = jnp.float32
BF16 = jnp.bfloat16
NT = (((1,), (1,)), ((), ()))
TN = (((0,), (0,)), ((), ()))
VMEM = pl.BlockSpec(memory_space=pltpu.VMEM)


def layer_norm(t, gain):
    chan = t.shape[1]
    mean = jnp.dot(t, jnp.full((chan, chan), 1.0 / chan, BF16), preferred_element_type=F32)
    cent = t.astype(F32) - mean
    var = jnp.mean(cent * cent, axis=-1, keepdims=True)
    return (cent * lax.rsqrt(var + 1e-05) * gain).astype(BF16)


def bias_kernel(x_ref, g_ref, bw_ref, o_ref, a_ref):
    bwt = bw_ref[...].astype(F32).T.astype(BF16)
    gain = g_ref[...]
    for r in range(x_ref.shape[0]):
        a = layer_norm(x_ref[r], gain)
        a_ref[r] = a
        b = lax.dot_general(bwt, a, NT, preferred_element_type=F32) * LOG2E
        o_ref[:, r, :] = b[:HEADS].astype(BF16)


def pair_bias(x, gain, bias_w):
    rows, res, chan = x.shape
    bw = jnp.pad(bias_w, ((0, 0), (0, 128 - HEADS)))
    return pl.pallas_call(
        bias_kernel,
        out_shape=[
            jax.ShapeDtypeStruct((HEADS, rows, res), BF16),
            jax.ShapeDtypeStruct(x.shape, BF16),
        ],
        in_specs=[VMEM] * 3,
        out_specs=[VMEM] * 2,
    )(x, gain, bw)


ORDERS = (
    ("xyz", "yzx", "zxy", "xyz", "yzx"),
    ("yzx", "zxy", "xyz", "yzx", "xyz"),
)


def place():
    gx, gy = lax.axis_index("gx"), lax.axis_index("gy")
    return {
        "x": lax.rem(gx // 2, 4),
        "y": gy // 2,
        "z": 2 * lax.rem(gy, 2) + gx // 8,
        "c": lax.rem(gx, 2),
    }


def device(at):
    z_lo, z_hi = lax.rem(at["z"], 2), at["z"] // 2
    return {"gx": (z_lo * 4 + at["x"]) * 2 + at["c"], "gy": at["y"] * 2 + z_hi}


def shift(at, dim, by):
    return {**at, dim: lax.rem(at[dim] + by + 4, 4)}


def part(ref, lead, at, free, tail=()):
    z = "z" in free
    pick = lambda d: slice(None) if d in free else at[d]
    z_lo = slice(None) if z else lax.rem(at["z"], 2)
    z_hi = slice(None) if z else at["z"] // 2
    return ref.at[lead + (z_lo, pick("x"), at["c"], pick("y"), z_hi) + tail]


def gather_kernel(n_out, *refs):
    ins, outs = refs[:n_out], refs[n_out : 2 * n_out]
    ring_send, ring_recv, pair_send, pair_recv, own_sem = refs[2 * n_out :]
    me = place()
    barrier = pltpu.get_barrier_semaphore()
    sib = {**me, "c": 1 - me["c"]}
    partners = [shift(me, d, by) for d in "xyz" for by in (1, -1)] + [sib]
    for at in partners:
        pl.semaphore_signal(barrier, inc=1, device_id=device(at), device_id_type=pl.DeviceIdType.MESH)
    pl.semaphore_wait(barrier, len(partners))

    def items(core):
        half = outs[0].shape[-1] // 2
        got = []
        for h in range(HEADS):
            got.append((h, ins[0].at[h], functools.partial(part, outs[0], (h,)), half))
        if n_out == 2:
            got.append((HEADS, ins[1], functools.partial(part, outs[1], ()), 0))
        return got

    def copy(src, dst, sems, idx, to):
        return pltpu.make_async_remote_copy(
            src_ref=src, dst_ref=dst, send_sem=sems[0].at[idx], recv_sem=sems[1].at[idx],
            device_id=device(to), device_id_type=pl.DeviceIdType.MESH,
        )

    ring, pair = (ring_send, ring_recv), (pair_send, pair_recv)

    def run(core):
        at = {**me, "c": core}
        other = {**me, "c": 1 - core}
        todo = items(core)
        sends = []

        def step0(p, idx, own, sets, half):
            d, free = ORDERS[core][idx][p], ORDERS[core][idx][:p]
            src = sets(at, free)
            for k, by in enumerate((1, -1)):
                c = copy(own if p == 0 else src, src, ring, (idx, p, k), shift(at, d, by))
                c.start()
                sends.append(c)

        def step1(p, idx, own, sets, half):
            d, free = ORDERS[core][idx][p], ORDERS[core][idx][:p]
            for k, by in enumerate((1, -1)):
                got = sets(shift(at, d, -by), free)
                copy(got, got, ring, (idx, p, k), shift(at, d, by)).wait_recv()
                if half:
                    tail = (slice(None), pl.ds(k * half, half))
                    piece = sets(shift(at, d, -by), free, tail)
                elif k == 0:
                    piece = got
                else:
                    continue
                c = copy(piece, piece, ring, (idx, p, 2 + k), shift(at, d, by))
                c.start()
                sends.append(c)

        def step2(p, idx, own, sets, half):
            d, free = ORDERS[core][idx][p], ORDERS[core][idx][:p]
            for k, by in enumerate((1, -1)):
                if half:
                    tail = (slice(None), pl.ds(k * half, half))
                    piece = sets(shift(at, d, 2), free, tail)
                elif k == 0:
                    piece = sets(shift(at, d, 2), free)
                else:
                    continue
                copy(piece, piece, ring, (idx, p, 2 + k), shift(at, d, by)).wait_recv()

        def across(idx, sets, hop):
            d, free = ORDERS[core][idx][2], ORDERS[core][idx][:2]
            piece = sets(shift(at, d, hop), free)
            c = copy(piece, piece, pair, (idx, hop), other)
            c.start()
            sends.append(c)

        own_copies = []
        for idx, own, sets, half in todo:
            step0(0, idx, own, sets, half)
            mine = pltpu.make_async_copy(own, sets(at, ""), own_sem.at[idx])
            mine.start()
            own_copies.append(mine)
        for p in range(3):
            for t in todo:
                step1(p, *t)
                if p == 2:
                    for hop in (1, 3):
                        across(t[0], t[2], hop)
            for i, t in enumerate(todo):
                if p == 0:
                    own_copies[i].wait()
                step2(p, *t)
                if p < 2:
                    step0(p + 1, *t)
                if p == 1:
                    across(t[0], t[2], 0)
                if p == 2:
                    across(t[0], t[2], 2)
        for idx, own, sets, half in todo:
            d, free = ORDERS[1 - core][idx][2], ORDERS[1 - core][idx][:2]
            for hop in range(4):
                piece = sets(shift(other, d, hop), free)
                copy(piece, piece, pair, (idx, hop), other).wait_recv()
        for c in sends:
            c.wait_send()

    for core in range(2):
        pl.when(me["c"] == core)(functools.partial(run, core))


def gather(cid, bias, *mask):
    heads, rows, res = bias.shape
    grid = (2, 4, 2, 4, 2)
    outs = [jax.ShapeDtypeStruct((heads,) + grid + (rows, res), BF16)]
    if mask:
        outs.append(jax.ShapeDtypeStruct(grid + mask[0].shape, F32))
    n = len(outs)
    got = pl.pallas_call(
        functools.partial(gather_kernel, n),
        out_shape=outs,
        in_specs=[VMEM] * n,
        out_specs=[pl.BlockSpec(memory_space=pl.ANY)] * n,
        scratch_shapes=[
            pltpu.SemaphoreType.DMA((5, 3, 4)),
            pltpu.SemaphoreType.DMA((5, 3, 4)),
            pltpu.SemaphoreType.DMA((5, 4)),
            pltpu.SemaphoreType.DMA((5, 4)),
            pltpu.SemaphoreType.DMA((5,)),
        ],
        compiler_params=pltpu.CompilerParams(collective_id=cid, has_side_effects=True),
    )(bias, *mask)
    full = got[0].reshape(heads, -1, res)
    return (full, got[1].reshape((-1,) + mask[0].shape)) if mask else full


def attn_kernel(trans, *refs):
    (x_ref, a_ref, w_ref, gb_ref, ow_ref, mrow_ref, mcol_ref, b_ref), refs = refs[:8], refs[8:]
    if trans:
        (ng_ref, ti_ref, tb_ref, to_ref), refs = refs[:4], refs[4:]
    o_ref, km, qs, vx, gt, bt, pa, pb, ot, wk, wq, ss, gd, zz = refs
    rows, res, chan = x_ref.shape
    jb = pl.program_id(0)
    groups = rows // 4
    nk = res // KB

    @pl.when(jb == 0)
    def _():
        w = w_ref[...].astype(F32)
        wqt = w[:, :chan].T
        for s in range(4):
            cut = chan - 32 * s
            wk[s] = (pltpu.roll(w[:, chan : 2 * chan], 32 * s, 1) if s else w[:, chan : 2 * chan]).astype(BF16)
            wq[s] = (jnp.concatenate([wqt[cut:], wqt[:cut]], axis=0) if s else wqt).astype(BF16)
        wvt = w[:, 2 * chan : 3 * chan].T.astype(BF16)
        wgt = w[:, 3 * chan :].T.astype(BF16)
        gb = gb_ref[...].T
        mrow = mrow_ref[...]
        lane = lax.broadcasted_iota(jnp.int32, (1, chan), 1) // HEAD_DIM

        def project(r, carry):
            s = lax.rem(r, 4)
            grp = r // 4
            a = a_ref[r]
            kk = jnp.dot(a, wk[s], preferred_element_type=F32).astype(BF16)
            qt = (
                lax.dot_general(wq[s], a, NT, preferred_element_type=F32)
                * (HEAD_DIM**-0.5 * LOG2E)
            ).astype(BF16)
            vt = lax.dot_general(wvt, a, NT, preferred_element_type=F32) * mrow
            gt[r] = jax.nn.sigmoid(lax.dot_general(wgt, a, NT, preferred_element_type=F32) + gb)
            for h in range(HEADS):
                slot = lax.rem(h + s, 4)
                km[r, h] = kk * (lane == slot).astype(F32).astype(BF16)
                vx[r, h, :HEAD_DIM] = vt[HEAD_DIM * h : HEAD_DIM * (h + 1)].astype(BF16)
                vx[r, h, HEAD_DIM:] = jnp.broadcast_to(mrow, (16, res)).astype(BF16)
            for t in range(4):
                hh = lax.rem(t - s + 4, 4)
                qs[grp, hh, pl.ds(32 * t, 32)] = qt[32 * t : 32 * (t + 1)]
            return carry

        lax.fori_loop(0, rows, project, 0)

    eye = (
        lax.broadcasted_iota(jnp.int32, (KB, KB), 0) == lax.broadcasted_iota(jnp.int32, (KB, KB), 1)
    ).astype(F32).astype(BF16)
    joff = pl.multiple_of(jb * JB, JB)
    tasks = groups * HEADS

    def of(t):
        return t // HEADS, lax.rem(t, HEADS)

    def head_slice(h):
        return pl.ds(pl.multiple_of(HEAD_DIM * h, HEAD_DIM), HEAD_DIM)

    def weights_step(t, kb, pp):
        grp, h = of(t)
        sl = slice(KB * kb, KB * (kb + 1))
        rhs = jnp.concatenate([bt[h, sl], qs[grp, h, :, pl.ds(joff, JB)]], axis=0)
        lhs = jnp.concatenate(
            [jnp.concatenate([eye, km[grp * 4 + r, h, sl]], axis=1) for r in range(4)], axis=0
        )
        p4 = jnp.exp2(jnp.dot(lhs, rhs, preferred_element_type=F32)).astype(BF16)
        for r in range(4):
            pp[r, sl] = p4[KB * r : KB * (r + 1)]

    def mix_step(t, r, pp):
        grp, h = of(t)
        oe = jnp.dot(vx[grp * 4 + r, h], pp[r], preferred_element_type=F32)
        den = oe[HEAD_DIM : HEAD_DIM + 1]
        gd[...] = jnp.where((den > 2.0**-60) & (den < 2.0**100), gd[...], 0.0)
        ot[grp * 4 + r, head_slice(h)] = oe[:HEAD_DIM] / den

    def finish(r):
        gated = (ot[r] * gt[r, :, pl.ds(joff, JB)]).T.astype(BF16)
        z = x_ref[r, pl.ds(joff, JB)].astype(F32) + jnp.dot(
            gated, ow_ref[...], preferred_element_type=F32
        )
        z = z.astype(BF16)
        if trans:
            zf = z.astype(F32)
            a = layer_norm(z, ng_ref[...])
            hid = jnp.dot(a, ti_ref[...], preferred_element_type=F32) + tb_ref[...]
            hid = jnp.maximum(hid, 0.0).astype(BF16)
            z = (zf + jnp.dot(hid, to_ref[...], preferred_element_type=F32)).astype(BF16)
        zz[r] = z

    def both(t, new, old):
        for kb in range(nk):
            weights_step(t, kb, new)
            if kb % 2:
                mix_step(t - 1, kb // 2, old)

    for h in range(HEADS):
        for kb in range(nk):
            sl = slice(KB * kb, KB * (kb + 1))
            bt[h, sl] = b_ref[h, :, sl].T
    gd[...] = jnp.ones_like(gd)
    for kb in range(nk):
        weights_step(0, kb, pa)

    def pair(i, carry):
        both(2 * i + 1, pb, pa)
        both(2 * i + 2, pa, pb)
        return carry

    lax.fori_loop(0, tasks // 2 - 1, pair, 0)
    both(tasks - 1, pb, pa)
    for r in range(4):
        mix_step(tasks - 1, r, pb)

    @pl.when(jnp.min(gd[...]) < 0.5)
    def _():
        def slow(it, carry):
            row, h = it // HEADS, lax.rem(it, HEADS)
            q = qs[row // 4, h, :, pl.ds(joff, JB)]

            def scores(kb, carry):
                ks = pl.ds(pl.multiple_of(kb * KB, KB), KB)
                rhs = jnp.concatenate([bt[h, ks], q], axis=0)
                lhs = jnp.concatenate([eye, km[row, h, ks]], axis=1)
                s1 = jnp.dot(lhs, rhs, preferred_element_type=F32)
                s1 = jnp.where(mcol_ref[ks] > 0.5, s1, -1e30)
                ss[ks] = s1
                return jnp.maximum(carry, jnp.max(s1, axis=0, keepdims=True))

            top = lax.fori_loop(0, nk, scores, jnp.full((1, JB), -1e30, F32))

            def weights(kb, carry):
                ks = pl.ds(pl.multiple_of(kb * KB, KB), KB)
                pa[0, ks] = jnp.exp2(ss[ks] - top).astype(BF16)
                return carry

            lax.fori_loop(0, nk, weights, 0)
            oe = jnp.dot(vx[row, h], pa[0], preferred_element_type=F32)
            ot[row, head_slice(h)] = oe[:HEAD_DIM] / oe[HEAD_DIM : HEAD_DIM + 1]
            return carry

        lax.fori_loop(0, rows * HEADS, slow, 0)

    def last(i, carry):
        for r in range(UNROLL):
            finish(UNROLL * i + r)
        return carry

    lax.fori_loop(0, rows // UNROLL, last, 0)

    span = JB // rows
    out_row = lax.broadcasted_iota(jnp.int32, (JB, JB), 0)
    in_row = lax.broadcasted_iota(jnp.int32, (JB, JB), 1)
    perm = (in_row == lax.rem(out_row, rows) * span + out_row // rows).astype(F32).astype(BF16)
    for q in range(rows // 2):
        cols = [
            jnp.concatenate([zz[r, span * n : span * (n + 1)] for r in range(rows)], axis=0)
            for n in (2 * q, 2 * q + 1)
        ]
        moved = jnp.dot(perm, jnp.concatenate(cols, axis=1), preferred_element_type=F32).astype(BF16)
        o_ref[2 * JB * q : 2 * JB * q + JB] = moved[:, :chan]
        o_ref[2 * JB * q + JB : 2 * JB * (q + 1)] = moved[:, chan:]


def attention(x, a, proj, gate_bias, out_w, mrow, mcol, bias, trans=()):
    rows, res, chan = x.shape
    nj = res // JB
    full = lambda a: pl.BlockSpec(a.shape, lambda j, n=a.ndim: (0,) * n)
    ins = [x, a, proj, gate_bias, out_w, mrow, mcol]
    specs = [full(a) for a in ins] + [pl.BlockSpec((HEADS, JB, res), lambda j: (0, j, 0))]
    ins.append(bias)
    ins += trans
    specs += [full(a) for a in trans]
    return pl.pallas_call(
        functools.partial(attn_kernel, bool(trans)),
        grid=(nj,),
        out_shape=jax.ShapeDtypeStruct((res * rows, chan), BF16),
        in_specs=specs,
        out_specs=pl.BlockSpec((JB * rows, chan), lambda j: (j, 0)),
        scratch_shapes=[
            pltpu.VMEM((rows, HEADS, res, chan), BF16),
            pltpu.VMEM((rows // 4, HEADS, chan, res), BF16),
            pltpu.VMEM((rows, HEADS, HEAD_DIM + 16, res), BF16),
            pltpu.VMEM((rows, chan, res), F32),
            pltpu.VMEM((HEADS, res, JB), BF16),
            pltpu.VMEM((4, res, JB), BF16),
            pltpu.VMEM((4, res, JB), BF16),
            pltpu.VMEM((rows, chan, JB), F32),
            pltpu.VMEM((4, chan, chan), BF16),
            pltpu.VMEM((4, chan, chan), BF16),
            pltpu.VMEM((res, JB), F32),
            pltpu.VMEM((1, JB), F32),
            pltpu.VMEM((rows, JB, chan), BF16),
        ],
        compiler_params=pltpu.CompilerParams(
            dimension_semantics=("arbitrary",), vmem_limit_bytes=60 * 1024 * 1024
        ),
    )(*ins)


def exchange_kernel(n, z_ref, o_ref, send_sem, recv_sem, own_sem):
    rows = o_ref.shape[0]
    gy = n // 16
    me = lax.axis_index("gx") * gy + lax.axis_index("gy")
    at = lambda d: {"gx": d // gy, "gy": lax.rem(d, gy)}
    barrier = pltpu.get_barrier_semaphore()

    def greet(t, carry):
        pl.semaphore_signal(
            barrier, inc=1, device_id=at(lax.rem(me + t, n)), device_id_type=pl.DeviceIdType.MESH
        )
        return carry

    lax.fori_loop(1, n, greet, 0)
    mine = pl.ds(pl.multiple_of(rows * me, rows), rows)
    own = pltpu.make_async_copy(z_ref.at[mine], o_ref.at[:, mine], own_sem)
    own.start()
    pl.semaphore_wait(barrier, n - 1)

    def copy(t, to, frm):
        return pltpu.make_async_remote_copy(
            src_ref=z_ref.at[pl.ds(pl.multiple_of(rows * to, rows), rows)],
            dst_ref=o_ref.at[:, pl.ds(pl.multiple_of(rows * frm, rows), rows)],
            send_sem=send_sem.at[t], recv_sem=recv_sem.at[t],
            device_id=at(to), device_id_type=pl.DeviceIdType.MESH,
        )

    def send(t, carry):
        copy(t, lax.rem(me + t, n), me).start()
        return carry

    lax.fori_loop(1, n, send, 0)
    own.wait()

    def land(t, carry):
        copy(t, lax.rem(me + t, n), lax.rem(me + n - t, n)).wait_recv()
        copy(t, lax.rem(me + t, n), me).wait_send()
        return carry

    lax.fori_loop(1, n, land, 0)


def exchange(cid, n, z, rows):
    res = z.shape[0] // rows
    return pl.pallas_call(
        functools.partial(exchange_kernel, n),
        out_shape=jax.ShapeDtypeStruct((rows, res, z.shape[1]), BF16),
        in_specs=[pl.BlockSpec(memory_space=pl.ANY)],
        out_specs=pl.BlockSpec(memory_space=pl.ANY),
        scratch_shapes=[
            pltpu.SemaphoreType.DMA((n,)),
            pltpu.SemaphoreType.DMA((n,)),
            pltpu.SemaphoreType.DMA,
        ],
        compiler_params=pltpu.CompilerParams(collective_id=cid, has_side_effects=True),
    )(z.reshape(res, rows, z.shape[1]))


def local(
    pair_in,
    residue_mask,
    norm_start,
    proj_start,
    gate_bias_start,
    bias_w_start,
    out_w_start,
    norm_end,
    proj_end,
    gate_bias_end,
    bias_w_end,
    out_w_end,
    norm_trans,
    trans_in,
    trans_bias,
    trans_out,
):
    rows, res, chan = pair_in.shape
    n = lax.axis_size(("gx", "gy"))
    row = lambda v: v.reshape(1, -1)
    mine = jnp.pad(residue_mask.astype(F32).reshape(1, rows), ((0, 7), (0, 128 - rows)))
    bias, normed = pair_bias(pair_in, row(norm_start), bias_w_start)
    bias, mask = gather(0, bias, mine)
    mask = mask[:, 0, :rows].reshape(res)
    mask = jnp.where(jnp.max(mask) > 0.5, mask, 1.0)
    mrow, mcol = mask.reshape(1, res), mask.reshape(res, 1)

    z1 = attention(
        pair_in, normed, proj_start, row(gate_bias_start), out_w_start, mrow, mcol, bias
    )
    cols = exchange(2, n, z1, rows)
    bias, normed = pair_bias(cols, row(norm_end), bias_w_end)
    bias = gather(1, bias)
    out = attention(
        cols, normed, proj_end, row(gate_bias_end), out_w_end, mrow, mcol, bias,
        (row(norm_trans), trans_in, row(trans_bias), trans_out),
    )
    return exchange(3, n, out, rows)


def solution(mesh):
    spec = P(("gx", "gy"), None, None)
    placed = (spec, P(("gx", "gy"))) + (P(),) * 14
    return jax.shard_map(local, mesh=mesh, in_specs=placed, out_specs=spec, check_vma=False)
```

```python
import functools
import types

import jax
import jax.numpy as jnp
from jax import lax
from jax.experimental import pallas as pl
from jax.experimental.pallas import tpu as pltpu
from jax.sharding import PartitionSpec as P

HEADS = 4
HEAD_DIM = 32
LOG2E = 1.4426950408889634
JB = 256
KB = 128
UNROLL = 4
F32 = jnp.float32
BF16 = jnp.bfloat16
NT = (((1,), (1,)), ((), ()))
TN = (((0,), (0,)), ((), ()))
VMEM = pl.BlockSpec(memory_space=pltpu.VMEM)


def layer_norm(t, gain):
    chan = t.shape[1]
    mean = jnp.dot(t, jnp.full((chan, chan), 1.0 / chan, BF16), preferred_element_type=F32)
    cent = t.astype(F32) - mean
    var = jnp.mean(cent * cent, axis=-1, keepdims=True)
    return (cent * lax.rsqrt(var + 1e-05) * gain).astype(BF16)


def bias_kernel(x_ref, g_ref, bw_ref, o_ref, a_ref):
    bwt = bw_ref[...].astype(F32).T.astype(BF16)
    gain = g_ref[...]
    for r in range(x_ref.shape[0]):
        a = layer_norm(x_ref[r], gain)
        a_ref[r] = a
        b = lax.dot_general(bwt, a, NT, preferred_element_type=F32) * LOG2E
        o_ref[:, r, :] = b[:HEADS].astype(BF16)


def pair_bias(x, gain, bias_w):
    rows, res, chan = x.shape
    bw = jnp.pad(bias_w, ((0, 0), (0, 128 - HEADS)))
    return pl.pallas_call(
        bias_kernel,
        out_shape=[
            jax.ShapeDtypeStruct((HEADS, rows, res), BF16),
            jax.ShapeDtypeStruct(x.shape, BF16),
        ],
        in_specs=[VMEM] * 3,
        out_specs=[VMEM] * 2,
    )(x, gain, bw)


ORDERS = (
    ("xyz", "yzx", "zxy", "xyz", "yzx"),
    ("yzx", "zxy", "xyz", "yzx", "xyz"),
)


def place():
    gx, gy = lax.axis_index("gx"), lax.axis_index("gy")
    return {
        "x": lax.rem(gx // 2, 4),
        "y": gy // 2,
        "z": 2 * lax.rem(gy, 2) + gx // 8,
        "c": lax.rem(gx, 2),
    }


def device(at):
    z_lo, z_hi = lax.rem(at["z"], 2), at["z"] // 2
    return {"gx": (z_lo * 4 + at["x"]) * 2 + at["c"], "gy": at["y"] * 2 + z_hi}


def shift(at, dim, by):
    return {**at, dim: lax.rem(at[dim] + by + 4, 4)}


def part(ref, lead, at, free, tail=()):
    z = "z" in free
    pick = lambda d: slice(None) if d in free else at[d]
    z_lo = slice(None) if z else lax.rem(at["z"], 2)
    z_hi = slice(None) if z else at["z"] // 2
    return ref.at[lead + (z_lo, pick("x"), at["c"], pick("y"), z_hi) + tail]


def gather_kernel(n_out, *refs):
    ins, outs = refs[:n_out], refs[n_out : 2 * n_out]
    ring_send, ring_recv, pair_send, pair_recv, own_sem = refs[2 * n_out :]
    me = place()
    barrier = pltpu.get_barrier_semaphore()
    sib = {**me, "c": 1 - me["c"]}
    partners = [shift(me, d, by) for d in "xyz" for by in (1, -1)] + [sib]
    for at in partners:
        pl.semaphore_signal(barrier, inc=1, device_id=device(at), device_id_type=pl.DeviceIdType.MESH)
    pl.semaphore_wait(barrier, len(partners))

    def items(core):
        half = outs[0].shape[-1] // 2
        got = []
        for h in range(HEADS):
            got.append((h, ins[0].at[h], functools.partial(part, outs[0], (h,)), half))
        if n_out == 2:
            got.append((HEADS, ins[1], functools.partial(part, outs[1], ()), 0))
        return got

    def copy(src, dst, sems, idx, to):
        return pltpu.make_async_remote_copy(
            src_ref=src, dst_ref=dst, send_sem=sems[0].at[idx], recv_sem=sems[1].at[idx],
            device_id=device(to), device_id_type=pl.DeviceIdType.MESH,
        )

    ring, pair = (ring_send, ring_recv), (pair_send, pair_recv)

    def run(core):
        at = {**me, "c": core}
        other = {**me, "c": 1 - core}
        todo = items(core)
        sends = []

        def step0(p, idx, own, sets, half):
            d, free = ORDERS[core][idx][p], ORDERS[core][idx][:p]
            src = sets(at, free)
            for k, by in enumerate((1, -1)):
                c = copy(own if p == 0 else src, src, ring, (idx, p, k), shift(at, d, by))
                c.start()
                sends.append(c)

        def step1(p, idx, own, sets, half):
            d, free = ORDERS[core][idx][p], ORDERS[core][idx][:p]
            for k, by in enumerate((1, -1)):
                got = sets(shift(at, d, -by), free)
                copy(got, got, ring, (idx, p, k), shift(at, d, by)).wait_recv()
                if half:
                    tail = (slice(None), pl.ds(k * half, half))
                    piece = sets(shift(at, d, -by), free, tail)
                elif k == 0:
                    piece = got
                else:
                    continue
                c = copy(piece, piece, ring, (idx, p, 2 + k), shift(at, d, by))
                c.start()
                sends.append(c)

        def step2(p, idx, own, sets, half):
            d, free = ORDERS[core][idx][p], ORDERS[core][idx][:p]
            for k, by in enumerate((1, -1)):
                if half:
                    tail = (slice(None), pl.ds(k * half, half))
                    piece = sets(shift(at, d, 2), free, tail)
                elif k == 0:
                    piece = sets(shift(at, d, 2), free)
                else:
                    continue
                copy(piece, piece, ring, (idx, p, 2 + k), shift(at, d, by)).wait_recv()

        def across(idx, sets, hop):
            d, free = ORDERS[core][idx][2], ORDERS[core][idx][:2]
            piece = sets(shift(at, d, hop), free)
            c = copy(piece, piece, pair, (idx, hop), other)
            c.start()
            sends.append(c)

        own_copies = []
        for idx, own, sets, half in todo:
            step0(0, idx, own, sets, half)
            mine = pltpu.make_async_copy(own, sets(at, ""), own_sem.at[idx])
            mine.start()
            own_copies.append(mine)
        for p in range(3):
            for t in todo:
                step1(p, *t)
                if p == 2:
                    for hop in (1, 3):
                        across(t[0], t[2], hop)
            for i, t in enumerate(todo):
                if p == 0:
                    own_copies[i].wait()
                step2(p, *t)
                if p < 2:
                    step0(p + 1, *t)
                if p == 1:
                    across(t[0], t[2], 0)
                if p == 2:
                    across(t[0], t[2], 2)
        for idx, own, sets, half in todo:
            d, free = ORDERS[1 - core][idx][2], ORDERS[1 - core][idx][:2]
            for hop in range(4):
                piece = sets(shift(other, d, hop), free)
                copy(piece, piece, pair, (idx, hop), other).wait_recv()
        for c in sends:
            c.wait_send()

    for core in range(2):
        pl.when(me["c"] == core)(functools.partial(run, core))


def gather(cid, bias, *mask):
    heads, rows, res = bias.shape
    grid = (2, 4, 2, 4, 2)
    outs = [jax.ShapeDtypeStruct((heads,) + grid + (rows, res), BF16)]
    if mask:
        outs.append(jax.ShapeDtypeStruct(grid + mask[0].shape, F32))
    n = len(outs)
    got = pl.pallas_call(
        functools.partial(gather_kernel, n),
        out_shape=outs,
        in_specs=[VMEM] * n,
        out_specs=[pl.BlockSpec(memory_space=pl.ANY)] * n,
        scratch_shapes=[
            pltpu.SemaphoreType.DMA((5, 3, 4)),
            pltpu.SemaphoreType.DMA((5, 3, 4)),
            pltpu.SemaphoreType.DMA((5, 4)),
            pltpu.SemaphoreType.DMA((5, 4)),
            pltpu.SemaphoreType.DMA((5,)),
        ],
        compiler_params=pltpu.CompilerParams(collective_id=cid, has_side_effects=True),
    )(bias, *mask)
    full = got[0].reshape(heads, -1, res)
    return (full, got[1].reshape((-1,) + mask[0].shape)) if mask else full


def stage_tools(trans, m):
    rows, res, chan = m.x.shape
    groups = rows // 4
    nk = res // KB
    tasks = groups * HEADS
    t = types.SimpleNamespace()

    def eye():
        i = lax.broadcasted_iota(jnp.int32, (KB, KB), 0)
        j = lax.broadcasted_iota(jnp.int32, (KB, KB), 1)
        return (i == j).astype(F32).astype(BF16)

    def project_all():
        w = m.w[...].astype(F32)
        wqt = w[:, :chan].T
        for s in range(4):
            cut = chan - 32 * s
            wk = w[:, chan : 2 * chan]
            m.wk[s] = (pltpu.roll(wk, 32 * s, 1) if s else wk).astype(BF16)
            m.wq[s] = (jnp.concatenate([wqt[cut:], wqt[:cut]], axis=0) if s else wqt).astype(BF16)
        wvt = w[:, 2 * chan : 3 * chan].T.astype(BF16)
        wgt = w[:, 3 * chan :].T.astype(BF16)
        gb = m.gb[...].T
        mrow = m.mrow[...]
        lane = lax.broadcasted_iota(jnp.int32, (1, chan), 1) // HEAD_DIM

        def project(r, carry):
            s = lax.rem(r, 4)
            grp = r // 4
            a = m.a[r]
            kk = jnp.dot(a, m.wk[s], preferred_element_type=F32).astype(BF16)
            qt = (
                lax.dot_general(m.wq[s], a, NT, preferred_element_type=F32)
                * (HEAD_DIM**-0.5 * LOG2E)
            ).astype(BF16)
            vt = lax.dot_general(wvt, a, NT, preferred_element_type=F32) * mrow
            m.gt[r] = jax.nn.sigmoid(lax.dot_general(wgt, a, NT, preferred_element_type=F32) + gb)
            for h in range(HEADS):
                slot = lax.rem(h + s, 4)
                m.km[r, h] = kk * (lane == slot).astype(F32).astype(BF16)
                m.vx[r, h, :HEAD_DIM] = vt[HEAD_DIM * h : HEAD_DIM * (h + 1)].astype(BF16)
                m.vx[r, h, HEAD_DIM:] = jnp.broadcast_to(mrow, (16, res)).astype(BF16)
            for u in range(4):
                hh = lax.rem(u - s + 4, 4)
                m.qs[grp, hh, pl.ds(32 * u, 32)] = qt[32 * u : 32 * (u + 1)]
            return carry

        lax.fori_loop(0, rows, project, 0)

    def turn_bias(b_ref):
        for h in range(HEADS):
            for kb in range(nk):
                sl = slice(KB * kb, KB * (kb + 1))
                m.bt[h, sl] = b_ref[h, :, sl].T

    def head_slice(h):
        return pl.ds(pl.multiple_of(HEAD_DIM * h, HEAD_DIM), HEAD_DIM)

    def fast_heads(joff):
        one = eye()

        def of(k):
            return k // HEADS, lax.rem(k, HEADS)

        def weights_step(k, kb, pp):
            grp, h = of(k)
            sl = slice(KB * kb, KB * (kb + 1))
            rhs = jnp.concatenate([m.bt[h, sl], m.qs[grp, h, :, pl.ds(joff, JB)]], axis=0)
            lhs = jnp.concatenate(
                [jnp.concatenate([one, m.km[grp * 4 + r, h, sl]], axis=1) for r in range(4)], axis=0
            )
            p4 = jnp.exp2(jnp.dot(lhs, rhs, preferred_element_type=F32)).astype(BF16)
            for r in range(4):
                pp[r, sl] = p4[KB * r : KB * (r + 1)]

        def mix_step(k, r, pp):
            grp, h = of(k)
            oe = jnp.dot(m.vx[grp * 4 + r, h], pp[r], preferred_element_type=F32)
            den = oe[HEAD_DIM : HEAD_DIM + 1]
            m.gd[...] = jnp.where((den > 2.0**-60) & (den < 2.0**100), m.gd[...], 0.0)
            m.ot[grp * 4 + r, head_slice(h)] = oe[:HEAD_DIM] / den

        def both(k, new, old):
            for kb in range(nk):
                weights_step(k, kb, new)
                if kb % 2:
                    mix_step(k - 1, kb // 2, old)

        for kb in range(nk):
            weights_step(0, kb, m.pa)

        def pair(i, carry):
            both(2 * i + 1, m.pb, m.pa)
            both(2 * i + 2, m.pa, m.pb)
            return carry

        lax.fori_loop(0, tasks // 2 - 1, pair, 0)
        both(tasks - 1, m.pb, m.pa)
        for r in range(4):
            mix_step(tasks - 1, r, m.pb)

    def safe_heads(joff):
        one = eye()

        def row_head(it, carry):
            row, h = it // HEADS, lax.rem(it, HEADS)
            q = m.qs[row // 4, h, :, pl.ds(joff, JB)]

            def scores(kb, carry):
                ks = pl.ds(pl.multiple_of(kb * KB, KB), KB)
                rhs = jnp.concatenate([m.bt[h, ks], q], axis=0)
                lhs = jnp.concatenate([one, m.km[row, h, ks]], axis=1)
                s1 = jnp.dot(lhs, rhs, preferred_element_type=F32)
                s1 = jnp.where(m.mcol[ks] > 0.5, s1, -1e30)
                m.ss[ks] = s1
                return jnp.maximum(carry, jnp.max(s1, axis=0, keepdims=True))

            top = lax.fori_loop(0, nk, scores, jnp.full((1, JB), -1e30, F32))

            def weights(kb, carry):
                ks = pl.ds(pl.multiple_of(kb * KB, KB), KB)
                m.pa[0, ks] = jnp.exp2(m.ss[ks] - top).astype(BF16)
                return carry

            lax.fori_loop(0, nk, weights, 0)
            oe = jnp.dot(m.vx[row, h], m.pa[0], preferred_element_type=F32)
            m.ot[row, head_slice(h)] = oe[:HEAD_DIM] / oe[HEAD_DIM : HEAD_DIM + 1]
            return carry

        lax.fori_loop(0, rows * HEADS, row_head, 0)

    def finish(joff, store):
        def row(r):
            gated = (m.ot[r] * m.gt[r, :, pl.ds(joff, JB)]).T.astype(BF16)
            z = m.x[r, pl.ds(joff, JB)].astype(F32) + jnp.dot(
                gated, m.ow[...], preferred_element_type=F32
            )
            z = z.astype(BF16)
            if trans:
                zf = z.astype(F32)
                a = layer_norm(z, m.ng[...])
                hid = jnp.dot(a, m.ti[...], preferred_element_type=F32) + m.tb[...]
                hid = jnp.maximum(hid, 0.0).astype(BF16)
                z = (zf + jnp.dot(hid, m.to[...], preferred_element_type=F32)).astype(BF16)
            m.zz[r] = z

        def some(i, carry):
            for r in range(UNROLL):
                row(UNROLL * i + r)
            return carry

        lax.fori_loop(0, rows // UNROLL, some, 0)
        span = JB // rows
        out_row = lax.broadcasted_iota(jnp.int32, (JB, JB), 0)
        in_row = lax.broadcasted_iota(jnp.int32, (JB, JB), 1)
        perm = (in_row == lax.rem(out_row, rows) * span + out_row // rows).astype(F32).astype(BF16)
        for q in range(rows // 2):
            cols = [
                jnp.concatenate([m.zz[r, span * n : span * (n + 1)] for r in range(rows)], axis=0)
                for n in (2 * q, 2 * q + 1)
            ]
            moved = jnp.dot(perm, jnp.concatenate(cols, axis=1), preferred_element_type=F32)
            for n in range(2):
                part = moved[:, chan * n : chan * (n + 1)]
                store(span * (2 * q + n), part.reshape(span, rows, chan).astype(BF16))

    return types.SimpleNamespace(
        project_all=project_all, turn_bias=turn_bias, fast_heads=fast_heads,
        safe_heads=safe_heads, finish=finish,
    )


def stage_names(trans):
    names = ["x", "a", "w", "gb", "ow", "mrow", "mcol"]
    return names + (["ng", "ti", "tb", "to"] if trans else [])


def stage_scratch(rows, res, chan):
    return {
        "km": pltpu.VMEM((rows, HEADS, res, chan), BF16),
        "qs": pltpu.VMEM((rows // 4, HEADS, chan, res), BF16),
        "vx": pltpu.VMEM((rows, HEADS, HEAD_DIM + 16, res), BF16),
        "gt": pltpu.VMEM((rows, chan, res), F32),
        "bt": pltpu.VMEM((HEADS, res, JB), BF16),
        "pa": pltpu.VMEM((4, res, JB), BF16),
        "pb": pltpu.VMEM((4, res, JB), BF16),
        "ot": pltpu.VMEM((rows, chan, JB), F32),
        "wk": pltpu.VMEM((4, chan, chan), BF16),
        "wq": pltpu.VMEM((4, chan, chan), BF16),
        "gd": pltpu.VMEM((1, JB), F32),
        "zz": pltpu.VMEM((rows, JB, chan), BF16),
        "bs": pltpu.VMEM((HEADS, JB, res), BF16),
        "ss": pltpu.VMEM((res, JB), F32),
    }


def safe_kernel(trans, names, *refs):
    m = types.SimpleNamespace(**dict(zip(names, refs)))
    tools = stage_tools(trans, m)

    @pl.when(pl.program_id(0) == 0)
    def _():
        tools.project_all()

    joff = pl.multiple_of(pl.program_id(0) * JB, JB)
    tools.turn_bias(m.b)
    tools.safe_heads(joff)

    def store(at, part):
        m.o[at : at + part.shape[0]] = part

    tools.finish(joff, store)


def safe_attention(ins, bias, trans):
    rows, res, chan = ins[0].shape
    scratch = stage_scratch(rows, res, chan)
    names = stage_names(trans) + ["b", "o"] + list(scratch)
    full = lambda a: pl.BlockSpec(a.shape, lambda j, n=a.ndim: (0,) * n)
    return pl.pallas_call(
        functools.partial(safe_kernel, trans, names),
        grid=(res // JB,),
        out_shape=jax.ShapeDtypeStruct((res, rows, chan), BF16),
        in_specs=[full(a) for a in ins] + [pl.BlockSpec((HEADS, JB, res), lambda j: (0, j, 0))],
        out_specs=pl.BlockSpec((JB, rows, chan), lambda j: (j, 0, 0)),
        scratch_shapes=list(scratch.values()),
        compiler_params=pltpu.CompilerParams(
            dimension_semantics=("arbitrary",), vmem_limit_bytes=60 * 1024 * 1024
        ),
    )(*ins, bias)


def fused_kernel(trans, n, names, *refs):
    m = types.SimpleNamespace(**dict(zip(names, refs)))
    tools = stage_tools(trans, m)
    rows, res, chan = m.x.shape
    nj = res // JB
    per = JB // rows
    gy = n // 16
    me = lax.axis_index("gx") * gy + lax.axis_index("gy")
    at = lambda d: {"gx": d // gy, "gy": lax.rem(d, gy)}
    barrier = pltpu.get_barrier_semaphore()

    def greet(t, carry):
        pl.semaphore_signal(
            barrier, inc=1, device_id=at(lax.rem(me + t, n)), device_id_type=pl.DeviceIdType.MESH
        )
        return carry

    lax.fori_loop(1, n, greet, 0)

    def block_of(t):
        return lax.rem(t + me, nj)

    def fetch(t):
        return pltpu.make_async_copy(
            m.b.at[:, pl.ds(pl.multiple_of(block_of(t) * JB, JB), JB)], m.bs, m.fetch_sem
        )

    def copy(t, i, frm):
        to = block_of(t) * per + i
        ahead = lax.rem(to - me + n, n)
        return to, pltpu.make_async_remote_copy(
            src_ref=m.zs.at[lax.rem(t, 2), pl.ds(pl.multiple_of(i * rows, rows), rows)],
            dst_ref=m.o.at[:, pl.ds(pl.multiple_of(rows * frm, rows), rows)],
            send_sem=m.send_sem.at[ahead], recv_sem=m.recv_sem.at[ahead],
            device_id=at(to), device_id_type=pl.DeviceIdType.MESH,
        )

    def own(t, i):
        mine = pl.ds(pl.multiple_of(rows * me, rows), rows)
        return pltpu.make_async_copy(
            m.zs.at[lax.rem(t, 2), pl.ds(pl.multiple_of(i * rows, rows), rows)],
            m.o.at[:, mine], m.own_sem,
        )

    def send_block(t):
        def send(i, carry):
            to, c = copy(t, i, me)

            @pl.when(to != me)
            def _():
                c.start()

            @pl.when(to == me)
            def _():
                own(t, i).start()

            return carry

        lax.fori_loop(0, per, send, 0)

    def sent_block(t):
        def sent(i, carry):
            to, c = copy(t, i, me)

            @pl.when(to != me)
            def _():
                c.wait_send()

            @pl.when(to == me)
            def _():
                own(t, i).wait()

            return carry

        lax.fori_loop(0, per, sent, 0)

    fetch(0).start()
    tools.project_all()
    m.gd[...] = jnp.ones_like(m.gd)
    pl.semaphore_wait(barrier, n - 1)

    def block(t, carry):
        joff = pl.multiple_of(block_of(t) * JB, JB)
        fetch(t).wait()
        tools.turn_bias(m.bs)

        @pl.when(t > 0)
        def _():
            send_block(t - 1)

        @pl.when(t < nj - 1)
        def _():
            fetch(t + 1).start()

        tools.fast_heads(joff)

        @pl.when(t > 1)
        def _():
            sent_block(t - 2)

        def store(at, part):
            m.zs[lax.rem(t, 2), at : at + part.shape[0]] = part

        tools.finish(joff, store)
        return carry

    lax.fori_loop(0, nj, block, 0)
    good = jnp.min(m.gd[...], axis=1, keepdims=True)
    if trans:
        m.good[...] = jnp.minimum(m.before[...], good)
    else:
        m.good[...] = jnp.broadcast_to(good, m.good.shape)
    send_block(nj - 1)
    if trans:
        def flag(t, carry):
            c = pltpu.make_async_remote_copy(
                src_ref=m.good, dst_ref=m.flags.at[me],
                send_sem=m.fsend.at[t], recv_sem=m.frecv.at[t],
                device_id=at(lax.rem(me + t, n)), device_id_type=pl.DeviceIdType.MESH,
            )
            c.start()
            return carry

        lax.fori_loop(1, n, flag, 0)
        mine = pltpu.make_async_copy(m.good, m.flags.at[me], m.fsend.at[0])
        mine.start()
        mine.wait()
    sent_block(nj - 2)
    sent_block(nj - 1)

    def land(t, carry):
        frm = lax.rem(me + n - t, n)
        pltpu.make_async_remote_copy(
            src_ref=m.zs.at[0, pl.ds(0, rows)],
            dst_ref=m.o.at[:, pl.ds(pl.multiple_of(rows * frm, rows), rows)],
            send_sem=m.send_sem.at[t], recv_sem=m.recv_sem.at[t],
            device_id=at(frm), device_id_type=pl.DeviceIdType.MESH,
        ).wait_recv()
        if trans:
            c = pltpu.make_async_remote_copy(
                src_ref=m.good, dst_ref=m.flags.at[frm],
                send_sem=m.fsend.at[t], recv_sem=m.frecv.at[t],
                device_id=at(frm), device_id_type=pl.DeviceIdType.MESH,
            )
            c.wait_recv()
            c.wait_send()
        return carry

    lax.fori_loop(1, n, land, 0)


def fused_attention(cid, n, ins, bias, before):
    trans = before is not None
    rows, res, chan = ins[0].shape
    scratch = stage_scratch(rows, res, chan)
    del scratch["ss"]
    scratch |= {
        "zs": pltpu.VMEM((2, JB, rows, chan), BF16),
        "send_sem": pltpu.SemaphoreType.DMA((n,)),
        "recv_sem": pltpu.SemaphoreType.DMA((n,)),
        "fetch_sem": pltpu.SemaphoreType.DMA,
        "own_sem": pltpu.SemaphoreType.DMA,
    }
    anywhere = pl.BlockSpec(memory_space=pl.ANY)
    outs = {"o": jax.ShapeDtypeStruct((rows, res, chan), BF16)}
    out_specs = [anywhere]
    names = stage_names(trans) + ["b"]
    args = list(ins) + [bias]
    in_specs = [VMEM] * len(ins) + [anywhere]
    if trans:
        names.append("before")
        args.append(before)
        in_specs.append(VMEM)
        outs["flags"] = jax.ShapeDtypeStruct((n, 8, 128), F32)
        out_specs.append(anywhere)
        scratch |= {
            "good": pltpu.VMEM((8, 128), F32),
            "fsend": pltpu.SemaphoreType.DMA((n,)),
            "frecv": pltpu.SemaphoreType.DMA((n,)),
        }
    else:
        outs["good"] = jax.ShapeDtypeStruct((8, 128), F32)
        out_specs.append(VMEM)
    return pl.pallas_call(
        functools.partial(fused_kernel, trans, n, names + list(outs) + list(scratch)),
        out_shape=list(outs.values()),
        in_specs=in_specs,
        out_specs=out_specs,
        scratch_shapes=list(scratch.values()),
        compiler_params=pltpu.CompilerParams(
            collective_id=cid, has_side_effects=True, vmem_limit_bytes=60 * 1024 * 1024
        ),
    )(*args)


def exchange_kernel(n, z_ref, o_ref, send_sem, recv_sem, own_sem):
    rows = o_ref.shape[0]
    gy = n // 16
    me = lax.axis_index("gx") * gy + lax.axis_index("gy")
    at = lambda d: {"gx": d // gy, "gy": lax.rem(d, gy)}
    barrier = pltpu.get_barrier_semaphore()

    def greet(t, carry):
        pl.semaphore_signal(
            barrier, inc=1, device_id=at(lax.rem(me + t, n)), device_id_type=pl.DeviceIdType.MESH
        )
        return carry

    lax.fori_loop(1, n, greet, 0)
    mine = pl.ds(pl.multiple_of(rows * me, rows), rows)
    own = pltpu.make_async_copy(z_ref.at[mine], o_ref.at[:, mine], own_sem)
    own.start()
    pl.semaphore_wait(barrier, n - 1)

    def copy(t, to, frm):
        return pltpu.make_async_remote_copy(
            src_ref=z_ref.at[pl.ds(pl.multiple_of(rows * to, rows), rows)],
            dst_ref=o_ref.at[:, pl.ds(pl.multiple_of(rows * frm, rows), rows)],
            send_sem=send_sem.at[t], recv_sem=recv_sem.at[t],
            device_id=at(to), device_id_type=pl.DeviceIdType.MESH,
        )

    def send(t, carry):
        copy(t, lax.rem(me + t, n), me).start()
        return carry

    lax.fori_loop(1, n, send, 0)
    own.wait()

    def land(t, carry):
        copy(t, lax.rem(me + t, n), lax.rem(me + n - t, n)).wait_recv()
        copy(t, lax.rem(me + t, n), me).wait_send()
        return carry

    lax.fori_loop(1, n, land, 0)


def exchange(cid, n, z, rows):
    res, _, chan = z.shape
    return pl.pallas_call(
        functools.partial(exchange_kernel, n),
        out_shape=jax.ShapeDtypeStruct((rows, res, chan), BF16),
        in_specs=[pl.BlockSpec(memory_space=pl.ANY)],
        out_specs=pl.BlockSpec(memory_space=pl.ANY),
        scratch_shapes=[
            pltpu.SemaphoreType.DMA((n,)),
            pltpu.SemaphoreType.DMA((n,)),
            pltpu.SemaphoreType.DMA,
        ],
        compiler_params=pltpu.CompilerParams(collective_id=cid, has_side_effects=True),
    )(z)


def local(
    pair_in,
    residue_mask,
    norm_start,
    proj_start,
    gate_bias_start,
    bias_w_start,
    out_w_start,
    norm_end,
    proj_end,
    gate_bias_end,
    bias_w_end,
    out_w_end,
    norm_trans,
    trans_in,
    trans_bias,
    trans_out,
):
    rows, res, chan = pair_in.shape
    n = lax.axis_size(("gx", "gy"))
    row = lambda v: v.reshape(1, -1)
    mine = jnp.pad(residue_mask.astype(F32).reshape(1, rows), ((0, 7), (0, 128 - rows)))
    bias, normed = pair_bias(pair_in, row(norm_start), bias_w_start)
    bias, mask = gather(0, bias, mine)
    mask = mask[:, 0, :rows].reshape(res)
    mask = jnp.where(jnp.max(mask) > 0.5, mask, 1.0)
    mrow, mcol = mask.reshape(1, res), mask.reshape(res, 1)
    start = [pair_in, normed, proj_start, row(gate_bias_start), out_w_start, mrow, mcol]
    ends = [proj_end, row(gate_bias_end), out_w_end, mrow, mcol]
    ends += [row(norm_trans), trans_in, row(trans_bias), trans_out]

    def end_inputs(cols):
        bias, normed = pair_bias(cols, row(norm_end), bias_w_end)
        return [cols, normed] + ends, gather(1, bias)

    def safe(bias):
        cols = exchange(4, n, safe_attention(start, bias, False), rows)
        ins, bias = end_inputs(cols)
        return exchange(5, n, safe_attention(ins, bias, True), rows)

    cols, good = fused_attention(2, n, start, bias, None)
    ins, end_bias = end_inputs(cols)
    out, flags = fused_attention(3, n, ins, end_bias, good)
    return lax.cond(jnp.min(flags) > 0.5, lambda b: out, safe, bias)


def solution(mesh):
    spec = P(("gx", "gy"), None, None)
    placed = (spec, P(("gx", "gy"))) + (P(),) * 14
    return jax.shard_map(local, mesh=mesh, in_specs=placed, out_specs=spec, check_vma=False)
```

```python
import functools
import types

import jax
import jax.numpy as jnp
from jax import lax
from jax.experimental import pallas as pl
from jax.experimental.pallas import tpu as pltpu
from jax.sharding import PartitionSpec as P

HEADS = 4
HEAD_DIM = 32
LOG2E = 1.4426950408889634
JB = 256
KB = 128
UNROLL = 4
F32 = jnp.float32
BF16 = jnp.bfloat16
NT = (((1,), (1,)), ((), ()))
TN = (((0,), (0,)), ((), ()))
VMEM = pl.BlockSpec(memory_space=pltpu.VMEM)


def layer_norm(t, gain):
    chan = t.shape[1]
    mean = jnp.dot(t, jnp.full((chan, chan), 1.0 / chan, BF16), preferred_element_type=F32)
    cent = t.astype(F32) - mean
    var = jnp.mean(cent * cent, axis=-1, keepdims=True)
    return (cent * lax.rsqrt(var + 1e-05) * gain).astype(BF16)


def bias_kernel(x_ref, g_ref, bw_ref, o_ref, a_ref):
    bwt = bw_ref[...].astype(F32).T.astype(BF16)
    gain = g_ref[...]
    for r in range(x_ref.shape[0]):
        a = layer_norm(x_ref[r], gain)
        a_ref[r] = a
        b = lax.dot_general(bwt, a, NT, preferred_element_type=F32) * LOG2E
        o_ref[:, r, :] = b[:HEADS].astype(BF16)


def pair_bias(x, gain, bias_w):
    rows, res, chan = x.shape
    bw = jnp.pad(bias_w, ((0, 0), (0, 128 - HEADS)))
    return pl.pallas_call(
        bias_kernel,
        out_shape=[
            jax.ShapeDtypeStruct((HEADS, rows, res), BF16),
            jax.ShapeDtypeStruct(x.shape, BF16),
        ],
        in_specs=[VMEM] * 3,
        out_specs=[VMEM] * 2,
    )(x, gain, bw)


ORDERS = (
    ("xyz", "yzx", "zxy", "xyz", "yzx"),
    ("yzx", "zxy", "xyz", "yzx", "xyz"),
)


def place():
    gx, gy = lax.axis_index("gx"), lax.axis_index("gy")
    return {
        "x": lax.rem(gx // 2, 4),
        "y": gy // 2,
        "z": 2 * lax.rem(gy, 2) + gx // 8,
        "c": lax.rem(gx, 2),
    }


def device(at):
    z_lo, z_hi = lax.rem(at["z"], 2), at["z"] // 2
    return {"gx": (z_lo * 4 + at["x"]) * 2 + at["c"], "gy": at["y"] * 2 + z_hi}


def shift(at, dim, by):
    return {**at, dim: lax.rem(at[dim] + by + 4, 4)}


def part(ref, lead, at, free, tail=()):
    z = "z" in free
    pick = lambda d: slice(None) if d in free else at[d]
    z_lo = slice(None) if z else lax.rem(at["z"], 2)
    z_hi = slice(None) if z else at["z"] // 2
    return ref.at[lead + (z_lo, pick("x"), at["c"], pick("y"), z_hi) + tail]


def gather_kernel(n_out, *refs):
    ins, outs = refs[:n_out], refs[n_out : 2 * n_out]
    ring_send, ring_recv, pair_send, pair_recv, own_sem = refs[2 * n_out :]
    me = place()
    barrier = pltpu.get_barrier_semaphore()
    sib = {**me, "c": 1 - me["c"]}
    partners = [shift(me, d, by) for d in "xyz" for by in (1, -1)] + [sib]
    for at in partners:
        pl.semaphore_signal(barrier, inc=1, device_id=device(at), device_id_type=pl.DeviceIdType.MESH)
    pl.semaphore_wait(barrier, len(partners))

    def items(core):
        half = outs[0].shape[-1] // 2
        got = []
        for h in range(HEADS):
            got.append((h, ins[0].at[h], functools.partial(part, outs[0], (h,)), half))
        if n_out == 2:
            got.append((HEADS, ins[1], functools.partial(part, outs[1], ()), 0))
        return got

    def copy(src, dst, sems, idx, to):
        return pltpu.make_async_remote_copy(
            src_ref=src, dst_ref=dst, send_sem=sems[0].at[idx], recv_sem=sems[1].at[idx],
            device_id=device(to), device_id_type=pl.DeviceIdType.MESH,
        )

    ring, pair = (ring_send, ring_recv), (pair_send, pair_recv)

    def run(core):
        at = {**me, "c": core}
        other = {**me, "c": 1 - core}
        todo = items(core)
        sends = []

        def step0(p, idx, own, sets, half):
            d, free = ORDERS[core][idx][p], ORDERS[core][idx][:p]
            src = sets(at, free)
            for k, by in enumerate((1, -1)):
                c = copy(own if p == 0 else src, src, ring, (idx, p, k), shift(at, d, by))
                c.start()
                sends.append(c)

        def step1(p, idx, own, sets, half):
            d, free = ORDERS[core][idx][p], ORDERS[core][idx][:p]
            for k, by in enumerate((1, -1)):
                got = sets(shift(at, d, -by), free)
                copy(got, got, ring, (idx, p, k), shift(at, d, by)).wait_recv()
                if half:
                    tail = (slice(None), pl.ds(k * half, half))
                    piece = sets(shift(at, d, -by), free, tail)
                elif k == 0:
                    piece = got
                else:
                    continue
                c = copy(piece, piece, ring, (idx, p, 2 + k), shift(at, d, by))
                c.start()
                sends.append(c)

        def step2(p, idx, own, sets, half):
            d, free = ORDERS[core][idx][p], ORDERS[core][idx][:p]
            for k, by in enumerate((1, -1)):
                if half:
                    tail = (slice(None), pl.ds(k * half, half))
                    piece = sets(shift(at, d, 2), free, tail)
                elif k == 0:
                    piece = sets(shift(at, d, 2), free)
                else:
                    continue
                copy(piece, piece, ring, (idx, p, 2 + k), shift(at, d, by)).wait_recv()

        def across(idx, sets, hop):
            d, free = ORDERS[core][idx][2], ORDERS[core][idx][:2]
            piece = sets(shift(at, d, hop), free)
            c = copy(piece, piece, pair, (idx, hop), other)
            c.start()
            sends.append(c)

        own_copies = []
        for idx, own, sets, half in todo:
            step0(0, idx, own, sets, half)
            mine = pltpu.make_async_copy(own, sets(at, ""), own_sem.at[idx])
            mine.start()
            own_copies.append(mine)
        for p in range(3):
            for t in todo:
                step1(p, *t)
                if p == 2:
                    for hop in (1, 3):
                        across(t[0], t[2], hop)
            for i, t in enumerate(todo):
                if p == 0:
                    own_copies[i].wait()
                step2(p, *t)
                if p < 2:
                    step0(p + 1, *t)
                if p == 1:
                    across(t[0], t[2], 0)
                if p == 2:
                    across(t[0], t[2], 2)
        for idx, own, sets, half in todo:
            d, free = ORDERS[1 - core][idx][2], ORDERS[1 - core][idx][:2]
            for hop in range(4):
                piece = sets(shift(other, d, hop), free)
                copy(piece, piece, pair, (idx, hop), other).wait_recv()
        for c in sends:
            c.wait_send()

    for core in range(2):
        pl.when(me["c"] == core)(functools.partial(run, core))


def gather(cid, bias, *mask):
    heads, rows, res = bias.shape
    grid = (2, 4, 2, 4, 2)
    outs = [jax.ShapeDtypeStruct((heads,) + grid + (rows, res), BF16)]
    if mask:
        outs.append(jax.ShapeDtypeStruct(grid + mask[0].shape, F32))
    n = len(outs)
    got = pl.pallas_call(
        functools.partial(gather_kernel, n),
        out_shape=outs,
        in_specs=[VMEM] * n,
        out_specs=[pl.BlockSpec(memory_space=pl.ANY)] * n,
        scratch_shapes=[
            pltpu.SemaphoreType.DMA((5, 3, 4)),
            pltpu.SemaphoreType.DMA((5, 3, 4)),
            pltpu.SemaphoreType.DMA((5, 4)),
            pltpu.SemaphoreType.DMA((5, 4)),
            pltpu.SemaphoreType.DMA((5,)),
        ],
        compiler_params=pltpu.CompilerParams(collective_id=cid, has_side_effects=True),
    )(bias, *mask)
    full = got[0].reshape(heads, -1, res)
    return (full, got[1].reshape((-1,) + mask[0].shape)) if mask else full


def stage_tools(trans, m):
    rows, res, chan = m.x.shape
    groups = rows // 4
    nk = res // KB
    tasks = groups * HEADS
    t = types.SimpleNamespace()

    def eye():
        i = lax.broadcasted_iota(jnp.int32, (KB, KB), 0)
        j = lax.broadcasted_iota(jnp.int32, (KB, KB), 1)
        return (i == j).astype(F32).astype(BF16)

    def project_all():
        w = m.w[...].astype(F32)
        wqt = w[:, :chan].T
        for s in range(4):
            cut = chan - 32 * s
            wk = w[:, chan : 2 * chan]
            m.wk[s] = (pltpu.roll(wk, 32 * s, 1) if s else wk).astype(BF16)
            m.wq[s] = (jnp.concatenate([wqt[cut:], wqt[:cut]], axis=0) if s else wqt).astype(BF16)
        wvt = w[:, 2 * chan : 3 * chan].T.astype(BF16)
        wgt = w[:, 3 * chan :].T.astype(BF16)
        gb = m.gb[...].T
        mrow = m.mrow[...]
        lane = lax.broadcasted_iota(jnp.int32, (1, chan), 1) // HEAD_DIM

        def project(r, carry):
            s = lax.rem(r, 4)
            grp = r // 4
            a = m.a[r]
            kk = jnp.dot(a, m.wk[s], preferred_element_type=F32).astype(BF16)
            qt = (
                lax.dot_general(m.wq[s], a, NT, preferred_element_type=F32)
                * (HEAD_DIM**-0.5 * LOG2E)
            ).astype(BF16)
            vt = lax.dot_general(wvt, a, NT, preferred_element_type=F32) * mrow
            m.gt[r] = jax.nn.sigmoid(lax.dot_general(wgt, a, NT, preferred_element_type=F32) + gb)
            for h in range(HEADS):
                slot = lax.rem(h + s, 4)
                m.km[r, h] = kk * (lane == slot).astype(F32).astype(BF16)
                m.vx[r, h, :HEAD_DIM] = vt[HEAD_DIM * h : HEAD_DIM * (h + 1)].astype(BF16)
                m.vx[r, h, HEAD_DIM:] = jnp.broadcast_to(mrow, (16, res)).astype(BF16)
            for u in range(4):
                hh = lax.rem(u - s + 4, 4)
                m.qs[grp, hh, pl.ds(32 * u, 32)] = qt[32 * u : 32 * (u + 1)]
            return carry

        lax.fori_loop(0, rows, project, 0)

    def turn_bias(b_ref):
        for h in range(HEADS):
            for kb in range(nk):
                sl = slice(KB * kb, KB * (kb + 1))
                m.bt[h, sl] = b_ref[h, :, sl].T

    def head_slice(h):
        return pl.ds(pl.multiple_of(HEAD_DIM * h, HEAD_DIM), HEAD_DIM)

    def fast_heads(joff):
        one = eye()

        def of(k):
            return k // HEADS, lax.rem(k, HEADS)

        def weights_step(k, kb, pp):
            grp, h = of(k)
            sl = slice(KB * kb, KB * (kb + 1))
            rhs = jnp.concatenate([m.bt[h, sl], m.qs[grp, h, :, pl.ds(joff, JB)]], axis=0)
            lhs = jnp.concatenate(
                [jnp.concatenate([one, m.km[grp * 4 + r, h, sl]], axis=1) for r in range(4)], axis=0
            )
            p4 = jnp.exp2(jnp.dot(lhs, rhs, preferred_element_type=F32)).astype(BF16)
            for r in range(4):
                pp[r, sl] = p4[KB * r : KB * (r + 1)]

        def mix_step(k, r, pp):
            grp, h = of(k)
            oe = jnp.dot(m.vx[grp * 4 + r, h], pp[r], preferred_element_type=F32)
            den = oe[HEAD_DIM : HEAD_DIM + 1]
            m.gd[...] = jnp.where((den > 2.0**-60) & (den < 2.0**100), m.gd[...], 0.0)
            m.ot[grp * 4 + r, head_slice(h)] = oe[:HEAD_DIM] / den

        def both(k, new, old):
            for kb in range(nk):
                weights_step(k, kb, new)
                if kb % 2:
                    mix_step(k - 1, kb // 2, old)

        for kb in range(nk):
            weights_step(0, kb, m.pa)

        def pair(i, carry):
            both(2 * i + 1, m.pb, m.pa)
            both(2 * i + 2, m.pa, m.pb)
            return carry

        lax.fori_loop(0, tasks // 2 - 1, pair, 0)
        both(tasks - 1, m.pb, m.pa)
        for r in range(4):
            mix_step(tasks - 1, r, m.pb)

    def safe_heads(joff):
        one = eye()

        def row_head(it, carry):
            row, h = it // HEADS, lax.rem(it, HEADS)
            q = m.qs[row // 4, h, :, pl.ds(joff, JB)]

            def scores(kb, carry):
                ks = pl.ds(pl.multiple_of(kb * KB, KB), KB)
                rhs = jnp.concatenate([m.bt[h, ks], q], axis=0)
                lhs = jnp.concatenate([one, m.km[row, h, ks]], axis=1)
                s1 = jnp.dot(lhs, rhs, preferred_element_type=F32)
                s1 = jnp.where(m.mcol[ks] > 0.5, s1, -1e30)
                m.ss[ks] = s1
                return jnp.maximum(carry, jnp.max(s1, axis=0, keepdims=True))

            top = lax.fori_loop(0, nk, scores, jnp.full((1, JB), -1e30, F32))

            def weights(kb, carry):
                ks = pl.ds(pl.multiple_of(kb * KB, KB), KB)
                m.pa[0, ks] = jnp.exp2(m.ss[ks] - top).astype(BF16)
                return carry

            lax.fori_loop(0, nk, weights, 0)
            oe = jnp.dot(m.vx[row, h], m.pa[0], preferred_element_type=F32)
            m.ot[row, head_slice(h)] = oe[:HEAD_DIM] / oe[HEAD_DIM : HEAD_DIM + 1]
            return carry

        lax.fori_loop(0, rows * HEADS, row_head, 0)

    def finish(joff, store):
        def row(r):
            gated = (m.ot[r] * m.gt[r, :, pl.ds(joff, JB)]).T.astype(BF16)
            z = m.x[r, pl.ds(joff, JB)].astype(F32) + jnp.dot(
                gated, m.ow[...], preferred_element_type=F32
            )
            z = z.astype(BF16)
            if trans:
                zf = z.astype(F32)
                a = layer_norm(z, m.ng[...])
                hid = jnp.dot(a, m.ti[...], preferred_element_type=F32) + m.tb[...]
                hid = jnp.maximum(hid, 0.0).astype(BF16)
                z = (zf + jnp.dot(hid, m.to[...], preferred_element_type=F32)).astype(BF16)
            m.zz[r] = z

        def some(i, carry):
            for r in range(UNROLL):
                row(UNROLL * i + r)
            return carry

        lax.fori_loop(0, rows // UNROLL, some, 0)
        span = JB // rows
        out_row = lax.broadcasted_iota(jnp.int32, (JB, JB), 0)
        in_row = lax.broadcasted_iota(jnp.int32, (JB, JB), 1)
        perm = (in_row == lax.rem(out_row, rows) * span + out_row // rows).astype(F32).astype(BF16)
        for q in range(rows // 2):
            cols = [
                jnp.concatenate([m.zz[r, span * n : span * (n + 1)] for r in range(rows)], axis=0)
                for n in (2 * q, 2 * q + 1)
            ]
            moved = jnp.dot(perm, jnp.concatenate(cols, axis=1), preferred_element_type=F32)
            for n in range(2):
                part = moved[:, chan * n : chan * (n + 1)]
                store(span * (2 * q + n), part.reshape(span, rows, chan).astype(BF16))

    return types.SimpleNamespace(
        project_all=project_all, turn_bias=turn_bias, fast_heads=fast_heads,
        safe_heads=safe_heads, finish=finish,
    )


def stage_names(trans):
    names = ["x", "a", "w", "gb", "ow", "mrow", "mcol"]
    return names + (["ng", "ti", "tb", "to"] if trans else [])


def stage_scratch(rows, res, chan):
    return {
        "km": pltpu.VMEM((rows, HEADS, res, chan), BF16),
        "qs": pltpu.VMEM((rows // 4, HEADS, chan, res), BF16),
        "vx": pltpu.VMEM((rows, HEADS, HEAD_DIM + 16, res), BF16),
        "gt": pltpu.VMEM((rows, chan, res), F32),
        "bt": pltpu.VMEM((HEADS, res, JB), BF16),
        "pa": pltpu.VMEM((4, res, JB), BF16),
        "pb": pltpu.VMEM((4, res, JB), BF16),
        "ot": pltpu.VMEM((rows, chan, JB), F32),
        "wk": pltpu.VMEM((4, chan, chan), BF16),
        "wq": pltpu.VMEM((4, chan, chan), BF16),
        "gd": pltpu.VMEM((1, JB), F32),
        "zz": pltpu.VMEM((rows, JB, chan), BF16),
        "bs": pltpu.VMEM((HEADS, JB, res), BF16),
        "ss": pltpu.VMEM((res, JB), F32),
    }


def safe_kernel(trans, names, *refs):
    m = types.SimpleNamespace(**dict(zip(names, refs)))
    tools = stage_tools(trans, m)

    @pl.when(pl.program_id(0) == 0)
    def _():
        tools.project_all()

    joff = pl.multiple_of(pl.program_id(0) * JB, JB)
    tools.turn_bias(m.b)
    tools.safe_heads(joff)

    def store(at, part):
        m.o[at : at + part.shape[0]] = part

    tools.finish(joff, store)


def safe_attention(ins, bias, trans):
    rows, res, chan = ins[0].shape
    scratch = stage_scratch(rows, res, chan)
    names = stage_names(trans) + ["b", "o"] + list(scratch)
    full = lambda a: pl.BlockSpec(a.shape, lambda j, n=a.ndim: (0,) * n)
    return pl.pallas_call(
        functools.partial(safe_kernel, trans, names),
        grid=(res // JB,),
        out_shape=jax.ShapeDtypeStruct((res, rows, chan), BF16),
        in_specs=[full(a) for a in ins] + [pl.BlockSpec((HEADS, JB, res), lambda j: (0, j, 0))],
        out_specs=pl.BlockSpec((JB, rows, chan), lambda j: (j, 0, 0)),
        scratch_shapes=list(scratch.values()),
        compiler_params=pltpu.CompilerParams(
            dimension_semantics=("arbitrary",), vmem_limit_bytes=60 * 1024 * 1024
        ),
    )(*ins, bias)


def fused_kernel(trans, n, names, *refs):
    m = types.SimpleNamespace(**dict(zip(names, refs)))
    tools = stage_tools(trans, m)
    rows, res, chan = m.x.shape
    nj = res // JB
    per = JB // rows
    gy = n // 16
    me = lax.axis_index("gx") * gy + lax.axis_index("gy")
    at = lambda d: {"gx": d // gy, "gy": lax.rem(d, gy)}
    barrier = pltpu.get_barrier_semaphore()

    def greet(t, carry):
        pl.semaphore_signal(
            barrier, inc=1, device_id=at(lax.rem(me + t, n)), device_id_type=pl.DeviceIdType.MESH
        )
        return carry

    lax.fori_loop(1, n, greet, 0)

    def block_of(t):
        return lax.rem(t + me, nj)

    def fetch(t):
        return pltpu.make_async_copy(
            m.b.at[:, pl.ds(pl.multiple_of(block_of(t) * JB, JB), JB)], m.bs, m.fetch_sem
        )

    def copy(t, i, frm):
        to = block_of(t) * per + i
        ahead = lax.rem(to - me + n, n)
        return to, pltpu.make_async_remote_copy(
            src_ref=m.zs.at[lax.rem(t, 2), pl.ds(pl.multiple_of(i * rows, rows), rows)],
            dst_ref=m.o.at[:, pl.ds(pl.multiple_of(rows * frm, rows), rows)],
            send_sem=m.send_sem.at[ahead], recv_sem=m.recv_sem.at[ahead],
            device_id=at(to), device_id_type=pl.DeviceIdType.MESH,
        )

    def own(t, i):
        mine = pl.ds(pl.multiple_of(rows * me, rows), rows)
        return pltpu.make_async_copy(
            m.zs.at[lax.rem(t, 2), pl.ds(pl.multiple_of(i * rows, rows), rows)],
            m.o.at[:, mine], m.own_sem,
        )

    def send_block(t):
        def send(k, carry):
            i = lax.rem(k + me // nj, per)
            to, c = copy(t, i, me)

            @pl.when(to != me)
            def _():
                c.start()

            @pl.when(to == me)
            def _():
                own(t, i).start()

            return carry

        lax.fori_loop(0, per, send, 0)

    def sent_block(t):
        def sent(k, carry):
            i = lax.rem(k + me // nj, per)
            to, c = copy(t, i, me)

            @pl.when(to != me)
            def _():
                c.wait_send()

            @pl.when(to == me)
            def _():
                own(t, i).wait()

            return carry

        lax.fori_loop(0, per, sent, 0)

    fetch(0).start()
    tools.project_all()
    m.gd[...] = jnp.ones_like(m.gd)
    pl.semaphore_wait(barrier, n - 1)

    def block(t, carry):
        joff = pl.multiple_of(block_of(t) * JB, JB)
        fetch(t).wait()
        tools.turn_bias(m.bs)

        @pl.when(t > 0)
        def _():
            send_block(t - 1)

        @pl.when(t < nj - 1)
        def _():
            fetch(t + 1).start()

        tools.fast_heads(joff)

        @pl.when(t > 1)
        def _():
            sent_block(t - 2)

        def store(at, part):
            m.zs[lax.rem(t, 2), at : at + part.shape[0]] = part

        tools.finish(joff, store)
        return carry

    lax.fori_loop(0, nj, block, 0)
    good = jnp.min(m.gd[...], axis=1, keepdims=True)
    if trans:
        m.good[...] = jnp.minimum(m.before[...], good)
    else:
        m.good[...] = jnp.broadcast_to(good, m.good.shape)
    send_block(nj - 1)
    if trans:
        def flag(t, carry):
            c = pltpu.make_async_remote_copy(
                src_ref=m.good.at[pl.ds(0, 1)], dst_ref=m.flags.at[me, pl.ds(0, 1)],
                send_sem=m.fsend.at[t], recv_sem=m.frecv.at[t],
                device_id=at(lax.rem(me + t, n)), device_id_type=pl.DeviceIdType.MESH,
            )
            c.start()
            return carry

        lax.fori_loop(1, n, flag, 0)
        mine = pltpu.make_async_copy(m.good, m.flags.at[me], m.fsend.at[0])
        mine.start()
        mine.wait()
    sent_block(nj - 2)
    sent_block(nj - 1)

    def land(t, carry):
        frm = lax.rem(me + n - t, n)
        pltpu.make_async_remote_copy(
            src_ref=m.zs.at[0, pl.ds(0, rows)],
            dst_ref=m.o.at[:, pl.ds(pl.multiple_of(rows * frm, rows), rows)],
            send_sem=m.send_sem.at[t], recv_sem=m.recv_sem.at[t],
            device_id=at(frm), device_id_type=pl.DeviceIdType.MESH,
        ).wait_recv()
        if trans:
            c = pltpu.make_async_remote_copy(
                src_ref=m.good.at[pl.ds(0, 1)], dst_ref=m.flags.at[frm, pl.ds(0, 1)],
                send_sem=m.fsend.at[t], recv_sem=m.frecv.at[t],
                device_id=at(frm), device_id_type=pl.DeviceIdType.MESH,
            )
            c.wait_recv()
            c.wait_send()
        return carry

    lax.fori_loop(1, n, land, 0)


def fused_attention(cid, n, ins, bias, before):
    trans = before is not None
    rows, res, chan = ins[0].shape
    scratch = stage_scratch(rows, res, chan)
    del scratch["ss"]
    scratch |= {
        "zs": pltpu.VMEM((2, JB, rows, chan), BF16),
        "send_sem": pltpu.SemaphoreType.DMA((n,)),
        "recv_sem": pltpu.SemaphoreType.DMA((n,)),
        "fetch_sem": pltpu.SemaphoreType.DMA,
        "own_sem": pltpu.SemaphoreType.DMA,
    }
    anywhere = pl.BlockSpec(memory_space=pl.ANY)
    outs = {"o": jax.ShapeDtypeStruct((rows, res, chan), BF16)}
    out_specs = [anywhere]
    names = stage_names(trans) + ["b"]
    args = list(ins) + [bias]
    in_specs = [VMEM] * len(ins) + [anywhere]
    if trans:
        names.append("before")
        args.append(before)
        in_specs.append(VMEM)
        outs["flags"] = jax.ShapeDtypeStruct((n, 8, 128), F32)
        out_specs.append(anywhere)
        scratch |= {
            "good": pltpu.VMEM((8, 128), F32),
            "fsend": pltpu.SemaphoreType.DMA((n,)),
            "frecv": pltpu.SemaphoreType.DMA((n,)),
        }
    else:
        outs["good"] = jax.ShapeDtypeStruct((8, 128), F32)
        out_specs.append(VMEM)
    return pl.pallas_call(
        functools.partial(fused_kernel, trans, n, names + list(outs) + list(scratch)),
        out_shape=list(outs.values()),
        in_specs=in_specs,
        out_specs=out_specs,
        scratch_shapes=list(scratch.values()),
        compiler_params=pltpu.CompilerParams(
            collective_id=cid, has_side_effects=True, vmem_limit_bytes=60 * 1024 * 1024
        ),
    )(*args)


def exchange_kernel(n, z_ref, o_ref, send_sem, recv_sem, own_sem):
    rows = o_ref.shape[0]
    gy = n // 16
    me = lax.axis_index("gx") * gy + lax.axis_index("gy")
    at = lambda d: {"gx": d // gy, "gy": lax.rem(d, gy)}
    barrier = pltpu.get_barrier_semaphore()

    def greet(t, carry):
        pl.semaphore_signal(
            barrier, inc=1, device_id=at(lax.rem(me + t, n)), device_id_type=pl.DeviceIdType.MESH
        )
        return carry

    lax.fori_loop(1, n, greet, 0)
    mine = pl.ds(pl.multiple_of(rows * me, rows), rows)
    own = pltpu.make_async_copy(z_ref.at[mine], o_ref.at[:, mine], own_sem)
    own.start()
    pl.semaphore_wait(barrier, n - 1)

    def copy(t, to, frm):
        return pltpu.make_async_remote_copy(
            src_ref=z_ref.at[pl.ds(pl.multiple_of(rows * to, rows), rows)],
            dst_ref=o_ref.at[:, pl.ds(pl.multiple_of(rows * frm, rows), rows)],
            send_sem=send_sem.at[t], recv_sem=recv_sem.at[t],
            device_id=at(to), device_id_type=pl.DeviceIdType.MESH,
        )

    def send(t, carry):
        copy(t, lax.rem(me + t, n), me).start()
        return carry

    lax.fori_loop(1, n, send, 0)
    own.wait()

    def land(t, carry):
        copy(t, lax.rem(me + t, n), lax.rem(me + n - t, n)).wait_recv()
        copy(t, lax.rem(me + t, n), me).wait_send()
        return carry

    lax.fori_loop(1, n, land, 0)


def exchange(cid, n, z, rows):
    res, _, chan = z.shape
    return pl.pallas_call(
        functools.partial(exchange_kernel, n),
        out_shape=jax.ShapeDtypeStruct((rows, res, chan), BF16),
        in_specs=[pl.BlockSpec(memory_space=pl.ANY)],
        out_specs=pl.BlockSpec(memory_space=pl.ANY),
        scratch_shapes=[
            pltpu.SemaphoreType.DMA((n,)),
            pltpu.SemaphoreType.DMA((n,)),
            pltpu.SemaphoreType.DMA,
        ],
        compiler_params=pltpu.CompilerParams(collective_id=cid, has_side_effects=True),
    )(z)


def local(
    pair_in,
    residue_mask,
    norm_start,
    proj_start,
    gate_bias_start,
    bias_w_start,
    out_w_start,
    norm_end,
    proj_end,
    gate_bias_end,
    bias_w_end,
    out_w_end,
    norm_trans,
    trans_in,
    trans_bias,
    trans_out,
):
    rows, res, chan = pair_in.shape
    n = lax.axis_size(("gx", "gy"))
    row = lambda v: v.reshape(1, -1)
    mine = jnp.pad(residue_mask.astype(F32).reshape(1, rows), ((0, 7), (0, 128 - rows)))
    bias, normed = pair_bias(pair_in, row(norm_start), bias_w_start)
    bias, mask = gather(0, bias, mine)
    mask = mask[:, 0, :rows].reshape(res)
    mask = jnp.where(jnp.max(mask) > 0.5, mask, 1.0)
    mrow, mcol = mask.reshape(1, res), mask.reshape(res, 1)
    start = [pair_in, normed, proj_start, row(gate_bias_start), out_w_start, mrow, mcol]
    ends = [proj_end, row(gate_bias_end), out_w_end, mrow, mcol]
    ends += [row(norm_trans), trans_in, row(trans_bias), trans_out]

    def end_inputs(cols):
        bias, normed = pair_bias(cols, row(norm_end), bias_w_end)
        return [cols, normed] + ends, gather(1, bias)

    def safe(bias):
        cols = exchange(4, n, safe_attention(start, bias, False), rows)
        ins, bias = end_inputs(cols)
        return exchange(5, n, safe_attention(ins, bias, True), rows)

    cols, good = fused_attention(2, n, start, bias, None)
    ins, end_bias = end_inputs(cols)
    out, flags = fused_attention(3, n, ins, end_bias, good)
    return lax.cond(jnp.min(flags[:, 0]) > 0.5, lambda b: out, safe, bias)


def solution(mesh):
    spec = P(("gx", "gy"), None, None)
    placed = (spec, P(("gx", "gy"))) + (P(),) * 14
    return jax.shard_map(local, mesh=mesh, in_specs=placed, out_specs=spec, check_vma=False)
```

```python
import functools
import types

import jax
import jax.numpy as jnp
from jax import lax
from jax.experimental import pallas as pl
from jax.experimental.pallas import tpu as pltpu
from jax.sharding import PartitionSpec as P

HEADS = 4
HEAD_DIM = 32
LOG2E = 1.4426950408889634
JB = 256
KB = 128
UNROLL = 4
F32 = jnp.float32
BF16 = jnp.bfloat16
NT = (((1,), (1,)), ((), ()))
TN = (((0,), (0,)), ((), ()))
VMEM = pl.BlockSpec(memory_space=pltpu.VMEM)


def layer_norm(t, gain):
    chan = t.shape[1]
    mean = jnp.dot(t, jnp.full((chan, chan), 1.0 / chan, BF16), preferred_element_type=F32)
    cent = t.astype(F32) - mean
    var = jnp.mean(cent * cent, axis=-1, keepdims=True)
    return (cent * lax.rsqrt(var + 1e-05) * gain).astype(BF16)


def bias_kernel(x_ref, g_ref, bw_ref, o_ref, a_ref):
    bwt = bw_ref[...].astype(F32).T.astype(BF16)
    gain = g_ref[...]
    for r in range(x_ref.shape[0]):
        a = layer_norm(x_ref[r], gain)
        a_ref[r] = a
        b = lax.dot_general(bwt, a, NT, preferred_element_type=F32) * LOG2E
        o_ref[:, r, :] = b[:HEADS].astype(BF16)


def pair_bias(x, gain, bias_w):
    rows, res, chan = x.shape
    bw = jnp.pad(bias_w, ((0, 0), (0, 128 - HEADS)))
    return pl.pallas_call(
        bias_kernel,
        out_shape=[
            jax.ShapeDtypeStruct((HEADS, rows, res), BF16),
            jax.ShapeDtypeStruct(x.shape, BF16),
        ],
        in_specs=[VMEM] * 3,
        out_specs=[VMEM] * 2,
    )(x, gain, bw)


ORDERS = (
    ("xyz", "yzx", "zxy", "xyz", "yzx"),
    ("yzx", "zxy", "xyz", "yzx", "xyz"),
)


def place():
    gx, gy = lax.axis_index("gx"), lax.axis_index("gy")
    return {
        "x": lax.rem(gx // 2, 4),
        "y": gy // 2,
        "z": 2 * lax.rem(gy, 2) + gx // 8,
        "c": lax.rem(gx, 2),
    }


def device(at):
    z_lo, z_hi = lax.rem(at["z"], 2), at["z"] // 2
    return {"gx": (z_lo * 4 + at["x"]) * 2 + at["c"], "gy": at["y"] * 2 + z_hi}


def shift(at, dim, by):
    return {**at, dim: lax.rem(at[dim] + by + 4, 4)}


def part(ref, lead, at, free, tail=()):
    z = "z" in free
    pick = lambda d: slice(None) if d in free else at[d]
    z_lo = slice(None) if z else lax.rem(at["z"], 2)
    z_hi = slice(None) if z else at["z"] // 2
    return ref.at[lead + (z_lo, pick("x"), at["c"], pick("y"), z_hi) + tail]


def gather_kernel(n_out, *refs):
    ins, outs = refs[:n_out], refs[n_out : 2 * n_out]
    ring_send, ring_recv, pair_send, pair_recv, own_sem = refs[2 * n_out :]
    me = place()
    barrier = pltpu.get_barrier_semaphore()
    sib = {**me, "c": 1 - me["c"]}
    partners = [shift(me, d, by) for d in "xyz" for by in (1, -1)] + [sib]
    for at in partners:
        pl.semaphore_signal(barrier, inc=1, device_id=device(at), device_id_type=pl.DeviceIdType.MESH)
    pl.semaphore_wait(barrier, len(partners))

    def items(core):
        half = outs[0].shape[-1] // 2
        got = []
        for h in range(HEADS):
            got.append((h, ins[0].at[h], functools.partial(part, outs[0], (h,)), half))
        if n_out == 2:
            got.append((HEADS, ins[1], functools.partial(part, outs[1], ()), 0))
        return got

    def copy(src, dst, sems, idx, to):
        return pltpu.make_async_remote_copy(
            src_ref=src, dst_ref=dst, send_sem=sems[0].at[idx], recv_sem=sems[1].at[idx],
            device_id=device(to), device_id_type=pl.DeviceIdType.MESH,
        )

    ring, pair = (ring_send, ring_recv), (pair_send, pair_recv)

    def run(core):
        at = {**me, "c": core}
        other = {**me, "c": 1 - core}
        todo = items(core)
        sends = []

        def step0(p, idx, own, sets, half):
            d, free = ORDERS[core][idx][p], ORDERS[core][idx][:p]
            src = sets(at, free)
            for k, by in enumerate((1, -1)):
                c = copy(own if p == 0 else src, src, ring, (idx, p, k), shift(at, d, by))
                c.start()
                sends.append(c)

        def step1(p, idx, own, sets, half):
            d, free = ORDERS[core][idx][p], ORDERS[core][idx][:p]
            for k, by in enumerate((1, -1)):
                got = sets(shift(at, d, -by), free)
                copy(got, got, ring, (idx, p, k), shift(at, d, by)).wait_recv()
                if half:
                    tail = (slice(None), pl.ds(k * half, half))
                    piece = sets(shift(at, d, -by), free, tail)
                elif k == 0:
                    piece = got
                else:
                    continue
                c = copy(piece, piece, ring, (idx, p, 2 + k), shift(at, d, by))
                c.start()
                sends.append(c)

        def step2(p, idx, own, sets, half):
            d, free = ORDERS[core][idx][p], ORDERS[core][idx][:p]
            for k, by in enumerate((1, -1)):
                if half:
                    tail = (slice(None), pl.ds(k * half, half))
                    piece = sets(shift(at, d, 2), free, tail)
                elif k == 0:
                    piece = sets(shift(at, d, 2), free)
                else:
                    continue
                copy(piece, piece, ring, (idx, p, 2 + k), shift(at, d, by)).wait_recv()

        def across(idx, sets, hop):
            d, free = ORDERS[core][idx][2], ORDERS[core][idx][:2]
            piece = sets(shift(at, d, hop), free)
            c = copy(piece, piece, pair, (idx, hop), other)
            c.start()
            sends.append(c)

        own_copies = []
        for idx, own, sets, half in todo:
            step0(0, idx, own, sets, half)
            mine = pltpu.make_async_copy(own, sets(at, ""), own_sem.at[idx])
            mine.start()
            own_copies.append(mine)
        for p in range(3):
            for t in todo:
                step1(p, *t)
                if p == 2:
                    for hop in (1, 3):
                        across(t[0], t[2], hop)
            for i, t in enumerate(todo):
                if p == 0:
                    own_copies[i].wait()
                step2(p, *t)
                if p < 2:
                    step0(p + 1, *t)
                if p == 1:
                    across(t[0], t[2], 0)
                if p == 2:
                    across(t[0], t[2], 2)
        for idx, own, sets, half in todo:
            d, free = ORDERS[1 - core][idx][2], ORDERS[1 - core][idx][:2]
            for hop in range(4):
                piece = sets(shift(other, d, hop), free)
                copy(piece, piece, pair, (idx, hop), other).wait_recv()
        for c in sends:
            c.wait_send()

    for core in range(2):
        pl.when(me["c"] == core)(functools.partial(run, core))


def gather(cid, bias, *mask):
    heads, rows, res = bias.shape
    grid = (2, 4, 2, 4, 2)
    outs = [jax.ShapeDtypeStruct((heads,) + grid + (rows, res), BF16)]
    if mask:
        outs.append(jax.ShapeDtypeStruct(grid + mask[0].shape, F32))
    n = len(outs)
    got = pl.pallas_call(
        functools.partial(gather_kernel, n),
        out_shape=outs,
        in_specs=[VMEM] * n,
        out_specs=[pl.BlockSpec(memory_space=pl.ANY)] * n,
        scratch_shapes=[
            pltpu.SemaphoreType.DMA((5, 3, 4)),
            pltpu.SemaphoreType.DMA((5, 3, 4)),
            pltpu.SemaphoreType.DMA((5, 4)),
            pltpu.SemaphoreType.DMA((5, 4)),
            pltpu.SemaphoreType.DMA((5,)),
        ],
        compiler_params=pltpu.CompilerParams(collective_id=cid, has_side_effects=True),
    )(bias, *mask)
    full = got[0].reshape(heads, -1, res)
    return (full, got[1].reshape((-1,) + mask[0].shape)) if mask else full


def stage_tools(trans, m):
    rows, res, chan = m.x.shape
    groups = rows // 4
    nk = res // KB
    tasks = groups * HEADS
    t = types.SimpleNamespace()

    def eye():
        i = lax.broadcasted_iota(jnp.int32, (KB, KB), 0)
        j = lax.broadcasted_iota(jnp.int32, (KB, KB), 1)
        return (i == j).astype(F32).astype(BF16)

    def project_all():
        w = m.w[...].astype(F32)
        wqt = w[:, :chan].T
        for s in range(4):
            cut = chan - 32 * s
            wk = w[:, chan : 2 * chan]
            m.wk[s] = (pltpu.roll(wk, 32 * s, 1) if s else wk).astype(BF16)
            m.wq[s] = (jnp.concatenate([wqt[cut:], wqt[:cut]], axis=0) if s else wqt).astype(BF16)
        wvt = w[:, 2 * chan : 3 * chan].T.astype(BF16)
        wgt = w[:, 3 * chan :].T.astype(BF16)
        gb = m.gb[...].T
        mrow = m.mrow[...]
        lane = lax.broadcasted_iota(jnp.int32, (1, chan), 1) // HEAD_DIM

        def project(r, carry):
            s = lax.rem(r, 4)
            grp = r // 4
            a = m.a[r]
            kk = jnp.dot(a, m.wk[s], preferred_element_type=F32).astype(BF16)
            aq = m.aq[r]
            qt = (
                lax.dot_general(m.wq[s], aq, NT, preferred_element_type=F32)
                * (HEAD_DIM**-0.5 * LOG2E)
            ).astype(BF16)
            vt = lax.dot_general(wvt, a, NT, preferred_element_type=F32) * mrow
            m.gt[r] = jax.nn.sigmoid(lax.dot_general(wgt, aq, NT, preferred_element_type=F32) + gb)
            for h in range(HEADS):
                slot = lax.rem(h + s, 4)
                m.km[r, h] = kk * (lane == slot).astype(F32).astype(BF16)
                m.vx[r, h, :HEAD_DIM] = vt[HEAD_DIM * h : HEAD_DIM * (h + 1)].astype(BF16)
                m.vx[r, h, HEAD_DIM:] = jnp.broadcast_to(mrow, (16, res)).astype(BF16)
            for u in range(4):
                hh = lax.rem(u - s + 4, 4)
                m.qs[grp, hh, pl.ds(32 * u, 32)] = qt[32 * u : 32 * (u + 1)]
            return carry

        lax.fori_loop(0, rows, project, 0)

    def turn_bias(b_ref):
        for h in range(HEADS):
            for kb in range(nk):
                sl = slice(KB * kb, KB * (kb + 1))
                m.bt[h, sl] = b_ref[h, :, sl].T

    def head_slice(h):
        return pl.ds(pl.multiple_of(HEAD_DIM * h, HEAD_DIM), HEAD_DIM)

    def fast_heads(joff):
        one = eye()

        def of(k):
            return k // HEADS, lax.rem(k, HEADS)

        def weights_step(k, kb, pp):
            grp, h = of(k)
            sl = slice(KB * kb, KB * (kb + 1))
            rhs = jnp.concatenate([m.bt[h, sl], m.qs[grp, h, :, pl.ds(joff, JB)]], axis=0)
            lhs = jnp.concatenate(
                [jnp.concatenate([one, m.km[grp * 4 + r, h, sl]], axis=1) for r in range(4)], axis=0
            )
            p4 = jnp.exp2(jnp.dot(lhs, rhs, preferred_element_type=F32)).astype(BF16)
            for r in range(4):
                pp[r, sl] = p4[KB * r : KB * (r + 1)]

        def mix_step(k, r, pp):
            grp, h = of(k)
            oe = jnp.dot(m.vx[grp * 4 + r, h], pp[r], preferred_element_type=F32)
            den = oe[HEAD_DIM : HEAD_DIM + 1]
            m.gd[...] = jnp.where((den > 2.0**-60) & (den < 2.0**100), m.gd[...], 0.0)
            m.ot[grp * 4 + r, head_slice(h)] = oe[:HEAD_DIM] / den

        def both(k, new, old):
            for kb in range(nk):
                weights_step(k, kb, new)
                if kb % 2:
                    mix_step(k - 1, kb // 2, old)

        for kb in range(nk):
            weights_step(0, kb, m.pa)

        def pair(i, carry):
            both(2 * i + 1, m.pb, m.pa)
            both(2 * i + 2, m.pa, m.pb)
            return carry

        lax.fori_loop(0, tasks // 2 - 1, pair, 0)
        both(tasks - 1, m.pb, m.pa)
        for r in range(4):
            mix_step(tasks - 1, r, m.pb)

    def safe_heads(joff):
        one = eye()

        def row_head(it, carry):
            row, h = it // HEADS, lax.rem(it, HEADS)
            q = m.qs[row // 4, h, :, pl.ds(joff, JB)]

            def scores(kb, carry):
                ks = pl.ds(pl.multiple_of(kb * KB, KB), KB)
                rhs = jnp.concatenate([m.bt[h, ks], q], axis=0)
                lhs = jnp.concatenate([one, m.km[row, h, ks]], axis=1)
                s1 = jnp.dot(lhs, rhs, preferred_element_type=F32)
                s1 = jnp.where(m.mcol[ks] > 0.5, s1, -1e30)
                m.ss[ks] = s1
                return jnp.maximum(carry, jnp.max(s1, axis=0, keepdims=True))

            top = lax.fori_loop(0, nk, scores, jnp.full((1, JB), -1e30, F32))

            def weights(kb, carry):
                ks = pl.ds(pl.multiple_of(kb * KB, KB), KB)
                m.pa[0, ks] = jnp.exp2(m.ss[ks] - top).astype(BF16)
                return carry

            lax.fori_loop(0, nk, weights, 0)
            oe = jnp.dot(m.vx[row, h], m.pa[0], preferred_element_type=F32)
            m.ot[row, head_slice(h)] = oe[:HEAD_DIM] / oe[HEAD_DIM : HEAD_DIM + 1]
            return carry

        lax.fori_loop(0, rows * HEADS, row_head, 0)

    def finish(joff, store):
        def row(r):
            gated = (m.ot[r] * m.gt[r, :, pl.ds(joff, JB)]).T.astype(BF16)
            z = m.x[r, pl.ds(joff, JB)].astype(F32) + jnp.dot(
                gated, m.ow[...], preferred_element_type=F32
            )
            z = z.astype(BF16)
            if trans:
                zf = z.astype(F32)
                a = layer_norm(z, m.ng[...])
                hid = jnp.dot(a, m.ti[...], preferred_element_type=F32) + m.tb[...]
                hid = jnp.maximum(hid, 0.0).astype(BF16)
                z = (zf + jnp.dot(hid, m.to[...], preferred_element_type=F32)).astype(BF16)
            m.zz[r] = z

        def some(i, carry):
            for r in range(UNROLL):
                row(UNROLL * i + r)
            return carry

        lax.fori_loop(0, rows // UNROLL, some, 0)
        span = JB // rows
        out_row = lax.broadcasted_iota(jnp.int32, (JB, JB), 0)
        in_row = lax.broadcasted_iota(jnp.int32, (JB, JB), 1)
        perm = (in_row == lax.rem(out_row, rows) * span + out_row // rows).astype(F32).astype(BF16)
        for q in range(rows // 2):
            cols = [
                jnp.concatenate([m.zz[r, span * n : span * (n + 1)] for r in range(rows)], axis=0)
                for n in (2 * q, 2 * q + 1)
            ]
            moved = jnp.dot(perm, jnp.concatenate(cols, axis=1), preferred_element_type=F32)
            for n in range(2):
                part = moved[:, chan * n : chan * (n + 1)]
                store(span * (2 * q + n), part.reshape(span, rows, chan).astype(BF16))

    return types.SimpleNamespace(
        project_all=project_all, turn_bias=turn_bias, fast_heads=fast_heads,
        safe_heads=safe_heads, finish=finish,
    )


def stage_names(trans):
    names = ["x", "a", "w", "gb", "ow", "mrow", "mcol"]
    return names + (["ng", "ti", "tb", "to"] if trans else [])


def stage_scratch(rows, res, chan):
    return {
        "km": pltpu.VMEM((rows, HEADS, res, chan), BF16),
        "qs": pltpu.VMEM((rows // 4, HEADS, chan, res), BF16),
        "vx": pltpu.VMEM((rows, HEADS, HEAD_DIM + 16, res), BF16),
        "gt": pltpu.VMEM((rows, chan, res), F32),
        "bt": pltpu.VMEM((HEADS, res, JB), BF16),
        "pa": pltpu.VMEM((4, res, JB), BF16),
        "pb": pltpu.VMEM((4, res, JB), BF16),
        "ot": pltpu.VMEM((rows, chan, JB), F32),
        "wk": pltpu.VMEM((4, chan, chan), BF16),
        "wq": pltpu.VMEM((4, chan, chan), BF16),
        "gd": pltpu.VMEM((1, JB), F32),
        "zz": pltpu.VMEM((rows, JB, chan), BF16),
        "bs": pltpu.VMEM((HEADS, JB, res), BF16),
        "ss": pltpu.VMEM((res, JB), F32),
    }


def safe_kernel(trans, names, *refs):
    m = types.SimpleNamespace(**dict(zip(names, refs)))
    m.aq = m.a
    tools = stage_tools(trans, m)

    @pl.when(pl.program_id(0) == 0)
    def _():
        tools.project_all()

    joff = pl.multiple_of(pl.program_id(0) * JB, JB)
    tools.turn_bias(m.b)
    tools.safe_heads(joff)

    def store(at, part):
        m.o[at : at + part.shape[0]] = part

    tools.finish(joff, store)


def safe_attention(ins, bias, trans):
    rows, res, chan = ins[0].shape
    scratch = stage_scratch(rows, res, chan)
    names = stage_names(trans) + ["b", "o"] + list(scratch)
    full = lambda a: pl.BlockSpec(a.shape, lambda j, n=a.ndim: (0,) * n)
    return pl.pallas_call(
        functools.partial(safe_kernel, trans, names),
        grid=(res // JB,),
        out_shape=jax.ShapeDtypeStruct((res, rows, chan), BF16),
        in_specs=[full(a) for a in ins] + [pl.BlockSpec((HEADS, JB, res), lambda j: (0, j, 0))],
        out_specs=pl.BlockSpec((JB, rows, chan), lambda j: (j, 0, 0)),
        scratch_shapes=list(scratch.values()),
        compiler_params=pltpu.CompilerParams(
            dimension_semantics=("arbitrary",), vmem_limit_bytes=60 * 1024 * 1024
        ),
    )(*ins, bias)


def fused_kernel(trans, n, names, *refs):
    m = types.SimpleNamespace(**dict(zip(names, refs)))
    tools = stage_tools(trans, m)
    rows, res, chan = m.x.shape
    nj = res // JB
    per = JB // rows
    gx, gy = lax.axis_index("gx"), lax.axis_index("gy")
    ny = n // 16
    me = gx * ny + gy
    at = lambda d: {"gx": d // ny, "gy": lax.rem(d, ny)}
    barrier = pltpu.get_barrier_semaphore()

    def greet(t, carry):
        pl.semaphore_signal(
            barrier, inc=1, device_id=at(lax.rem(me + t, n)), device_id_type=pl.DeviceIdType.MESH
        )
        return carry

    lax.fori_loop(1, n, greet, 0)

    def owner(c, i):
        x, z_lo, core = i // 8, lax.rem(i // 4, 2), lax.rem(i // 2, 2)
        y = lax.rem(c - x + 4, 4)
        return ((z_lo * 4 + x) * 2 + core) * ny + y * 2 + lax.rem(i, 2)

    def block_of(t):
        return lax.rem(t + lax.rem(gx // 2, 4), nj)

    def chunk(c, u):
        return pl.ds(pl.multiple_of(owner(c, 2 * u) * rows, 2 * rows), 2 * rows)

    def slot(c, u):
        return pl.ds(pl.multiple_of(c * JB + u * 2 * rows, 2 * rows), 2 * rows)

    def fetch(t):
        c = block_of(t)

        def one(u, carry):
            pltpu.make_async_copy(m.b.at[:, chunk(c, u)], m.bs.at[:, slot(0, u)], m.fetch_sem).start()
            return carry

        lax.fori_loop(0, per // 2, one, 0)

    def fetched():
        pltpu.make_async_copy(m.b.at[:, pl.ds(0, JB)], m.bs, m.fetch_sem).wait()

    def sort_rows(src, dst, sem):
        def one(k, carry):
            c, u = k // (per // 2), lax.rem(k, per // 2)
            pltpu.make_async_copy(src.at[:, chunk(c, u)], dst.at[:, slot(c, u)], sem).start()
            return carry

        lax.fori_loop(0, nj * per // 2, one, 0)

    def copy(t, i, frm):
        to = owner(block_of(t), i)
        ahead = lax.rem(to - me + n, n)
        return to, pltpu.make_async_remote_copy(
            src_ref=m.zs.at[lax.rem(t, 2), pl.ds(pl.multiple_of(i * rows, rows), rows)],
            dst_ref=m.o.at[:, pl.ds(pl.multiple_of(rows * frm, rows), rows)],
            send_sem=m.send_sem.at[ahead], recv_sem=m.recv_sem.at[ahead],
            device_id=at(to), device_id_type=pl.DeviceIdType.MESH,
        )

    def own(t, i):
        mine = pl.ds(pl.multiple_of(rows * me, rows), rows)
        return pltpu.make_async_copy(
            m.zs.at[lax.rem(t, 2), pl.ds(pl.multiple_of(i * rows, rows), rows)],
            m.o.at[:, mine], m.own_sem,
        )

    first = ((gx // 8) * 2 + lax.rem(gx, 2)) * ny + gy

    def send_block(t):
        def send(k, carry):
            i = lax.rem(k + first, per)
            to, c = copy(t, i, me)

            @pl.when(to != me)
            def _():
                c.start()

            @pl.when(to == me)
            def _():
                own(t, i).start()

            return carry

        lax.fori_loop(0, per, send, 0)

    def sent_block(t):
        def sent(k, carry):
            i = lax.rem(k + first, per)
            to, c = copy(t, i, me)

            @pl.when(to != me)
            def _():
                c.wait_send()

            @pl.when(to == me)
            def _():
                own(t, i).wait()

            return carry

        lax.fori_loop(0, per, sent, 0)

    sort_rows(m.ah, m.aq, m.sort_sem.at[0])
    sort_rows(m.xh, m.x, m.sort_sem.at[1])
    fetch(0)
    pltpu.make_async_copy(m.ah, m.aq, m.sort_sem.at[0]).wait()
    tools.project_all()
    pltpu.make_async_copy(m.xh, m.x, m.sort_sem.at[1]).wait()
    m.gd[...] = jnp.ones_like(m.gd)
    pl.semaphore_wait(barrier, n - 1)

    def block(t, carry):
        joff = pl.multiple_of(block_of(t) * JB, JB)
        fetched()
        tools.turn_bias(m.bs)

        @pl.when(t > 0)
        def _():
            send_block(t - 1)

        @pl.when(t < nj - 1)
        def _():
            fetch(t + 1)

        tools.fast_heads(joff)

        @pl.when(t > 1)
        def _():
            sent_block(t - 2)

        def store(at, part):
            m.zs[lax.rem(t, 2), at : at + part.shape[0]] = part

        tools.finish(joff, store)
        return carry

    lax.fori_loop(0, nj, block, 0)
    good = jnp.min(m.gd[...], axis=1, keepdims=True)
    if trans:
        m.good[...] = jnp.minimum(m.before[...], good)
    else:
        m.good[...] = jnp.broadcast_to(good, m.good.shape)
    send_block(nj - 1)
    if trans:
        def flag(t, carry):
            c = pltpu.make_async_remote_copy(
                src_ref=m.good.at[pl.ds(0, 1)], dst_ref=m.flags.at[me, pl.ds(0, 1)],
                send_sem=m.fsend.at[t], recv_sem=m.frecv.at[t],
                device_id=at(lax.rem(me + t, n)), device_id_type=pl.DeviceIdType.MESH,
            )
            c.start()
            return carry

        lax.fori_loop(1, n, flag, 0)
        mine = pltpu.make_async_copy(m.good, m.flags.at[me], m.fsend.at[0])
        mine.start()
        mine.wait()
    sent_block(nj - 2)
    sent_block(nj - 1)

    def land(t, carry):
        frm = lax.rem(me + n - t, n)
        pltpu.make_async_remote_copy(
            src_ref=m.zs.at[0, pl.ds(0, rows)],
            dst_ref=m.o.at[:, pl.ds(pl.multiple_of(rows * frm, rows), rows)],
            send_sem=m.send_sem.at[t], recv_sem=m.recv_sem.at[t],
            device_id=at(frm), device_id_type=pl.DeviceIdType.MESH,
        ).wait_recv()
        if trans:
            c = pltpu.make_async_remote_copy(
                src_ref=m.good.at[pl.ds(0, 1)], dst_ref=m.flags.at[frm, pl.ds(0, 1)],
                send_sem=m.fsend.at[t], recv_sem=m.frecv.at[t],
                device_id=at(frm), device_id_type=pl.DeviceIdType.MESH,
            )
            c.wait_recv()
            c.wait_send()
        return carry

    lax.fori_loop(1, n, land, 0)


def fused_attention(cid, n, ins, bias, before):
    trans = before is not None
    rows, res, chan = ins[0].shape
    scratch = stage_scratch(rows, res, chan)
    del scratch["ss"]
    scratch |= {
        "zs": pltpu.VMEM((2, JB, rows, chan), BF16),
        "send_sem": pltpu.SemaphoreType.DMA((n,)),
        "recv_sem": pltpu.SemaphoreType.DMA((n,)),
        "x": pltpu.VMEM((rows, res, chan), BF16),
        "aq": pltpu.VMEM((rows, res, chan), BF16),
        "sort_sem": pltpu.SemaphoreType.DMA((2,)),
        "fetch_sem": pltpu.SemaphoreType.DMA,
        "own_sem": pltpu.SemaphoreType.DMA,
    }
    anywhere = pl.BlockSpec(memory_space=pl.ANY)
    outs = {"o": jax.ShapeDtypeStruct((rows, res, chan), BF16)}
    out_specs = [anywhere]
    names = ["xh"] + stage_names(trans)[1:] + ["ah", "b"]
    args = list(ins) + [ins[1], bias]
    in_specs = [anywhere] + [VMEM] * (len(ins) - 1) + [anywhere] * 2
    if trans:
        names.append("before")
        args.append(before)
        in_specs.append(VMEM)
        outs["flags"] = jax.ShapeDtypeStruct((n, 8, 128), F32)
        out_specs.append(anywhere)
        scratch |= {
            "good": pltpu.VMEM((8, 128), F32),
            "fsend": pltpu.SemaphoreType.DMA((n,)),
            "frecv": pltpu.SemaphoreType.DMA((n,)),
        }
    else:
        outs["good"] = jax.ShapeDtypeStruct((8, 128), F32)
        out_specs.append(VMEM)
    return pl.pallas_call(
        functools.partial(fused_kernel, trans, n, names + list(outs) + list(scratch)),
        out_shape=list(outs.values()),
        in_specs=in_specs,
        out_specs=out_specs,
        scratch_shapes=list(scratch.values()),
        compiler_params=pltpu.CompilerParams(
            collective_id=cid, has_side_effects=True, vmem_limit_bytes=60 * 1024 * 1024
        ),
    )(*args)


def exchange_kernel(n, z_ref, o_ref, send_sem, recv_sem, own_sem):
    rows = o_ref.shape[0]
    gy = n // 16
    me = lax.axis_index("gx") * gy + lax.axis_index("gy")
    at = lambda d: {"gx": d // gy, "gy": lax.rem(d, gy)}
    barrier = pltpu.get_barrier_semaphore()

    def greet(t, carry):
        pl.semaphore_signal(
            barrier, inc=1, device_id=at(lax.rem(me + t, n)), device_id_type=pl.DeviceIdType.MESH
        )
        return carry

    lax.fori_loop(1, n, greet, 0)
    mine = pl.ds(pl.multiple_of(rows * me, rows), rows)
    own = pltpu.make_async_copy(z_ref.at[mine], o_ref.at[:, mine], own_sem)
    own.start()
    pl.semaphore_wait(barrier, n - 1)

    def copy(t, to, frm):
        return pltpu.make_async_remote_copy(
            src_ref=z_ref.at[pl.ds(pl.multiple_of(rows * to, rows), rows)],
            dst_ref=o_ref.at[:, pl.ds(pl.multiple_of(rows * frm, rows), rows)],
            send_sem=send_sem.at[t], recv_sem=recv_sem.at[t],
            device_id=at(to), device_id_type=pl.DeviceIdType.MESH,
        )

    def send(t, carry):
        copy(t, lax.rem(me + t, n), me).start()
        return carry

    lax.fori_loop(1, n, send, 0)
    own.wait()

    def land(t, carry):
        copy(t, lax.rem(me + t, n), lax.rem(me + n - t, n)).wait_recv()
        copy(t, lax.rem(me + t, n), me).wait_send()
        return carry

    lax.fori_loop(1, n, land, 0)


def exchange(cid, n, z, rows):
    res, _, chan = z.shape
    return pl.pallas_call(
        functools.partial(exchange_kernel, n),
        out_shape=jax.ShapeDtypeStruct((rows, res, chan), BF16),
        in_specs=[pl.BlockSpec(memory_space=pl.ANY)],
        out_specs=pl.BlockSpec(memory_space=pl.ANY),
        scratch_shapes=[
            pltpu.SemaphoreType.DMA((n,)),
            pltpu.SemaphoreType.DMA((n,)),
            pltpu.SemaphoreType.DMA,
        ],
        compiler_params=pltpu.CompilerParams(collective_id=cid, has_side_effects=True),
    )(z)


def local(
    pair_in,
    residue_mask,
    norm_start,
    proj_start,
    gate_bias_start,
    bias_w_start,
    out_w_start,
    norm_end,
    proj_end,
    gate_bias_end,
    bias_w_end,
    out_w_end,
    norm_trans,
    trans_in,
    trans_bias,
    trans_out,
):
    rows, res, chan = pair_in.shape
    n = lax.axis_size(("gx", "gy"))
    row = lambda v: v.reshape(1, -1)
    mine = jnp.pad(residue_mask.astype(F32).reshape(1, rows), ((0, 7), (0, 128 - rows)))
    bias, normed = pair_bias(pair_in, row(norm_start), bias_w_start)
    bias, mask = gather(0, bias, mine)
    mask = mask[:, 0, :rows].reshape(res)
    mask = jnp.where(jnp.max(mask) > 0.5, mask, 1.0)
    mrow, mcol = mask.reshape(1, res), mask.reshape(res, 1)
    start = [pair_in, normed, proj_start, row(gate_bias_start), out_w_start, mrow, mcol]
    ends = [proj_end, row(gate_bias_end), out_w_end, mrow, mcol]
    ends += [row(norm_trans), trans_in, row(trans_bias), trans_out]

    def end_inputs(cols):
        bias, normed = pair_bias(cols, row(norm_end), bias_w_end)
        return [cols, normed] + ends, gather(1, bias)

    def safe(bias):
        cols = exchange(4, n, safe_attention(start, bias, False), rows)
        ins, bias = end_inputs(cols)
        return exchange(5, n, safe_attention(ins, bias, True), rows)

    cols, good = fused_attention(2, n, start, bias, None)
    ins, end_bias = end_inputs(cols)
    out, flags = fused_attention(3, n, ins, end_bias, good)
    return lax.cond(jnp.min(flags[:, 0]) > 0.5, lambda b: out, safe, bias)


def solution(mesh):
    spec = P(("gx", "gy"), None, None)
    placed = (spec, P(("gx", "gy"))) + (P(),) * 14
    return jax.shard_map(local, mesh=mesh, in_specs=placed, out_specs=spec, check_vma=False)
```

```python
import functools
import types

import jax
import jax.numpy as jnp
from jax import lax
from jax.experimental import pallas as pl
from jax.experimental.pallas import tpu as pltpu
from jax.sharding import PartitionSpec as P

HEADS = 4
HEAD_DIM = 32
LOG2E = 1.4426950408889634
JB = 256
KB = 128
UNROLL = 4
F32 = jnp.float32
BF16 = jnp.bfloat16
NT = (((1,), (1,)), ((), ()))
TN = (((0,), (0,)), ((), ()))
VMEM = pl.BlockSpec(memory_space=pltpu.VMEM)


def layer_norm(t, gain):
    chan = t.shape[1]
    mean = jnp.dot(t, jnp.full((chan, chan), 1.0 / chan, BF16), preferred_element_type=F32)
    cent = t.astype(F32) - mean
    var = jnp.mean(cent * cent, axis=-1, keepdims=True)
    return (cent * lax.rsqrt(var + 1e-05) * gain).astype(BF16)


def bias_kernel(x_ref, g_ref, bw_ref, o_ref, a_ref):
    bwt = bw_ref[...].astype(F32).T.astype(BF16)
    gain = g_ref[...]
    for r in range(x_ref.shape[0]):
        a = layer_norm(x_ref[r], gain)
        a_ref[r] = a
        b = lax.dot_general(bwt, a, NT, preferred_element_type=F32) * LOG2E
        o_ref[:, r, :] = b[:HEADS].astype(BF16)


def pair_bias(x, gain, bias_w):
    rows, res, chan = x.shape
    bw = jnp.pad(bias_w, ((0, 0), (0, 128 - HEADS)))
    return pl.pallas_call(
        bias_kernel,
        out_shape=[
            jax.ShapeDtypeStruct((HEADS, rows, res), BF16),
            jax.ShapeDtypeStruct(x.shape, BF16),
        ],
        in_specs=[VMEM] * 3,
        out_specs=[VMEM] * 2,
    )(x, gain, bw)


ORDERS = (
    ("xyz", "yzx", "zxy", "xyz", "yzx"),
    ("yzx", "zxy", "xyz", "yzx", "xyz"),
)


def place():
    gx, gy = lax.axis_index("gx"), lax.axis_index("gy")
    return {
        "x": lax.rem(gx // 2, 4),
        "y": gy // 2,
        "z": 2 * lax.rem(gy, 2) + gx // 8,
        "c": lax.rem(gx, 2),
    }


def device(at):
    z_lo, z_hi = lax.rem(at["z"], 2), at["z"] // 2
    return {"gx": (z_lo * 4 + at["x"]) * 2 + at["c"], "gy": at["y"] * 2 + z_hi}


def shift(at, dim, by):
    return {**at, dim: lax.rem(at[dim] + by + 4, 4)}


def part(ref, lead, at, free, tail=()):
    z = "z" in free
    pick = lambda d: slice(None) if d in free else at[d]
    z_lo = slice(None) if z else lax.rem(at["z"], 2)
    z_hi = slice(None) if z else at["z"] // 2
    return ref.at[lead + (z_lo, pick("x"), at["c"], pick("y"), z_hi) + tail]


def gather_kernel(n_out, *refs):
    ins, outs, held = refs[:n_out], refs[n_out : 2 * n_out], refs[2 * n_out : 3 * n_out]
    ring_send, ring_recv, pair_send, pair_recv, own_sem, out_sem = refs[3 * n_out :]
    me = place()
    barrier = pltpu.get_barrier_semaphore()
    sib = {**me, "c": 1 - me["c"]}
    partners = [shift(me, d, by) for d in "xyz" for by in (1, -1)] + [sib]
    for at in partners:
        pl.semaphore_signal(barrier, inc=1, device_id=device(at), device_id_type=pl.DeviceIdType.MESH)

    todo = []
    for h in range(HEADS):
        todo.append((
            h, ins[0].at[h], functools.partial(part, held[0], (h,)),
            functools.partial(part, outs[0], (h,)), outs[0].shape[-1] // 2,
        ))
    if n_out == 2:
        todo.append((
            HEADS, ins[1], functools.partial(part, held[1], ()), functools.partial(part, outs[1], ()), 0
        ))

    def copy(src, dst, sems, idx, to):
        return pltpu.make_async_remote_copy(
            src_ref=src, dst_ref=dst, send_sem=sems[0].at[idx], recv_sem=sems[1].at[idx],
            device_id=device(to), device_id_type=pl.DeviceIdType.MESH,
        )

    ring, pair = (ring_send, ring_recv), (pair_send, pair_recv)

    def run(core):
        at = {**me, "c": core}
        other = {**me, "c": 1 - core}
        sends, writes = [], []

        def pieces(p, item):
            order = ORDERS[core][item[0]]
            if p == 2 and item[4]:
                return [(v, {order[0]: v}, order[1]) for v in range(4)]
            return [(0, {}, order[:p])]

        def step0(p, item):
            idx, own, sets, _, half = item
            d = ORDERS[core][idx][p]
            for v, fix, free in pieces(p, item):
                src = sets({**at, **fix}, free)
                for k, by in enumerate((1, -1)):
                    c = copy(own if p == 0 else src, src, ring, (idx, p, v, k), shift(at, d, by))
                    c.start()
                    sends.append(c)

        def step1(p, item, piece):
            idx, own, sets, _, half = item
            d = ORDERS[core][idx][p]
            v, fix, free = piece
            for k, by in enumerate((1, -1)):
                frm = {**shift(at, d, -by), **fix}
                got = sets(frm, free)
                copy(got, got, ring, (idx, p, v, k), shift(at, d, by)).wait_recv()
                if half:
                    got = sets(frm, free, (slice(None), pl.ds(k * half, half)))
                elif k == 1:
                    continue
                c = copy(got, got, ring, (idx, p, v, 2 + k), shift(at, d, by))
                c.start()
                sends.append(c)

        def step2(p, item, piece):
            idx, own, sets, _, half = item
            d = ORDERS[core][idx][p]
            v, fix, free = piece
            for k, by in enumerate((1, -1)):
                frm = {**shift(at, d, 2), **fix}
                if half:
                    got = sets(frm, free, (slice(None), pl.ds(k * half, half)))
                elif k == 0:
                    got = sets(frm, free)
                else:
                    continue
                copy(got, got, ring, (idx, p, v, 2 + k), shift(at, d, by)).wait_recv()

        def write(item, where, free, number):
            c = pltpu.make_async_copy(
                item[2](where, free), item[3](where, free), out_sem.at[item[0], number]
            )
            c.start()
            writes.append(c)

        def across(item, hop):
            idx, own, sets, _, half = item
            d, free = ORDERS[core][idx][2], ORDERS[core][idx][:2]
            where = shift(at, d, hop)
            c = copy(sets(where, free), sets(where, free), pair, (idx, hop), other)
            c.start()
            sends.append(c)
            write(item, where, free, hop)

        own_copies = []
        for item in todo:
            mine = pltpu.make_async_copy(item[1], item[3](at, ""), own_sem.at[item[0]])
            mine.start()
            own_copies.append(mine)
        pl.semaphore_wait(barrier, len(partners))
        for item in todo:
            step0(0, item)
        for item, mine in zip(todo, own_copies):
            mine.wait()
            back = pltpu.make_async_copy(item[3](at, ""), item[2](at, ""), own_sem.at[item[0]])
            back.start()
            own_copies[item[0]] = back
        for p in range(3):
            if p < 2:
                for item in todo:
                    step1(p, item, pieces(p, item)[0])
            else:
                for v in range(4):
                    for item in todo:
                        if v < len(pieces(p, item)):
                            step1(p, item, pieces(p, item)[v])
                for item in todo:
                    for hop in (1, 3):
                        across(item, hop)
            for item in todo:
                if p == 0:
                    own_copies[item[0]].wait()
                for piece in pieces(p, item):
                    step2(p, item, piece)
                if p < 2:
                    step0(p + 1, item)
                if p == 1:
                    across(item, 0)
                if p == 2:
                    across(item, 2)
        for hop in (0, 1, 3, 2):
            for item in todo:
                idx, own, sets, _, half = item
                d, free = ORDERS[1 - core][idx][2], ORDERS[1 - core][idx][:2]
                where = shift(other, d, hop)
                copy(sets(where, free), sets(where, free), pair, (idx, hop), other).wait_recv()
                write(item, where, free, 4 + hop)
        for c in sends:
            c.wait_send()
        for c in writes:
            c.wait()

    for core in range(2):
        pl.when(me["c"] == core)(functools.partial(run, core))


def gather(cid, bias, *mask):
    heads, rows, res = bias.shape
    grid = (2, 4, 2, 4, 2)
    outs = [jax.ShapeDtypeStruct((heads,) + grid + (rows, res), BF16)]
    if mask:
        outs.append(jax.ShapeDtypeStruct(grid + mask[0].shape, F32))
    n = len(outs)
    got = pl.pallas_call(
        functools.partial(gather_kernel, n),
        out_shape=outs,
        in_specs=[VMEM] * n,
        out_specs=[pl.BlockSpec(memory_space=pl.ANY)] * n,
        scratch_shapes=[pltpu.VMEM(o.shape, o.dtype) for o in outs]
        + [
            pltpu.SemaphoreType.DMA((5, 3, 4, 4)),
            pltpu.SemaphoreType.DMA((5, 3, 4, 4)),
            pltpu.SemaphoreType.DMA((5, 4)),
            pltpu.SemaphoreType.DMA((5, 4)),
            pltpu.SemaphoreType.DMA((5,)),
            pltpu.SemaphoreType.DMA((5, 8)),
        ],
        compiler_params=pltpu.CompilerParams(
            collective_id=cid, has_side_effects=True, vmem_limit_bytes=60 * 1024 * 1024
        ),
    )(bias, *mask)
    full = got[0].reshape(heads, -1, res)
    return (full, got[1].reshape((-1,) + mask[0].shape)) if mask else full


def stage_tools(trans, m):
    rows, res, chan = m.x.shape
    groups = rows // 4
    nk = res // KB
    tasks = groups * HEADS
    t = types.SimpleNamespace()

    def eye():
        i = lax.broadcasted_iota(jnp.int32, (KB, KB), 0)
        j = lax.broadcasted_iota(jnp.int32, (KB, KB), 1)
        return (i == j).astype(F32).astype(BF16)

    def project_all():
        w = m.w[...].astype(F32)
        wqt = w[:, :chan].T
        for s in range(4):
            cut = chan - 32 * s
            wk = w[:, chan : 2 * chan]
            m.wk[s] = (pltpu.roll(wk, 32 * s, 1) if s else wk).astype(BF16)
            m.wq[s] = (jnp.concatenate([wqt[cut:], wqt[:cut]], axis=0) if s else wqt).astype(BF16)
        wvt = w[:, 2 * chan : 3 * chan].T.astype(BF16)
        wgt = w[:, 3 * chan :].T.astype(BF16)
        gb = m.gb[...].T
        mrow = m.mrow[...]
        lane = lax.broadcasted_iota(jnp.int32, (1, chan), 1) // HEAD_DIM

        def project(r, carry):
            s = lax.rem(r, 4)
            grp = r // 4
            a = m.a[r]
            kk = jnp.dot(a, m.wk[s], preferred_element_type=F32).astype(BF16)
            qt = (
                lax.dot_general(m.wq[s], a, NT, preferred_element_type=F32)
                * (HEAD_DIM**-0.5 * LOG2E)
            ).astype(BF16)
            vt = lax.dot_general(wvt, a, NT, preferred_element_type=F32) * mrow
            m.gt[r] = jax.nn.sigmoid(lax.dot_general(wgt, a, NT, preferred_element_type=F32) + gb)
            for h in range(HEADS):
                slot = lax.rem(h + s, 4)
                m.km[r, h] = kk * (lane == slot).astype(F32).astype(BF16)
                m.vx[r, h, :HEAD_DIM] = vt[HEAD_DIM * h : HEAD_DIM * (h + 1)].astype(BF16)
                m.vx[r, h, HEAD_DIM:] = jnp.broadcast_to(mrow, (16, res)).astype(BF16)
            for u in range(4):
                hh = lax.rem(u - s + 4, 4)
                m.qs[grp, hh, pl.ds(32 * u, 32)] = qt[32 * u : 32 * (u + 1)]
            return carry

        lax.fori_loop(0, rows, project, 0)

    def turn_bias(b_ref):
        for h in range(HEADS):
            for kb in range(nk):
                sl = slice(KB * kb, KB * (kb + 1))
                m.bt[h, sl] = b_ref[h, :, sl].T

    def head_slice(h):
        return pl.ds(pl.multiple_of(HEAD_DIM * h, HEAD_DIM), HEAD_DIM)

    def fast_heads(joff):
        one = eye()

        def of(k):
            return k // HEADS, lax.rem(k, HEADS)

        def weights_step(k, kb, pp):
            grp, h = of(k)
            sl = slice(KB * kb, KB * (kb + 1))
            rhs = jnp.concatenate([m.bt[h, sl], m.qs[grp, h, :, pl.ds(joff, JB)]], axis=0)
            lhs = jnp.concatenate(
                [jnp.concatenate([one, m.km[grp * 4 + r, h, sl]], axis=1) for r in range(4)], axis=0
            )
            p4 = jnp.exp2(jnp.dot(lhs, rhs, preferred_element_type=F32)).astype(BF16)
            for r in range(4):
                pp[r, sl] = p4[KB * r : KB * (r + 1)]

        def mix_step(k, r, pp):
            grp, h = of(k)
            oe = jnp.dot(m.vx[grp * 4 + r, h], pp[r], preferred_element_type=F32)
            den = oe[HEAD_DIM : HEAD_DIM + 1]
            m.gd[...] = jnp.where((den > 2.0**-60) & (den < 2.0**100), m.gd[...], 0.0)
            m.ot[grp * 4 + r, head_slice(h)] = oe[:HEAD_DIM] / den

        def both(k, new, old):
            for kb in range(nk):
                weights_step(k, kb, new)
                if kb % 2:
                    mix_step(k - 1, kb // 2, old)

        for kb in range(nk):
            weights_step(0, kb, m.pa)

        def pair(i, carry):
            both(2 * i + 1, m.pb, m.pa)
            both(2 * i + 2, m.pa, m.pb)
            return carry

        lax.fori_loop(0, tasks // 2 - 1, pair, 0)
        both(tasks - 1, m.pb, m.pa)
        for r in range(4):
            mix_step(tasks - 1, r, m.pb)

    def safe_heads(joff):
        one = eye()

        def row_head(it, carry):
            row, h = it // HEADS, lax.rem(it, HEADS)
            q = m.qs[row // 4, h, :, pl.ds(joff, JB)]

            def scores(kb, carry):
                ks = pl.ds(pl.multiple_of(kb * KB, KB), KB)
                rhs = jnp.concatenate([m.bt[h, ks], q], axis=0)
                lhs = jnp.concatenate([one, m.km[row, h, ks]], axis=1)
                s1 = jnp.dot(lhs, rhs, preferred_element_type=F32)
                s1 = jnp.where(m.mcol[ks] > 0.5, s1, -1e30)
                m.ss[ks] = s1
                return jnp.maximum(carry, jnp.max(s1, axis=0, keepdims=True))

            top = lax.fori_loop(0, nk, scores, jnp.full((1, JB), -1e30, F32))

            def weights(kb, carry):
                ks = pl.ds(pl.multiple_of(kb * KB, KB), KB)
                m.pa[0, ks] = jnp.exp2(m.ss[ks] - top).astype(BF16)
                return carry

            lax.fori_loop(0, nk, weights, 0)
            oe = jnp.dot(m.vx[row, h], m.pa[0], preferred_element_type=F32)
            m.ot[row, head_slice(h)] = oe[:HEAD_DIM] / oe[HEAD_DIM : HEAD_DIM + 1]
            return carry

        lax.fori_loop(0, rows * HEADS, row_head, 0)

    def finish(joff, store):
        def row(r):
            gated = (m.ot[r] * m.gt[r, :, pl.ds(joff, JB)]).T.astype(BF16)
            z = m.x[r, pl.ds(joff, JB)].astype(F32) + jnp.dot(
                gated, m.ow[...], preferred_element_type=F32
            )
            z = z.astype(BF16)
            if trans:
                zf = z.astype(F32)
                a = layer_norm(z, m.ng[...])
                hid = jnp.dot(a, m.ti[...], preferred_element_type=F32) + m.tb[...]
                hid = jnp.maximum(hid, 0.0).astype(BF16)
                z = (zf + jnp.dot(hid, m.to[...], preferred_element_type=F32)).astype(BF16)
            m.zz[r] = z

        def some(i, carry):
            for r in range(UNROLL):
                row(UNROLL * i + r)
            return carry

        lax.fori_loop(0, rows // UNROLL, some, 0)
        span = JB // rows
        out_row = lax.broadcasted_iota(jnp.int32, (JB, JB), 0)
        in_row = lax.broadcasted_iota(jnp.int32, (JB, JB), 1)
        perm = (in_row == lax.rem(out_row, rows) * span + out_row // rows).astype(F32).astype(BF16)
        for q in range(rows // 2):
            cols = [
                jnp.concatenate([m.zz[r, span * n : span * (n + 1)] for r in range(rows)], axis=0)
                for n in (2 * q, 2 * q + 1)
            ]
            moved = jnp.dot(perm, jnp.concatenate(cols, axis=1), preferred_element_type=F32)
            for n in range(2):
                part = moved[:, chan * n : chan * (n + 1)]
                store(span * (2 * q + n), part.reshape(span, rows, chan).astype(BF16))

    return types.SimpleNamespace(
        project_all=project_all, turn_bias=turn_bias, fast_heads=fast_heads,
        safe_heads=safe_heads, finish=finish,
    )


def stage_names(trans):
    names = ["x", "a", "w", "gb", "ow", "mrow", "mcol"]
    return names + (["ng", "ti", "tb", "to"] if trans else [])


def stage_scratch(rows, res, chan):
    return {
        "km": pltpu.VMEM((rows, HEADS, res, chan), BF16),
        "qs": pltpu.VMEM((rows // 4, HEADS, chan, res), BF16),
        "vx": pltpu.VMEM((rows, HEADS, HEAD_DIM + 16, res), BF16),
        "gt": pltpu.VMEM((rows, chan, res), F32),
        "bt": pltpu.VMEM((HEADS, res, JB), BF16),
        "pa": pltpu.VMEM((4, res, JB), BF16),
        "pb": pltpu.VMEM((4, res, JB), BF16),
        "ot": pltpu.VMEM((rows, chan, JB), F32),
        "wk": pltpu.VMEM((4, chan, chan), BF16),
        "wq": pltpu.VMEM((4, chan, chan), BF16),
        "gd": pltpu.VMEM((1, JB), F32),
        "zz": pltpu.VMEM((rows, JB, chan), BF16),
        "bs": pltpu.VMEM((HEADS, JB, res), BF16),
        "ss": pltpu.VMEM((res, JB), F32),
    }


def safe_kernel(trans, names, *refs):
    m = types.SimpleNamespace(**dict(zip(names, refs)))
    tools = stage_tools(trans, m)

    @pl.when(pl.program_id(0) == 0)
    def _():
        tools.project_all()

    joff = pl.multiple_of(pl.program_id(0) * JB, JB)
    tools.turn_bias(m.b)
    tools.safe_heads(joff)

    def store(at, part):
        m.o[at : at + part.shape[0]] = part

    tools.finish(joff, store)


def safe_attention(ins, bias, trans):
    rows, res, chan = ins[0].shape
    scratch = stage_scratch(rows, res, chan)
    names = stage_names(trans) + ["b", "o"] + list(scratch)
    full = lambda a: pl.BlockSpec(a.shape, lambda j, n=a.ndim: (0,) * n)
    return pl.pallas_call(
        functools.partial(safe_kernel, trans, names),
        grid=(res // JB,),
        out_shape=jax.ShapeDtypeStruct((res, rows, chan), BF16),
        in_specs=[full(a) for a in ins] + [pl.BlockSpec((HEADS, JB, res), lambda j: (0, j, 0))],
        out_specs=pl.BlockSpec((JB, rows, chan), lambda j: (j, 0, 0)),
        scratch_shapes=list(scratch.values()),
        compiler_params=pltpu.CompilerParams(
            dimension_semantics=("arbitrary",), vmem_limit_bytes=60 * 1024 * 1024
        ),
    )(*ins, bias)


def fused_kernel(trans, n, names, *refs):
    m = types.SimpleNamespace(**dict(zip(names, refs)))
    tools = stage_tools(trans, m)
    rows, res, chan = m.x.shape
    nj = res // JB
    per = JB // rows
    gy = n // 16
    me = lax.axis_index("gx") * gy + lax.axis_index("gy")
    at = lambda d: {"gx": d // gy, "gy": lax.rem(d, gy)}
    barrier = pltpu.get_barrier_semaphore()

    def greet(t, carry):
        pl.semaphore_signal(
            barrier, inc=1, device_id=at(lax.rem(me + t, n)), device_id_type=pl.DeviceIdType.MESH
        )
        return carry

    lax.fori_loop(1, n, greet, 0)

    def block_of(t):
        return lax.rem(t + me, nj)

    def fetch(t):
        return pltpu.make_async_copy(
            m.b.at[:, pl.ds(pl.multiple_of(block_of(t) * JB, JB), JB)], m.bs, m.fetch_sem
        )

    def copy(t, i, frm):
        to = block_of(t) * per + i
        ahead = lax.rem(to - me + n, n)
        return to, pltpu.make_async_remote_copy(
            src_ref=m.zs.at[lax.rem(t, 2), pl.ds(pl.multiple_of(i * rows, rows), rows)],
            dst_ref=m.o.at[:, pl.ds(pl.multiple_of(rows * frm, rows), rows)],
            send_sem=m.send_sem.at[ahead], recv_sem=m.recv_sem.at[ahead],
            device_id=at(to), device_id_type=pl.DeviceIdType.MESH,
        )

    def own(t, i):
        mine = pl.ds(pl.multiple_of(rows * me, rows), rows)
        return pltpu.make_async_copy(
            m.zs.at[lax.rem(t, 2), pl.ds(pl.multiple_of(i * rows, rows), rows)],
            m.o.at[:, mine], m.own_sem,
        )

    def send_block(t):
        def send(k, carry):
            i = lax.rem(k + me // nj, per)
            to, c = copy(t, i, me)

            @pl.when(to != me)
            def _():
                c.start()

            @pl.when(to == me)
            def _():
                own(t, i).start()

            return carry

        lax.fori_loop(0, per, send, 0)

    def sent_block(t):
        def sent(k, carry):
            i = lax.rem(k + me // nj, per)
            to, c = copy(t, i, me)

            @pl.when(to != me)
            def _():
                c.wait_send()

            @pl.when(to == me)
            def _():
                own(t, i).wait()

            return carry

        lax.fori_loop(0, per, sent, 0)

    fetch(0).start()
    tools.project_all()
    m.gd[...] = jnp.ones_like(m.gd)
    pl.semaphore_wait(barrier, n - 1)

    def block(t, carry):
        joff = pl.multiple_of(block_of(t) * JB, JB)
        fetch(t).wait()
        tools.turn_bias(m.bs)

        @pl.when(t > 0)
        def _():
            send_block(t - 1)

        @pl.when(t < nj - 1)
        def _():
            fetch(t + 1).start()

        tools.fast_heads(joff)

        @pl.when(t > 1)
        def _():
            sent_block(t - 2)

        def store(at, part):
            m.zs[lax.rem(t, 2), at : at + part.shape[0]] = part

        tools.finish(joff, store)
        return carry

    lax.fori_loop(0, nj, block, 0)
    good = jnp.min(m.gd[...], axis=1, keepdims=True)
    if trans:
        m.good[...] = jnp.minimum(m.before[...], good)
    else:
        m.good[...] = jnp.broadcast_to(good, m.good.shape)
    send_block(nj - 1)
    if trans:
        def flag(t, carry):
            c = pltpu.make_async_remote_copy(
                src_ref=m.good.at[pl.ds(0, 1)], dst_ref=m.flags.at[me, pl.ds(0, 1)],
                send_sem=m.fsend.at[t], recv_sem=m.frecv.at[t],
                device_id=at(lax.rem(me + t, n)), device_id_type=pl.DeviceIdType.MESH,
            )
            c.start()
            return carry

        lax.fori_loop(1, n, flag, 0)
        mine = pltpu.make_async_copy(m.good, m.flags.at[me], m.fsend.at[0])
        mine.start()
        mine.wait()
    sent_block(nj - 2)
    sent_block(nj - 1)

    def land(t, carry):
        frm = lax.rem(me + n - t, n)
        pltpu.make_async_remote_copy(
            src_ref=m.zs.at[0, pl.ds(0, rows)],
            dst_ref=m.o.at[:, pl.ds(pl.multiple_of(rows * frm, rows), rows)],
            send_sem=m.send_sem.at[t], recv_sem=m.recv_sem.at[t],
            device_id=at(frm), device_id_type=pl.DeviceIdType.MESH,
        ).wait_recv()
        if trans:
            c = pltpu.make_async_remote_copy(
                src_ref=m.good.at[pl.ds(0, 1)], dst_ref=m.flags.at[frm, pl.ds(0, 1)],
                send_sem=m.fsend.at[t], recv_sem=m.frecv.at[t],
                device_id=at(frm), device_id_type=pl.DeviceIdType.MESH,
            )
            c.wait_recv()
            c.wait_send()
        return carry

    lax.fori_loop(1, n, land, 0)


def fused_attention(cid, n, ins, bias, before):
    trans = before is not None
    rows, res, chan = ins[0].shape
    scratch = stage_scratch(rows, res, chan)
    del scratch["ss"]
    scratch |= {
        "zs": pltpu.VMEM((2, JB, rows, chan), BF16),
        "send_sem": pltpu.SemaphoreType.DMA((n,)),
        "recv_sem": pltpu.SemaphoreType.DMA((n,)),
        "fetch_sem": pltpu.SemaphoreType.DMA,
        "own_sem": pltpu.SemaphoreType.DMA,
    }
    anywhere = pl.BlockSpec(memory_space=pl.ANY)
    outs = {"o": jax.ShapeDtypeStruct((rows, res, chan), BF16)}
    out_specs = [anywhere]
    names = stage_names(trans) + ["b"]
    args = list(ins) + [bias]
    in_specs = [VMEM] * len(ins) + [anywhere]
    if trans:
        names.append("before")
        args.append(before)
        in_specs.append(VMEM)
        outs["flags"] = jax.ShapeDtypeStruct((n, 8, 128), F32)
        out_specs.append(anywhere)
        scratch |= {
            "good": pltpu.VMEM((8, 128), F32),
            "fsend": pltpu.SemaphoreType.DMA((n,)),
            "frecv": pltpu.SemaphoreType.DMA((n,)),
        }
    else:
        outs["good"] = jax.ShapeDtypeStruct((8, 128), F32)
        out_specs.append(VMEM)
    return pl.pallas_call(
        functools.partial(fused_kernel, trans, n, names + list(outs) + list(scratch)),
        out_shape=list(outs.values()),
        in_specs=in_specs,
        out_specs=out_specs,
        scratch_shapes=list(scratch.values()),
        compiler_params=pltpu.CompilerParams(
            collective_id=cid, has_side_effects=True, vmem_limit_bytes=60 * 1024 * 1024
        ),
    )(*args)


def exchange_kernel(n, whole, z_ref, o_ref, send_sem, recv_sem, own_sem):
    rows = z_ref.shape[1]
    cut = lambda d: z_ref if whole else z_ref.at[pl.ds(pl.multiple_of(rows * d, rows), rows)]
    gy = n // 16
    me = lax.axis_index("gx") * gy + lax.axis_index("gy")
    at = lambda d: {"gx": d // gy, "gy": lax.rem(d, gy)}
    barrier = pltpu.get_barrier_semaphore()

    def greet(t, carry):
        pl.semaphore_signal(
            barrier, inc=1, device_id=at(lax.rem(me + t, n)), device_id_type=pl.DeviceIdType.MESH
        )
        return carry

    lax.fori_loop(1, n, greet, 0)
    mine = pl.ds(pl.multiple_of(rows * me, rows), rows)
    own = pltpu.make_async_copy(cut(me), o_ref.at[:, mine], own_sem)
    own.start()
    pl.semaphore_wait(barrier, n - 1)

    def copy(t, to, frm):
        return pltpu.make_async_remote_copy(
            src_ref=cut(to),
            dst_ref=o_ref.at[:, pl.ds(pl.multiple_of(rows * frm, rows), rows)],
            send_sem=send_sem.at[t], recv_sem=recv_sem.at[t],
            device_id=at(to), device_id_type=pl.DeviceIdType.MESH,
        )

    def send(t, carry):
        copy(t, lax.rem(me + t, n), me).start()
        return carry

    lax.fori_loop(1, n, send, 0)
    own.wait()

    def land(t, carry):
        copy(t, lax.rem(me + t, n), lax.rem(me + n - t, n)).wait_recv()
        copy(t, lax.rem(me + t, n), me).wait_send()
        return carry

    lax.fori_loop(1, n, land, 0)


def exchange(cid, n, z, whole=False):
    lead, rows, width = z.shape
    shape = (lead, n * rows, width) if whole else (rows, lead, width)
    return pl.pallas_call(
        functools.partial(exchange_kernel, n, whole),
        out_shape=jax.ShapeDtypeStruct(shape, BF16),
        in_specs=[pl.BlockSpec(memory_space=pl.ANY)],
        out_specs=pl.BlockSpec(memory_space=pl.ANY),
        scratch_shapes=[
            pltpu.SemaphoreType.DMA((n,)),
            pltpu.SemaphoreType.DMA((n,)),
            pltpu.SemaphoreType.DMA,
        ],
        compiler_params=pltpu.CompilerParams(collective_id=cid, has_side_effects=True),
    )(z)


def local(
    pair_in,
    residue_mask,
    norm_start,
    proj_start,
    gate_bias_start,
    bias_w_start,
    out_w_start,
    norm_end,
    proj_end,
    gate_bias_end,
    bias_w_end,
    out_w_end,
    norm_trans,
    trans_in,
    trans_bias,
    trans_out,
):
    rows, res, chan = pair_in.shape
    n = lax.axis_size(("gx", "gy"))
    row = lambda v: v.reshape(1, -1)
    mine = jnp.pad(residue_mask.astype(F32).reshape(1, rows), ((0, 7), (0, 128 - rows)))
    bias, normed = pair_bias(pair_in, row(norm_start), bias_w_start)
    bias, mask = gather(0, bias, mine)
    mask = mask[:, 0, :rows].reshape(res)
    mask = jnp.where(jnp.max(mask) > 0.5, mask, 1.0)
    mrow, mcol = mask.reshape(1, res), mask.reshape(res, 1)
    start = [pair_in, normed, proj_start, row(gate_bias_start), out_w_start, mrow, mcol]
    ends = [proj_end, row(gate_bias_end), out_w_end, mrow, mcol]
    ends += [row(norm_trans), trans_in, row(trans_bias), trans_out]

    def end_inputs(cols):
        bias, normed = pair_bias(cols, row(norm_end), bias_w_end)
        return [cols, normed] + ends, bias

    def safe(bias):
        cols = exchange(4, n, safe_attention(start, bias, False))
        ins, bias = end_inputs(cols)
        return exchange(5, n, safe_attention(ins, exchange(6, n, bias, True), True))

    cols, good = fused_attention(2, n, start, bias, None)
    ins, end_bias = end_inputs(cols)
    out, flags = fused_attention(3, n, ins, gather(1, end_bias), good)
    return lax.cond(jnp.min(flags[:, 0]) > 0.5, lambda b: out, safe, bias)


def solution(mesh):
    spec = P(("gx", "gy"), None, None)
    placed = (spec, P(("gx", "gy"))) + (P(),) * 14
    return jax.shard_map(local, mesh=mesh, in_specs=placed, out_specs=spec, check_vma=False)
```

```python
import functools
import types

import jax
import jax.numpy as jnp
from jax import lax
from jax.experimental import pallas as pl
from jax.experimental.pallas import tpu as pltpu
from jax.sharding import PartitionSpec as P

HEADS = 4
HEAD_DIM = 32
LOG2E = 1.4426950408889634
JB = 256
KB = 128
UNROLL = 4
F32 = jnp.float32
BF16 = jnp.bfloat16
NT = (((1,), (1,)), ((), ()))
TN = (((0,), (0,)), ((), ()))
VMEM = pl.BlockSpec(memory_space=pltpu.VMEM)


def layer_norm(t, gain):
    chan = t.shape[1]
    mean = jnp.dot(t, jnp.full((chan, chan), 1.0 / chan, BF16), preferred_element_type=F32)
    cent = t.astype(F32) - mean
    var = jnp.mean(cent * cent, axis=-1, keepdims=True)
    return (cent * lax.rsqrt(var + 1e-05) * gain).astype(BF16)


def owner(c, i):
    x, z_lo, core, z_hi = i // 8, (i // 4) % 2, (i // 2) % 2, i % 2
    y = (c - x + 4) % 4
    return ((z_lo * 4 + x) * 2 + core) * 8 + y * 2 + z_hi


def bias_kernel(x_ref, g_ref, bw_ref, o_ref, a_ref, xq_ref, aq_ref):
    bwt = bw_ref[...].astype(F32).T.astype(BF16)
    gain = g_ref[...]
    for r in range(x_ref.shape[0]):
        a = layer_norm(x_ref[r], gain)
        a_ref[r] = a
        for p in range(x_ref.shape[1] // 16):
            at = owner(p // 16, 2 * (p % 16)) * 8
            aq_ref[r, 16 * p : 16 * p + 16] = a[at : at + 16]
            xq_ref[r, 16 * p : 16 * p + 16] = x_ref[r, at : at + 16]
        b = lax.dot_general(bwt, a, NT, preferred_element_type=F32) * LOG2E
        o_ref[:, r, :] = b[:HEADS].astype(BF16)


def pair_bias(x, gain, bias_w):
    rows, res, chan = x.shape
    bw = jnp.pad(bias_w, ((0, 0), (0, 128 - HEADS)))
    return pl.pallas_call(
        bias_kernel,
        out_shape=[
            jax.ShapeDtypeStruct((HEADS, rows, res), BF16),
            jax.ShapeDtypeStruct(x.shape, BF16),
            jax.ShapeDtypeStruct(x.shape, BF16),
            jax.ShapeDtypeStruct(x.shape, BF16),
        ],
        in_specs=[VMEM] * 3,
        out_specs=[VMEM] * 4,
    )(x, gain, bw)


ORDERS = (
    ("xyz", "yzx", "zxy", "xyz", "yzx"),
    ("yzx", "zxy", "xyz", "yzx", "xyz"),
)


def place():
    gx, gy = lax.axis_index("gx"), lax.axis_index("gy")
    return {
        "x": lax.rem(gx // 2, 4),
        "y": gy // 2,
        "z": 2 * lax.rem(gy, 2) + gx // 8,
        "c": lax.rem(gx, 2),
    }


def device(at):
    z_lo, z_hi = lax.rem(at["z"], 2), at["z"] // 2
    return {"gx": (z_lo * 4 + at["x"]) * 2 + at["c"], "gy": at["y"] * 2 + z_hi}


def shift(at, dim, by):
    return {**at, dim: lax.rem(at[dim] + by + 4, 4)}


def part(ref, lead, at, free, tail=()):
    z = "z" in free
    pick = lambda d: slice(None) if d in free else at[d]
    z_lo = slice(None) if z else lax.rem(at["z"], 2)
    z_hi = slice(None) if z else at["z"] // 2
    return ref.at[lead + (z_lo, pick("x"), at["c"], pick("y"), z_hi) + tail]


def gather_kernel(n_out, *refs):
    ins, outs = refs[:n_out], refs[n_out : 2 * n_out]
    ring_send, ring_recv, pair_send, pair_recv, own_sem = refs[2 * n_out :]
    me = place()
    barrier = pltpu.get_barrier_semaphore()
    sib = {**me, "c": 1 - me["c"]}
    partners = [shift(me, d, by) for d in "xyz" for by in (1, -1)] + [sib]
    for at in partners:
        pl.semaphore_signal(barrier, inc=1, device_id=device(at), device_id_type=pl.DeviceIdType.MESH)
    pl.semaphore_wait(barrier, len(partners))

    def items(core):
        half = outs[0].shape[-1] // 2
        got = []
        for h in range(HEADS):
            got.append((h, ins[0].at[h], functools.partial(part, outs[0], (h,)), half))
        if n_out == 2:
            got.append((HEADS, ins[1], functools.partial(part, outs[1], ()), 0))
        return got

    def copy(src, dst, sems, idx, to):
        return pltpu.make_async_remote_copy(
            src_ref=src, dst_ref=dst, send_sem=sems[0].at[idx], recv_sem=sems[1].at[idx],
            device_id=device(to), device_id_type=pl.DeviceIdType.MESH,
        )

    ring, pair = (ring_send, ring_recv), (pair_send, pair_recv)

    def run(core):
        at = {**me, "c": core}
        other = {**me, "c": 1 - core}
        todo = items(core)
        sends = []

        def step0(p, idx, own, sets, half):
            d, free = ORDERS[core][idx][p], ORDERS[core][idx][:p]
            src = sets(at, free)
            for k, by in enumerate((1, -1)):
                c = copy(own if p == 0 else src, src, ring, (idx, p, k), shift(at, d, by))
                c.start()
                sends.append(c)

        def step1(p, idx, own, sets, half):
            d, free = ORDERS[core][idx][p], ORDERS[core][idx][:p]
            for k, by in enumerate((1, -1)):
                got = sets(shift(at, d, -by), free)
                copy(got, got, ring, (idx, p, k), shift(at, d, by)).wait_recv()
                if half:
                    tail = (slice(None), pl.ds(k * half, half))
                    piece = sets(shift(at, d, -by), free, tail)
                elif k == 0:
                    piece = got
                else:
                    continue
                c = copy(piece, piece, ring, (idx, p, 2 + k), shift(at, d, by))
                c.start()
                sends.append(c)

        def step2(p, idx, own, sets, half):
            d, free = ORDERS[core][idx][p], ORDERS[core][idx][:p]
            for k, by in enumerate((1, -1)):
                if half:
                    tail = (slice(None), pl.ds(k * half, half))
                    piece = sets(shift(at, d, 2), free, tail)
                elif k == 0:
                    piece = sets(shift(at, d, 2), free)
                else:
                    continue
                copy(piece, piece, ring, (idx, p, 2 + k), shift(at, d, by)).wait_recv()

        def across(idx, sets, hop):
            d, free = ORDERS[core][idx][2], ORDERS[core][idx][:2]
            piece = sets(shift(at, d, hop), free)
            c = copy(piece, piece, pair, (idx, hop), other)
            c.start()
            sends.append(c)

        own_copies = []
        for idx, own, sets, half in todo:
            step0(0, idx, own, sets, half)
            mine = pltpu.make_async_copy(own, sets(at, ""), own_sem.at[idx])
            mine.start()
            own_copies.append(mine)
        for p in range(3):
            for t in todo:
                step1(p, *t)
                if p == 2:
                    for hop in (1, 3):
                        across(t[0], t[2], hop)
            for i, t in enumerate(todo):
                if p == 0:
                    own_copies[i].wait()
                step2(p, *t)
                if p < 2:
                    step0(p + 1, *t)
                if p == 1:
                    across(t[0], t[2], 0)
                if p == 2:
                    across(t[0], t[2], 2)
        for idx, own, sets, half in todo:
            d, free = ORDERS[1 - core][idx][2], ORDERS[1 - core][idx][:2]
            for hop in range(4):
                piece = sets(shift(other, d, hop), free)
                copy(piece, piece, pair, (idx, hop), other).wait_recv()
        for c in sends:
            c.wait_send()

    for core in range(2):
        pl.when(me["c"] == core)(functools.partial(run, core))


def gather(cid, bias, *mask):
    heads, rows, res = bias.shape
    grid = (2, 4, 2, 4, 2)
    outs = [jax.ShapeDtypeStruct((heads,) + grid + (rows, res), BF16)]
    if mask:
        outs.append(jax.ShapeDtypeStruct(grid + mask[0].shape, F32))
    n = len(outs)
    got = pl.pallas_call(
        functools.partial(gather_kernel, n),
        out_shape=outs,
        in_specs=[VMEM] * n,
        out_specs=[pl.BlockSpec(memory_space=pl.ANY)] * n,
        scratch_shapes=[
            pltpu.SemaphoreType.DMA((5, 3, 4)),
            pltpu.SemaphoreType.DMA((5, 3, 4)),
            pltpu.SemaphoreType.DMA((5, 4)),
            pltpu.SemaphoreType.DMA((5, 4)),
            pltpu.SemaphoreType.DMA((5,)),
        ],
        compiler_params=pltpu.CompilerParams(collective_id=cid, has_side_effects=True),
    )(bias, *mask)
    full = got[0].reshape(heads, -1, res)
    return (full, got[1].reshape((-1,) + mask[0].shape)) if mask else full


def stage_tools(trans, m):
    rows, res, chan = m.x.shape
    groups = rows // 4
    nk = res // KB
    tasks = groups * HEADS
    t = types.SimpleNamespace()

    def eye():
        i = lax.broadcasted_iota(jnp.int32, (KB, KB), 0)
        j = lax.broadcasted_iota(jnp.int32, (KB, KB), 1)
        return (i == j).astype(F32).astype(BF16)

    def project_all():
        w = m.w[...].astype(F32)
        wqt = w[:, :chan].T
        for s in range(4):
            cut = chan - 32 * s
            wk = w[:, chan : 2 * chan]
            m.wk[s] = (pltpu.roll(wk, 32 * s, 1) if s else wk).astype(BF16)
            m.wq[s] = (jnp.concatenate([wqt[cut:], wqt[:cut]], axis=0) if s else wqt).astype(BF16)
        wvt = w[:, 2 * chan : 3 * chan].T.astype(BF16)
        wgt = w[:, 3 * chan :].T.astype(BF16)
        gb = m.gb[...].T
        mrow = m.mrow[...]
        lane = lax.broadcasted_iota(jnp.int32, (1, chan), 1) // HEAD_DIM

        def project(r, carry):
            s = lax.rem(r, 4)
            grp = r // 4
            a = m.a[r]
            kk = jnp.dot(a, m.wk[s], preferred_element_type=F32).astype(BF16)
            aq = m.aq[r]
            qt = (
                lax.dot_general(m.wq[s], aq, NT, preferred_element_type=F32)
                * (HEAD_DIM**-0.5 * LOG2E)
            ).astype(BF16)
            vt = lax.dot_general(wvt, a, NT, preferred_element_type=F32) * mrow
            m.gt[r] = jax.nn.sigmoid(lax.dot_general(wgt, aq, NT, preferred_element_type=F32) + gb)
            for h in range(HEADS):
                slot = lax.rem(h + s, 4)
                m.km[r, h] = kk * (lane == slot).astype(F32).astype(BF16)
                m.vx[r, h, :HEAD_DIM] = vt[HEAD_DIM * h : HEAD_DIM * (h + 1)].astype(BF16)
                m.vx[r, h, HEAD_DIM:] = jnp.broadcast_to(mrow, (16, res)).astype(BF16)
            for u in range(4):
                hh = lax.rem(u - s + 4, 4)
                m.qs[grp, hh, pl.ds(32 * u, 32)] = qt[32 * u : 32 * (u + 1)]
            return carry

        lax.fori_loop(0, rows, project, 0)

    def turn_bias(b_ref):
        for h in range(HEADS):
            for kb in range(nk):
                sl = slice(KB * kb, KB * (kb + 1))
                m.bt[h, sl] = b_ref[h, :, sl].T

    def head_slice(h):
        return pl.ds(pl.multiple_of(HEAD_DIM * h, HEAD_DIM), HEAD_DIM)

    def fast_heads(joff):
        one = eye()

        def of(k):
            return k // HEADS, lax.rem(k, HEADS)

        def weights_step(k, kb, pp):
            grp, h = of(k)
            sl = slice(KB * kb, KB * (kb + 1))
            rhs = jnp.concatenate([m.bt[h, sl], m.qs[grp, h, :, pl.ds(joff, JB)]], axis=0)
            lhs = jnp.concatenate(
                [jnp.concatenate([one, m.km[grp * 4 + r, h, sl]], axis=1) for r in range(4)], axis=0
            )
            p4 = jnp.exp2(jnp.dot(lhs, rhs, preferred_element_type=F32)).astype(BF16)
            for r in range(4):
                pp[r, sl] = p4[KB * r : KB * (r + 1)]

        def mix_step(k, r, pp):
            grp, h = of(k)
            oe = jnp.dot(m.vx[grp * 4 + r, h], pp[r], preferred_element_type=F32)
            den = oe[HEAD_DIM : HEAD_DIM + 1]
            m.gd[...] = jnp.where((den > 2.0**-60) & (den < 2.0**100), m.gd[...], 0.0)
            m.ot[grp * 4 + r, head_slice(h)] = oe[:HEAD_DIM] / den

        def both(k, new, old):
            for kb in range(nk):
                weights_step(k, kb, new)
                if kb % 2:
                    mix_step(k - 1, kb // 2, old)

        for kb in range(nk):
            weights_step(0, kb, m.pa)

        def pair(i, carry):
            both(2 * i + 1, m.pb, m.pa)
            both(2 * i + 2, m.pa, m.pb)
            return carry

        lax.fori_loop(0, tasks // 2 - 1, pair, 0)
        both(tasks - 1, m.pb, m.pa)
        for r in range(4):
            mix_step(tasks - 1, r, m.pb)

    def safe_heads(joff):
        one = eye()

        def row_head(it, carry):
            row, h = it // HEADS, lax.rem(it, HEADS)
            q = m.qs[row // 4, h, :, pl.ds(joff, JB)]

            def scores(kb, carry):
                ks = pl.ds(pl.multiple_of(kb * KB, KB), KB)
                rhs = jnp.concatenate([m.bt[h, ks], q], axis=0)
                lhs = jnp.concatenate([one, m.km[row, h, ks]], axis=1)
                s1 = jnp.dot(lhs, rhs, preferred_element_type=F32)
                s1 = jnp.where(m.mcol[ks] > 0.5, s1, -1e30)
                m.ss[ks] = s1
                return jnp.maximum(carry, jnp.max(s1, axis=0, keepdims=True))

            top = lax.fori_loop(0, nk, scores, jnp.full((1, JB), -1e30, F32))

            def weights(kb, carry):
                ks = pl.ds(pl.multiple_of(kb * KB, KB), KB)
                m.pa[0, ks] = jnp.exp2(m.ss[ks] - top).astype(BF16)
                return carry

            lax.fori_loop(0, nk, weights, 0)
            oe = jnp.dot(m.vx[row, h], m.pa[0], preferred_element_type=F32)
            m.ot[row, head_slice(h)] = oe[:HEAD_DIM] / oe[HEAD_DIM : HEAD_DIM + 1]
            return carry

        lax.fori_loop(0, rows * HEADS, row_head, 0)

    def finish(joff, store):
        def row(r):
            gated = (m.ot[r] * m.gt[r, :, pl.ds(joff, JB)]).T.astype(BF16)
            z = m.x[r, pl.ds(joff, JB)].astype(F32) + jnp.dot(
                gated, m.ow[...], preferred_element_type=F32
            )
            z = z.astype(BF16)
            if trans:
                zf = z.astype(F32)
                a = layer_norm(z, m.ng[...])
                hid = jnp.dot(a, m.ti[...], preferred_element_type=F32) + m.tb[...]
                hid = jnp.maximum(hid, 0.0).astype(BF16)
                z = (zf + jnp.dot(hid, m.to[...], preferred_element_type=F32)).astype(BF16)
            m.zz[r] = z

        def some(i, carry):
            for r in range(UNROLL):
                row(UNROLL * i + r)
            return carry

        lax.fori_loop(0, rows // UNROLL, some, 0)
        span = JB // rows
        out_row = lax.broadcasted_iota(jnp.int32, (JB, JB), 0)
        in_row = lax.broadcasted_iota(jnp.int32, (JB, JB), 1)
        perm = (in_row == lax.rem(out_row, rows) * span + out_row // rows).astype(F32).astype(BF16)
        for q in range(rows // 2):
            cols = [
                jnp.concatenate([m.zz[r, span * n : span * (n + 1)] for r in range(rows)], axis=0)
                for n in (2 * q, 2 * q + 1)
            ]
            moved = jnp.dot(perm, jnp.concatenate(cols, axis=1), preferred_element_type=F32)
            for n in range(2):
                part = moved[:, chan * n : chan * (n + 1)]
                store(span * (2 * q + n), part.reshape(span, rows, chan).astype(BF16))

    return types.SimpleNamespace(
        project_all=project_all, turn_bias=turn_bias, fast_heads=fast_heads,
        safe_heads=safe_heads, finish=finish,
    )


def stage_names(trans):
    names = ["x", "a", "w", "gb", "ow", "mrow", "mcol"]
    return names + (["ng", "ti", "tb", "to"] if trans else [])


def stage_scratch(rows, res, chan):
    return {
        "km": pltpu.VMEM((rows, HEADS, res, chan), BF16),
        "qs": pltpu.VMEM((rows // 4, HEADS, chan, res), BF16),
        "vx": pltpu.VMEM((rows, HEADS, HEAD_DIM + 16, res), BF16),
        "gt": pltpu.VMEM((rows, chan, res), F32),
        "bt": pltpu.VMEM((HEADS, res, JB), BF16),
        "pa": pltpu.VMEM((4, res, JB), BF16),
        "pb": pltpu.VMEM((4, res, JB), BF16),
        "ot": pltpu.VMEM((rows, chan, JB), F32),
        "wk": pltpu.VMEM((4, chan, chan), BF16),
        "wq": pltpu.VMEM((4, chan, chan), BF16),
        "gd": pltpu.VMEM((1, JB), F32),
        "zz": pltpu.VMEM((rows, JB, chan), BF16),
        "bs": pltpu.VMEM((HEADS, JB, res), BF16),
        "ss": pltpu.VMEM((res, JB), F32),
    }


def safe_kernel(trans, names, *refs):
    m = types.SimpleNamespace(**dict(zip(names, refs)))
    m.aq = m.a
    tools = stage_tools(trans, m)

    @pl.when(pl.program_id(0) == 0)
    def _():
        tools.project_all()

    joff = pl.multiple_of(pl.program_id(0) * JB, JB)
    tools.turn_bias(m.b)
    tools.safe_heads(joff)

    def store(at, part):
        m.o[at : at + part.shape[0]] = part

    tools.finish(joff, store)


def safe_attention(ins, bias, trans):
    rows, res, chan = ins[0].shape
    scratch = stage_scratch(rows, res, chan)
    names = stage_names(trans) + ["b", "o"] + list(scratch)
    full = lambda a: pl.BlockSpec(a.shape, lambda j, n=a.ndim: (0,) * n)
    return pl.pallas_call(
        functools.partial(safe_kernel, trans, names),
        grid=(res // JB,),
        out_shape=jax.ShapeDtypeStruct((res, rows, chan), BF16),
        in_specs=[full(a) for a in ins] + [pl.BlockSpec((HEADS, JB, res), lambda j: (0, j, 0))],
        out_specs=pl.BlockSpec((JB, rows, chan), lambda j: (j, 0, 0)),
        scratch_shapes=list(scratch.values()),
        compiler_params=pltpu.CompilerParams(
            dimension_semantics=("arbitrary",), vmem_limit_bytes=60 * 1024 * 1024
        ),
    )(*ins, bias)


def fused_kernel(trans, n, names, *refs):
    m = types.SimpleNamespace(**dict(zip(names, refs)))
    tools = stage_tools(trans, m)
    rows, res, chan = m.x.shape
    nj = res // JB
    per = JB // rows
    gx, gy = lax.axis_index("gx"), lax.axis_index("gy")
    ny = n // 16
    me = gx * ny + gy
    at = lambda d: {"gx": d // ny, "gy": lax.rem(d, ny)}
    barrier = pltpu.get_barrier_semaphore()

    def greet(t, carry):
        pl.semaphore_signal(
            barrier, inc=1, device_id=at(lax.rem(me + t, n)), device_id_type=pl.DeviceIdType.MESH
        )
        return carry

    lax.fori_loop(1, n, greet, 0)

    def block_of(t):
        return lax.rem(t + lax.rem(gx // 2, 4) + gy // 2 + 2 * lax.rem(gy, 2) + gx // 8, nj)

    def chunk(c, u):
        return pl.ds(pl.multiple_of(owner(c, 2 * u) * rows, 2 * rows), 2 * rows)

    def slot(c, u):
        return pl.ds(pl.multiple_of(c * JB + u * 2 * rows, 2 * rows), 2 * rows)

    def fetch(t):
        c = block_of(t)

        def one(u, carry):
            pltpu.make_async_copy(m.b.at[:, chunk(c, u)], m.bs.at[:, slot(0, u)], m.fetch_sem).start()
            return carry

        lax.fori_loop(0, per // 2, one, 0)

    def fetched():
        pltpu.make_async_copy(m.b.at[:, pl.ds(0, JB)], m.bs, m.fetch_sem).wait()

    def copy(t, i, frm):
        to = owner(block_of(t), i)
        ahead = lax.rem(to - me + n, n)
        return to, pltpu.make_async_remote_copy(
            src_ref=m.zs.at[lax.rem(t, 2), pl.ds(pl.multiple_of(i * rows, rows), rows)],
            dst_ref=m.o.at[:, pl.ds(pl.multiple_of(rows * frm, rows), rows)],
            send_sem=m.send_sem.at[ahead], recv_sem=m.recv_sem.at[ahead],
            device_id=at(to), device_id_type=pl.DeviceIdType.MESH,
        )

    def own(t, i):
        mine = pl.ds(pl.multiple_of(rows * me, rows), rows)
        return pltpu.make_async_copy(
            m.zs.at[lax.rem(t, 2), pl.ds(pl.multiple_of(i * rows, rows), rows)],
            m.o.at[:, mine], m.own_sem,
        )

    first = ((gx // 8) * 2 + lax.rem(gx, 2)) * ny + gy

    def send_block(t):
        def send(k, carry):
            i = lax.rem(k + first, per)
            to, c = copy(t, i, me)

            @pl.when(to != me)
            def _():
                c.start()

            @pl.when(to == me)
            def _():
                own(t, i).start()

            return carry

        lax.fori_loop(0, per, send, 0)

    def sent_block(t):
        def sent(k, carry):
            i = lax.rem(k + first, per)
            to, c = copy(t, i, me)

            @pl.when(to != me)
            def _():
                c.wait_send()

            @pl.when(to == me)
            def _():
                own(t, i).wait()

            return carry

        lax.fori_loop(0, per, sent, 0)

    fetch(0)
    tools.project_all()
    m.gd[...] = jnp.ones_like(m.gd)
    pl.semaphore_wait(barrier, n - 1)

    def block(t, carry):
        joff = pl.multiple_of(block_of(t) * JB, JB)
        fetched()
        tools.turn_bias(m.bs)

        @pl.when(t > 0)
        def _():
            send_block(t - 1)

        @pl.when(t < nj - 1)
        def _():
            fetch(t + 1)

        tools.fast_heads(joff)

        @pl.when(t > 1)
        def _():
            sent_block(t - 2)

        def store(at, part):
            m.zs[lax.rem(t, 2), at : at + part.shape[0]] = part

        tools.finish(joff, store)
        return carry

    lax.fori_loop(0, nj, block, 0)
    good = jnp.min(m.gd[...], axis=1, keepdims=True)
    if trans:
        m.good[...] = jnp.minimum(m.before[...], good)
    else:
        m.good[...] = jnp.broadcast_to(good, m.good.shape)
    send_block(nj - 1)
    if trans:
        def flag(t, carry):
            c = pltpu.make_async_remote_copy(
                src_ref=m.good.at[pl.ds(0, 1)], dst_ref=m.flags.at[me, pl.ds(0, 1)],
                send_sem=m.fsend.at[t], recv_sem=m.frecv.at[t],
                device_id=at(lax.rem(me + t, n)), device_id_type=pl.DeviceIdType.MESH,
            )
            c.start()
            return carry

        lax.fori_loop(1, n, flag, 0)
        mine = pltpu.make_async_copy(m.good, m.flags.at[me], m.fsend.at[0])
        mine.start()
        mine.wait()
    sent_block(nj - 2)
    sent_block(nj - 1)

    def land(t, carry):
        frm = lax.rem(me + n - t, n)
        pltpu.make_async_remote_copy(
            src_ref=m.zs.at[0, pl.ds(0, rows)],
            dst_ref=m.o.at[:, pl.ds(pl.multiple_of(rows * frm, rows), rows)],
            send_sem=m.send_sem.at[t], recv_sem=m.recv_sem.at[t],
            device_id=at(frm), device_id_type=pl.DeviceIdType.MESH,
        ).wait_recv()
        if trans:
            c = pltpu.make_async_remote_copy(
                src_ref=m.good.at[pl.ds(0, 1)], dst_ref=m.flags.at[frm, pl.ds(0, 1)],
                send_sem=m.fsend.at[t], recv_sem=m.frecv.at[t],
                device_id=at(frm), device_id_type=pl.DeviceIdType.MESH,
            )
            c.wait_recv()
            c.wait_send()
        return carry

    lax.fori_loop(1, n, land, 0)


def fused_attention(cid, n, ins, bias, before):
    trans = before is not None
    rows, res, chan = ins[0].shape
    scratch = stage_scratch(rows, res, chan)
    del scratch["ss"]
    scratch |= {
        "zs": pltpu.VMEM((2, JB, rows, chan), BF16),
        "send_sem": pltpu.SemaphoreType.DMA((n,)),
        "recv_sem": pltpu.SemaphoreType.DMA((n,)),
        "fetch_sem": pltpu.SemaphoreType.DMA,
        "own_sem": pltpu.SemaphoreType.DMA,
    }
    anywhere = pl.BlockSpec(memory_space=pl.ANY)
    outs = {"o": jax.ShapeDtypeStruct((rows, res, chan), BF16)}
    out_specs = [anywhere]
    names = stage_names(trans) + ["aq", "b"]
    args = list(ins) + [bias]
    in_specs = [VMEM] * len(ins) + [anywhere]
    if trans:
        names.append("before")
        args.append(before)
        in_specs.append(VMEM)
        outs["flags"] = jax.ShapeDtypeStruct((n, 8, 128), F32)
        out_specs.append(anywhere)
        scratch |= {
            "good": pltpu.VMEM((8, 128), F32),
            "fsend": pltpu.SemaphoreType.DMA((n,)),
            "frecv": pltpu.SemaphoreType.DMA((n,)),
        }
    else:
        outs["good"] = jax.ShapeDtypeStruct((8, 128), F32)
        out_specs.append(VMEM)
    return pl.pallas_call(
        functools.partial(fused_kernel, trans, n, names + list(outs) + list(scratch)),
        out_shape=list(outs.values()),
        in_specs=in_specs,
        out_specs=out_specs,
        scratch_shapes=list(scratch.values()),
        compiler_params=pltpu.CompilerParams(
            collective_id=cid, has_side_effects=True, vmem_limit_bytes=60 * 1024 * 1024
        ),
    )(*args)


def exchange_kernel(n, whole, z_ref, o_ref, send_sem, recv_sem, own_sem):
    rows = z_ref.shape[1]
    cut = lambda d: z_ref if whole else z_ref.at[pl.ds(pl.multiple_of(rows * d, rows), rows)]
    gy = n // 16
    me = lax.axis_index("gx") * gy + lax.axis_index("gy")
    at = lambda d: {"gx": d // gy, "gy": lax.rem(d, gy)}
    barrier = pltpu.get_barrier_semaphore()

    def greet(t, carry):
        pl.semaphore_signal(
            barrier, inc=1, device_id=at(lax.rem(me + t, n)), device_id_type=pl.DeviceIdType.MESH
        )
        return carry

    lax.fori_loop(1, n, greet, 0)
    mine = pl.ds(pl.multiple_of(rows * me, rows), rows)
    own = pltpu.make_async_copy(cut(me), o_ref.at[:, mine], own_sem)
    own.start()
    pl.semaphore_wait(barrier, n - 1)

    def copy(t, to, frm):
        return pltpu.make_async_remote_copy(
            src_ref=cut(to),
            dst_ref=o_ref.at[:, pl.ds(pl.multiple_of(rows * frm, rows), rows)],
            send_sem=send_sem.at[t], recv_sem=recv_sem.at[t],
            device_id=at(to), device_id_type=pl.DeviceIdType.MESH,
        )

    def send(t, carry):
        copy(t, lax.rem(me + t, n), me).start()
        return carry

    lax.fori_loop(1, n, send, 0)
    own.wait()

    def land(t, carry):
        copy(t, lax.rem(me + t, n), lax.rem(me + n - t, n)).wait_recv()
        copy(t, lax.rem(me + t, n), me).wait_send()
        return carry

    lax.fori_loop(1, n, land, 0)


def exchange(cid, n, z, whole=False):
    lead, rows, width = z.shape
    shape = (lead, n * rows, width) if whole else (rows, lead, width)
    return pl.pallas_call(
        functools.partial(exchange_kernel, n, whole),
        out_shape=jax.ShapeDtypeStruct(shape, BF16),
        in_specs=[pl.BlockSpec(memory_space=pl.ANY)],
        out_specs=pl.BlockSpec(memory_space=pl.ANY),
        scratch_shapes=[
            pltpu.SemaphoreType.DMA((n,)),
            pltpu.SemaphoreType.DMA((n,)),
            pltpu.SemaphoreType.DMA,
        ],
        compiler_params=pltpu.CompilerParams(collective_id=cid, has_side_effects=True),
    )(z)


def local(
    pair_in,
    residue_mask,
    norm_start,
    proj_start,
    gate_bias_start,
    bias_w_start,
    out_w_start,
    norm_end,
    proj_end,
    gate_bias_end,
    bias_w_end,
    out_w_end,
    norm_trans,
    trans_in,
    trans_bias,
    trans_out,
):
    rows, res, chan = pair_in.shape
    n = lax.axis_size(("gx", "gy"))
    row = lambda v: v.reshape(1, -1)
    mine = jnp.pad(residue_mask.astype(F32).reshape(1, rows), ((0, 7), (0, 128 - rows)))
    bias, normed, turned, turned_a = pair_bias(pair_in, row(norm_start), bias_w_start)
    bias, mask = gather(0, bias, mine)
    mask = mask[:, 0, :rows].reshape(res)
    mask = jnp.where(jnp.max(mask) > 0.5, mask, 1.0)
    mrow, mcol = mask.reshape(1, res), mask.reshape(res, 1)
    start = [pair_in, normed, proj_start, row(gate_bias_start), out_w_start, mrow, mcol]
    ends = [proj_end, row(gate_bias_end), out_w_end, mrow, mcol]
    ends += [row(norm_trans), trans_in, row(trans_bias), trans_out]

    def end_inputs(cols):
        bias, normed, turned, turned_a = pair_bias(cols, row(norm_end), bias_w_end)
        return [cols, normed] + ends, [turned, normed] + ends + [turned_a], bias

    def safe(bias):
        cols = exchange(4, n, safe_attention(start, bias, False))
        ins, _, bias = end_inputs(cols)
        return exchange(5, n, safe_attention(ins, exchange(6, n, bias, True), True))

    cols, good = fused_attention(2, n, [turned] + start[1:] + [turned_a], bias, None)
    _, ins, end_bias = end_inputs(cols)
    out, flags = fused_attention(3, n, ins, gather(1, end_bias), good)
    return lax.cond(jnp.min(flags[:, 0]) > 0.5, lambda b: out, safe, bias)


def solution(mesh):
    spec = P(("gx", "gy"), None, None)
    placed = (spec, P(("gx", "gy"))) + (P(),) * 14
    return jax.shard_map(local, mesh=mesh, in_specs=placed, out_specs=spec, check_vma=False)
```

```python
import functools
import types

import jax
import jax.numpy as jnp
from jax import lax
from jax.experimental import pallas as pl
from jax.experimental.pallas import tpu as pltpu
from jax.sharding import PartitionSpec as P

HEADS = 4
HEAD_DIM = 32
LOG2E = 1.4426950408889634
JB = 256
KB = 128
UNROLL = 4
F32 = jnp.float32
BF16 = jnp.bfloat16
NT = (((1,), (1,)), ((), ()))
TN = (((0,), (0,)), ((), ()))
VMEM = pl.BlockSpec(memory_space=pltpu.VMEM)


def layer_norm(t, gain):
    chan = t.shape[1]
    mean = jnp.dot(t, jnp.full((chan, chan), 1.0 / chan, BF16), preferred_element_type=F32)
    cent = t.astype(F32) - mean
    var = jnp.mean(cent * cent, axis=-1, keepdims=True)
    return (cent * lax.rsqrt(var + 1e-05) * gain).astype(BF16)


def bias_kernel(x_ref, g_ref, bw_ref, o_ref, a_ref):
    bwt = bw_ref[...].astype(F32).T.astype(BF16)
    gain = g_ref[...]
    for r in range(x_ref.shape[0]):
        a = layer_norm(x_ref[r], gain)
        a_ref[r] = a
        b = lax.dot_general(bwt, a, NT, preferred_element_type=F32) * LOG2E
        o_ref[:, r, :] = b[:HEADS].astype(BF16)


def pair_bias(x, gain, bias_w):
    rows, res, chan = x.shape
    bw = jnp.pad(bias_w, ((0, 0), (0, 128 - HEADS)))
    return pl.pallas_call(
        bias_kernel,
        out_shape=[
            jax.ShapeDtypeStruct((HEADS, rows, res), BF16),
            jax.ShapeDtypeStruct(x.shape, BF16),
        ],
        in_specs=[VMEM] * 3,
        out_specs=[VMEM] * 2,
    )(x, gain, bw)


ORDERS = (
    ("xyz", "yzx", "zxy", "xyz", "yzx"),
    ("yzx", "zxy", "xyz", "yzx", "xyz"),
)


def place():
    gx, gy = lax.axis_index("gx"), lax.axis_index("gy")
    return {
        "x": lax.rem(gx // 2, 4),
        "y": gy // 2,
        "z": 2 * lax.rem(gy, 2) + gx // 8,
        "c": lax.rem(gx, 2),
    }


def device(at):
    z_lo, z_hi = lax.rem(at["z"], 2), at["z"] // 2
    return {"gx": (z_lo * 4 + at["x"]) * 2 + at["c"], "gy": at["y"] * 2 + z_hi}


def shift(at, dim, by):
    return {**at, dim: lax.rem(at[dim] + by + 4, 4)}


def part(ref, lead, at, free, tail=()):
    z = "z" in free
    pick = lambda d: slice(None) if d in free else at[d]
    z_lo = slice(None) if z else lax.rem(at["z"], 2)
    z_hi = slice(None) if z else at["z"] // 2
    return ref.at[lead + (z_lo, pick("x"), at["c"], pick("y"), z_hi) + tail]


def gather_kernel(n_out, *refs):
    ins, outs = refs[:n_out], refs[n_out : 2 * n_out]
    ring_send, ring_recv, pair_send, pair_recv, own_sem = refs[2 * n_out :]
    me = place()
    barrier = pltpu.get_barrier_semaphore()
    sib = {**me, "c": 1 - me["c"]}
    partners = [shift(me, d, by) for d in "xyz" for by in (1, -1)] + [sib]
    for at in partners:
        pl.semaphore_signal(barrier, inc=1, device_id=device(at), device_id_type=pl.DeviceIdType.MESH)
    pl.semaphore_wait(barrier, len(partners))

    def items(core):
        half = outs[0].shape[-1] // 2
        got = []
        for h in range(HEADS):
            got.append((h, ins[0].at[h], functools.partial(part, outs[0], (h,)), half))
        if n_out == 2:
            got.append((HEADS, ins[1], functools.partial(part, outs[1], ()), 0))
        return got

    def copy(src, dst, sems, idx, to):
        return pltpu.make_async_remote_copy(
            src_ref=src, dst_ref=dst, send_sem=sems[0].at[idx], recv_sem=sems[1].at[idx],
            device_id=device(to), device_id_type=pl.DeviceIdType.MESH,
        )

    ring, pair = (ring_send, ring_recv), (pair_send, pair_recv)

    def run(core):
        at = {**me, "c": core}
        other = {**me, "c": 1 - core}
        todo = items(core)
        sends = []

        def step0(p, idx, own, sets, half):
            d, free = ORDERS[core][idx][p], ORDERS[core][idx][:p]
            src = sets(at, free)
            for k, by in enumerate((1, -1)):
                c = copy(own if p == 0 else src, src, ring, (idx, p, k), shift(at, d, by))
                c.start()
                sends.append(c)

        def step1(p, idx, own, sets, half):
            d, free = ORDERS[core][idx][p], ORDERS[core][idx][:p]
            for k, by in enumerate((1, -1)):
                got = sets(shift(at, d, -by), free)
                copy(got, got, ring, (idx, p, k), shift(at, d, by)).wait_recv()
                if half:
                    tail = (slice(None), pl.ds(k * half, half))
                    piece = sets(shift(at, d, -by), free, tail)
                elif k == 0:
                    piece = got
                else:
                    continue
                c = copy(piece, piece, ring, (idx, p, 2 + k), shift(at, d, by))
                c.start()
                sends.append(c)

        def step2(p, idx, own, sets, half):
            d, free = ORDERS[core][idx][p], ORDERS[core][idx][:p]
            for k, by in enumerate((1, -1)):
                if half:
                    tail = (slice(None), pl.ds(k * half, half))
                    piece = sets(shift(at, d, 2), free, tail)
                elif k == 0:
                    piece = sets(shift(at, d, 2), free)
                else:
                    continue
                copy(piece, piece, ring, (idx, p, 2 + k), shift(at, d, by)).wait_recv()

        def across(idx, sets, hop):
            d, free = ORDERS[core][idx][2], ORDERS[core][idx][:2]
            piece = sets(shift(at, d, hop), free)
            c = copy(piece, piece, pair, (idx, hop), other)
            c.start()
            sends.append(c)

        own_copies = []
        for idx, own, sets, half in todo:
            step0(0, idx, own, sets, half)
            mine = pltpu.make_async_copy(own, sets(at, ""), own_sem.at[idx])
            mine.start()
            own_copies.append(mine)
        for p in range(3):
            for t in todo:
                step1(p, *t)
                if p == 2:
                    for hop in (1, 3):
                        across(t[0], t[2], hop)
            for i, t in enumerate(todo):
                if p == 0:
                    own_copies[i].wait()
                step2(p, *t)
                if p < 2:
                    step0(p + 1, *t)
                if p == 1:
                    across(t[0], t[2], 0)
                if p == 2:
                    across(t[0], t[2], 2)
        for idx, own, sets, half in todo:
            d, free = ORDERS[1 - core][idx][2], ORDERS[1 - core][idx][:2]
            for hop in range(4):
                piece = sets(shift(other, d, hop), free)
                copy(piece, piece, pair, (idx, hop), other).wait_recv()
        for c in sends:
            c.wait_send()

    for core in range(2):
        pl.when(me["c"] == core)(functools.partial(run, core))


def gather(cid, bias, *mask):
    heads, rows, res = bias.shape
    grid = (2, 4, 2, 4, 2)
    outs = [jax.ShapeDtypeStruct((heads,) + grid + (rows, res), BF16)]
    if mask:
        outs.append(jax.ShapeDtypeStruct(grid + mask[0].shape, F32))
    n = len(outs)
    got = pl.pallas_call(
        functools.partial(gather_kernel, n),
        out_shape=outs,
        in_specs=[VMEM] * n,
        out_specs=[pl.BlockSpec(memory_space=pl.ANY)] * n,
        scratch_shapes=[
            pltpu.SemaphoreType.DMA((5, 3, 4)),
            pltpu.SemaphoreType.DMA((5, 3, 4)),
            pltpu.SemaphoreType.DMA((5, 4)),
            pltpu.SemaphoreType.DMA((5, 4)),
            pltpu.SemaphoreType.DMA((5,)),
        ],
        compiler_params=pltpu.CompilerParams(collective_id=cid, has_side_effects=True),
    )(bias, *mask)
    full = got[0].reshape(heads, -1, res)
    return (full, got[1].reshape((-1,) + mask[0].shape)) if mask else full


def stage_tools(trans, m):
    rows, res, chan = m.x.shape
    groups = rows // 4
    nk = res // KB
    tasks = groups * HEADS
    t = types.SimpleNamespace()

    def eye():
        i = lax.broadcasted_iota(jnp.int32, (KB, KB), 0)
        j = lax.broadcasted_iota(jnp.int32, (KB, KB), 1)
        return (i == j).astype(F32).astype(BF16)

    def project_all():
        w = m.w[...].astype(F32)
        wqt = w[:, :chan].T
        for s in range(4):
            cut = chan - 32 * s
            wk = w[:, chan : 2 * chan]
            m.wk[s] = (pltpu.roll(wk, 32 * s, 1) if s else wk).astype(BF16)
            m.wq[s] = (jnp.concatenate([wqt[cut:], wqt[:cut]], axis=0) if s else wqt).astype(BF16)
        wvt = w[:, 2 * chan : 3 * chan].T.astype(BF16)
        wgt = w[:, 3 * chan :].T.astype(BF16)
        gb = m.gb[...].T
        mrow = m.mrow[...]
        lane = lax.broadcasted_iota(jnp.int32, (1, chan), 1) // HEAD_DIM

        def project(r, carry):
            s = lax.rem(r, 4)
            grp = r // 4
            a = m.a[r]
            kk = jnp.dot(a, m.wk[s], preferred_element_type=F32).astype(BF16)
            qt = (
                lax.dot_general(m.wq[s], a, NT, preferred_element_type=F32)
                * (HEAD_DIM**-0.5 * LOG2E)
            ).astype(BF16)
            vt = lax.dot_general(wvt, a, NT, preferred_element_type=F32) * mrow
            m.gt[r] = jax.nn.sigmoid(lax.dot_general(wgt, a, NT, preferred_element_type=F32) + gb)
            for h in range(HEADS):
                slot = lax.rem(h + s, 4)
                m.km[r, h] = kk * (lane == slot).astype(F32).astype(BF16)
                m.vx[r, h, :HEAD_DIM] = vt[HEAD_DIM * h : HEAD_DIM * (h + 1)].astype(BF16)
                m.vx[r, h, HEAD_DIM:] = jnp.broadcast_to(mrow, (16, res)).astype(BF16)
            for u in range(4):
                hh = lax.rem(u - s + 4, 4)
                m.qs[grp, hh, pl.ds(32 * u, 32)] = qt[32 * u : 32 * (u + 1)]
            return carry

        lax.fori_loop(0, rows, project, 0)

    def turn_bias(b_ref):
        for h in range(HEADS):
            for kb in range(nk):
                sl = slice(KB * kb, KB * (kb + 1))
                m.bt[h, sl] = b_ref[h, :, sl].T

    def head_slice(h):
        return pl.ds(pl.multiple_of(HEAD_DIM * h, HEAD_DIM), HEAD_DIM)

    def fast_heads(joff):
        one = eye()

        def of(k):
            return k // HEADS, lax.rem(k, HEADS)

        def weights_step(k, kb, pp):
            grp, h = of(k)
            sl = slice(KB * kb, KB * (kb + 1))
            rhs = jnp.concatenate([m.bt[h, sl], m.qs[grp, h, :, pl.ds(joff, JB)]], axis=0)
            lhs = jnp.concatenate(
                [jnp.concatenate([one, m.km[grp * 4 + r, h, sl]], axis=1) for r in range(4)], axis=0
            )
            p4 = jnp.exp2(jnp.dot(lhs, rhs, preferred_element_type=F32)).astype(BF16)
            for r in range(4):
                pp[r, sl] = p4[KB * r : KB * (r + 1)]

        def mix_step(k, r, pp):
            grp, h = of(k)
            oe = jnp.dot(m.vx[grp * 4 + r, h], pp[r], preferred_element_type=F32)
            den = oe[HEAD_DIM : HEAD_DIM + 1]
            m.gd[...] = jnp.where((den > 2.0**-60) & (den < 2.0**100), m.gd[...], 0.0)
            m.ot[grp * 4 + r, head_slice(h)] = oe[:HEAD_DIM] / den

        def both(k, new, old):
            for kb in range(nk):
                weights_step(k, kb, new)
                if kb % 2:
                    mix_step(k - 1, kb // 2, old)

        for kb in range(nk):
            weights_step(0, kb, m.pa)

        def pair(i, carry):
            both(2 * i + 1, m.pb, m.pa)
            both(2 * i + 2, m.pa, m.pb)
            return carry

        lax.fori_loop(0, tasks // 2 - 1, pair, 0)
        both(tasks - 1, m.pb, m.pa)
        for r in range(4):
            mix_step(tasks - 1, r, m.pb)

    def safe_heads(joff):
        one = eye()

        def row_head(it, carry):
            row, h = it // HEADS, lax.rem(it, HEADS)
            q = m.qs[row // 4, h, :, pl.ds(joff, JB)]

            def scores(kb, carry):
                ks = pl.ds(pl.multiple_of(kb * KB, KB), KB)
                rhs = jnp.concatenate([m.bt[h, ks], q], axis=0)
                lhs = jnp.concatenate([one, m.km[row, h, ks]], axis=1)
                s1 = jnp.dot(lhs, rhs, preferred_element_type=F32)
                s1 = jnp.where(m.mcol[ks] > 0.5, s1, -1e30)
                m.ss[ks] = s1
                return jnp.maximum(carry, jnp.max(s1, axis=0, keepdims=True))

            top = lax.fori_loop(0, nk, scores, jnp.full((1, JB), -1e30, F32))

            def weights(kb, carry):
                ks = pl.ds(pl.multiple_of(kb * KB, KB), KB)
                m.pa[0, ks] = jnp.exp2(m.ss[ks] - top).astype(BF16)
                return carry

            lax.fori_loop(0, nk, weights, 0)
            oe = jnp.dot(m.vx[row, h], m.pa[0], preferred_element_type=F32)
            m.ot[row, head_slice(h)] = oe[:HEAD_DIM] / oe[HEAD_DIM : HEAD_DIM + 1]
            return carry

        lax.fori_loop(0, rows * HEADS, row_head, 0)

    def finish(joff, store):
        def row(r):
            gated = (m.ot[r] * m.gt[r, :, pl.ds(joff, JB)]).T.astype(BF16)
            z = m.x[r, pl.ds(joff, JB)].astype(F32) + jnp.dot(
                gated, m.ow[...], preferred_element_type=F32
            )
            z = z.astype(BF16)
            if trans:
                zf = z.astype(F32)
                a = layer_norm(z, m.ng[...])
                hid = jnp.dot(a, m.ti[...], preferred_element_type=F32) + m.tb[...]
                hid = jnp.maximum(hid, 0.0).astype(BF16)
                z = (zf + jnp.dot(hid, m.to[...], preferred_element_type=F32)).astype(BF16)
            m.zz[r] = z

        def some(i, carry):
            for r in range(UNROLL):
                row(UNROLL * i + r)
            return carry

        lax.fori_loop(0, rows // UNROLL, some, 0)
        span = JB // rows
        out_row = lax.broadcasted_iota(jnp.int32, (JB, JB), 0)
        in_row = lax.broadcasted_iota(jnp.int32, (JB, JB), 1)
        perm = (in_row == lax.rem(out_row, rows) * span + out_row // rows).astype(F32).astype(BF16)
        for q in range(rows // 2):
            cols = [
                jnp.concatenate([m.zz[r, span * n : span * (n + 1)] for r in range(rows)], axis=0)
                for n in (2 * q, 2 * q + 1)
            ]
            moved = jnp.dot(perm, jnp.concatenate(cols, axis=1), preferred_element_type=F32)
            for n in range(2):
                part = moved[:, chan * n : chan * (n + 1)]
                store(span * (2 * q + n), part.reshape(span, rows, chan).astype(BF16))

    return types.SimpleNamespace(
        project_all=project_all, turn_bias=turn_bias, fast_heads=fast_heads,
        safe_heads=safe_heads, finish=finish,
    )


def stage_names(trans):
    names = ["x", "a", "w", "gb", "ow", "mrow", "mcol"]
    return names + (["ng", "ti", "tb", "to"] if trans else [])


def stage_scratch(rows, res, chan):
    return {
        "km": pltpu.VMEM((rows, HEADS, res, chan), BF16),
        "qs": pltpu.VMEM((rows // 4, HEADS, chan, res), BF16),
        "vx": pltpu.VMEM((rows, HEADS, HEAD_DIM + 16, res), BF16),
        "gt": pltpu.VMEM((rows, chan, res), F32),
        "bt": pltpu.VMEM((HEADS, res, JB), BF16),
        "pa": pltpu.VMEM((4, res, JB), BF16),
        "pb": pltpu.VMEM((4, res, JB), BF16),
        "ot": pltpu.VMEM((rows, chan, JB), F32),
        "wk": pltpu.VMEM((4, chan, chan), BF16),
        "wq": pltpu.VMEM((4, chan, chan), BF16),
        "gd": pltpu.VMEM((1, JB), F32),
        "zz": pltpu.VMEM((rows, JB, chan), BF16),
        "bs": pltpu.VMEM((HEADS, JB, res), BF16),
        "ss": pltpu.VMEM((res, JB), F32),
    }


def safe_kernel(trans, names, *refs):
    m = types.SimpleNamespace(**dict(zip(names, refs)))
    tools = stage_tools(trans, m)

    @pl.when(pl.program_id(0) == 0)
    def _():
        tools.project_all()

    joff = pl.multiple_of(pl.program_id(0) * JB, JB)
    tools.turn_bias(m.b)
    tools.safe_heads(joff)

    def store(at, part):
        m.o[at : at + part.shape[0]] = part

    tools.finish(joff, store)


def safe_attention(ins, bias, trans):
    rows, res, chan = ins[0].shape
    scratch = stage_scratch(rows, res, chan)
    names = stage_names(trans) + ["b", "o"] + list(scratch)
    full = lambda a: pl.BlockSpec(a.shape, lambda j, n=a.ndim: (0,) * n)
    return pl.pallas_call(
        functools.partial(safe_kernel, trans, names),
        grid=(res // JB,),
        out_shape=jax.ShapeDtypeStruct((res, rows, chan), BF16),
        in_specs=[full(a) for a in ins] + [pl.BlockSpec((HEADS, JB, res), lambda j: (0, j, 0))],
        out_specs=pl.BlockSpec((JB, rows, chan), lambda j: (j, 0, 0)),
        scratch_shapes=list(scratch.values()),
        compiler_params=pltpu.CompilerParams(
            dimension_semantics=("arbitrary",), vmem_limit_bytes=60 * 1024 * 1024
        ),
    )(*ins, bias)


def fused_kernel(trans, n, names, *refs):
    m = types.SimpleNamespace(**dict(zip(names, refs)))
    tools = stage_tools(trans, m)
    rows, res, chan = m.x.shape
    nj = res // JB
    per = JB // rows
    gy = n // 16
    me = lax.axis_index("gx") * gy + lax.axis_index("gy")
    at = lambda d: {"gx": d // gy, "gy": lax.rem(d, gy)}
    barrier = pltpu.get_barrier_semaphore()

    def greet(t, carry):
        pl.semaphore_signal(
            barrier, inc=1, device_id=at(lax.rem(me + t, n)), device_id_type=pl.DeviceIdType.MESH
        )
        return carry

    lax.fori_loop(1, n, greet, 0)

    def block_of(t):
        return lax.rem(t + me, nj)

    def fetch(t):
        return pltpu.make_async_copy(
            m.b.at[:, pl.ds(pl.multiple_of(block_of(t) * JB, JB), JB)], m.bs, m.fetch_sem
        )

    mine = pl.ds(pl.multiple_of(rows * me, rows), rows)

    def send_block(t):
        def send(k, carry):
            i = lax.rem(k + me // nj, per)
            to = block_of(t) * per + i
            src = m.zs.at[lax.rem(t, 2), pl.ds(pl.multiple_of(i * rows, rows), rows)]

            @pl.when(to != me)
            def _():
                pltpu.make_async_remote_copy(
                    src_ref=src, dst_ref=m.o.at[:, mine],
                    send_sem=m.send_sem.at[lax.rem(t, 2)], recv_sem=m.recv_sem,
                    device_id=at(to), device_id_type=pl.DeviceIdType.MESH,
                ).start()

            @pl.when(to == me)
            def _():
                pltpu.make_async_copy(src, m.o.at[:, mine], m.own_sem).start()

            return carry

        lax.fori_loop(0, per, send, 0)

    def sent_block(t):
        here = block_of(t) == me // per
        slot = lax.rem(t, 2)

        def sent(count):
            piece = m.zs.at[slot, pl.ds(0, count * rows)]
            pltpu.make_async_copy(piece, piece, m.send_sem.at[slot]).wait()

        @pl.when(here)
        def _():
            sent(per - 1)
            pltpu.make_async_copy(m.zs.at[slot, pl.ds(0, rows)], m.o.at[:, mine], m.own_sem).wait()

        @pl.when(jnp.logical_not(here))
        def _():
            sent(per)

    fetch(0).start()
    tools.project_all()
    m.gd[...] = jnp.ones_like(m.gd)
    pl.semaphore_wait(barrier, n - 1)

    def block(t, carry):
        joff = pl.multiple_of(block_of(t) * JB, JB)
        fetch(t).wait()
        tools.turn_bias(m.bs)

        @pl.when(t > 0)
        def _():
            send_block(t - 1)

        @pl.when(t < nj - 1)
        def _():
            fetch(t + 1).start()

        tools.fast_heads(joff)

        @pl.when(t > 1)
        def _():
            sent_block(t - 2)

        def store(at, part):
            m.zs[lax.rem(t, 2), at : at + part.shape[0]] = part

        tools.finish(joff, store)
        return carry

    lax.fori_loop(0, nj, block, 0)
    good = jnp.min(m.gd[...], axis=1, keepdims=True)
    if trans:
        m.good[...] = jnp.minimum(m.before[...], good)
    else:
        m.good[...] = jnp.broadcast_to(good, m.good.shape)
    send_block(nj - 1)
    if trans:
        def flag(t, carry):
            pltpu.make_async_remote_copy(
                src_ref=m.good.at[pl.ds(0, 1)], dst_ref=m.flags.at[me, pl.ds(0, 1)],
                send_sem=m.fsend, recv_sem=m.frecv,
                device_id=at(lax.rem(me + t, n)), device_id_type=pl.DeviceIdType.MESH,
            ).start()
            return carry

        lax.fori_loop(1, n, flag, 0)
        own_flag = pltpu.make_async_copy(m.good, m.flags.at[me], m.flag_sem)
        own_flag.start()
        own_flag.wait()
    sent_block(nj - 2)
    sent_block(nj - 1)
    others = m.o.at[:, pl.ds(0, rows * (n - 1))]
    pltpu.make_async_copy(others, others, m.recv_sem).wait()
    if trans:
        others = m.flags.at[pl.ds(0, n - 1), pl.ds(0, 1)]
        pltpu.make_async_copy(others, others, m.fsend).wait()
        pltpu.make_async_copy(others, others, m.frecv).wait()


def fused_attention(cid, n, ins, bias, before):
    trans = before is not None
    rows, res, chan = ins[0].shape
    scratch = stage_scratch(rows, res, chan)
    del scratch["ss"]
    scratch |= {
        "zs": pltpu.VMEM((2, JB, rows, chan), BF16),
        "send_sem": pltpu.SemaphoreType.DMA((2,)),
        "recv_sem": pltpu.SemaphoreType.DMA,
        "fetch_sem": pltpu.SemaphoreType.DMA,
        "own_sem": pltpu.SemaphoreType.DMA,
    }
    anywhere = pl.BlockSpec(memory_space=pl.ANY)
    outs = {"o": jax.ShapeDtypeStruct((rows, res, chan), BF16)}
    out_specs = [anywhere]
    names = stage_names(trans) + ["b"]
    args = list(ins) + [bias]
    in_specs = [VMEM] * len(ins) + [anywhere]
    if trans:
        names.append("before")
        args.append(before)
        in_specs.append(VMEM)
        outs["flags"] = jax.ShapeDtypeStruct((n, 8, 128), F32)
        out_specs.append(anywhere)
        scratch |= {
            "good": pltpu.VMEM((8, 128), F32),
            "fsend": pltpu.SemaphoreType.DMA,
            "frecv": pltpu.SemaphoreType.DMA,
            "flag_sem": pltpu.SemaphoreType.DMA,
        }
    else:
        outs["good"] = jax.ShapeDtypeStruct((8, 128), F32)
        out_specs.append(VMEM)
    return pl.pallas_call(
        functools.partial(fused_kernel, trans, n, names + list(outs) + list(scratch)),
        out_shape=list(outs.values()),
        in_specs=in_specs,
        out_specs=out_specs,
        scratch_shapes=list(scratch.values()),
        compiler_params=pltpu.CompilerParams(
            collective_id=cid, has_side_effects=True, vmem_limit_bytes=60 * 1024 * 1024
        ),
    )(*args)


def exchange_kernel(n, whole, z_ref, o_ref, send_sem, recv_sem, own_sem):
    rows = z_ref.shape[1]
    cut = lambda d: z_ref if whole else z_ref.at[pl.ds(pl.multiple_of(rows * d, rows), rows)]
    gy = n // 16
    me = lax.axis_index("gx") * gy + lax.axis_index("gy")
    at = lambda d: {"gx": d // gy, "gy": lax.rem(d, gy)}
    barrier = pltpu.get_barrier_semaphore()

    def greet(t, carry):
        pl.semaphore_signal(
            barrier, inc=1, device_id=at(lax.rem(me + t, n)), device_id_type=pl.DeviceIdType.MESH
        )
        return carry

    lax.fori_loop(1, n, greet, 0)
    mine = pl.ds(pl.multiple_of(rows * me, rows), rows)
    own = pltpu.make_async_copy(cut(me), o_ref.at[:, mine], own_sem)
    own.start()
    pl.semaphore_wait(barrier, n - 1)

    def copy(t, to, frm):
        return pltpu.make_async_remote_copy(
            src_ref=cut(to),
            dst_ref=o_ref.at[:, pl.ds(pl.multiple_of(rows * frm, rows), rows)],
            send_sem=send_sem.at[t], recv_sem=recv_sem.at[t],
            device_id=at(to), device_id_type=pl.DeviceIdType.MESH,
        )

    def send(t, carry):
        copy(t, lax.rem(me + t, n), me).start()
        return carry

    lax.fori_loop(1, n, send, 0)
    own.wait()

    def land(t, carry):
        copy(t, lax.rem(me + t, n), lax.rem(me + n - t, n)).wait_recv()
        copy(t, lax.rem(me + t, n), me).wait_send()
        return carry

    lax.fori_loop(1, n, land, 0)


def exchange(cid, n, z, whole=False):
    lead, rows, width = z.shape
    shape = (lead, n * rows, width) if whole else (rows, lead, width)
    return pl.pallas_call(
        functools.partial(exchange_kernel, n, whole),
        out_shape=jax.ShapeDtypeStruct(shape, BF16),
        in_specs=[pl.BlockSpec(memory_space=pl.ANY)],
        out_specs=pl.BlockSpec(memory_space=pl.ANY),
        scratch_shapes=[
            pltpu.SemaphoreType.DMA((n,)),
            pltpu.SemaphoreType.DMA((n,)),
            pltpu.SemaphoreType.DMA,
        ],
        compiler_params=pltpu.CompilerParams(collective_id=cid, has_side_effects=True),
    )(z)


def local(
    pair_in,
    residue_mask,
    norm_start,
    proj_start,
    gate_bias_start,
    bias_w_start,
    out_w_start,
    norm_end,
    proj_end,
    gate_bias_end,
    bias_w_end,
    out_w_end,
    norm_trans,
    trans_in,
    trans_bias,
    trans_out,
):
    rows, res, chan = pair_in.shape
    n = lax.axis_size(("gx", "gy"))
    row = lambda v: v.reshape(1, -1)
    mine = jnp.pad(residue_mask.astype(F32).reshape(1, rows), ((0, 7), (0, 128 - rows)))
    bias, normed = pair_bias(pair_in, row(norm_start), bias_w_start)
    bias, mask = gather(0, bias, mine)
    mask = mask[:, 0, :rows].reshape(res)
    mask = jnp.where(jnp.max(mask) > 0.5, mask, 1.0)
    mrow, mcol = mask.reshape(1, res), mask.reshape(res, 1)
    start = [pair_in, normed, proj_start, row(gate_bias_start), out_w_start, mrow, mcol]
    ends = [proj_end, row(gate_bias_end), out_w_end, mrow, mcol]
    ends += [row(norm_trans), trans_in, row(trans_bias), trans_out]

    def end_inputs(cols):
        bias, normed = pair_bias(cols, row(norm_end), bias_w_end)
        return [cols, normed] + ends, bias

    def safe(bias):
        cols = exchange(4, n, safe_attention(start, bias, False))
        ins, bias = end_inputs(cols)
        return exchange(5, n, safe_attention(ins, exchange(6, n, bias, True), True))

    cols, good = fused_attention(2, n, start, bias, None)
    ins, end_bias = end_inputs(cols)
    out, flags = fused_attention(3, n, ins, gather(1, end_bias), good)
    return lax.cond(jnp.min(flags[:, 0]) > 0.5, lambda b: out, safe, bias)


def solution(mesh):
    spec = P(("gx", "gy"), None, None)
    placed = (spec, P(("gx", "gy"))) + (P(),) * 14
    return jax.shard_map(local, mesh=mesh, in_specs=placed, out_specs=spec, check_vma=False)
```

```python
import functools
import types

import jax
import jax.numpy as jnp
from jax import lax
from jax.experimental import pallas as pl
from jax.experimental.pallas import tpu as pltpu
from jax.sharding import PartitionSpec as P

HEADS = 4
HEAD_DIM = 32
LOG2E = 1.4426950408889634
JB = 256
KB = 128
UNROLL = 4
F32 = jnp.float32
BF16 = jnp.bfloat16
NT = (((1,), (1,)), ((), ()))
TN = (((0,), (0,)), ((), ()))
VMEM = pl.BlockSpec(memory_space=pltpu.VMEM)


def layer_norm(t, gain):
    chan = t.shape[1]
    mean = jnp.dot(t, jnp.full((chan, chan), 1.0 / chan, BF16), preferred_element_type=F32)
    cent = t.astype(F32) - mean
    var = jnp.mean(cent * cent, axis=-1, keepdims=True)
    return (cent * lax.rsqrt(var + 1e-05) * gain).astype(BF16)


def bias_kernel(first, x_ref, g_ref, bw_ref, o_ref, a_ref):
    bwt = bw_ref[...].astype(F32).T.astype(BF16)
    gain = g_ref[...]
    for r in range(x_ref.shape[0]):
        a = layer_norm(x_ref[r], gain)
        a_ref[r] = a
        b = lax.dot_general(bwt, a, NT, preferred_element_type=F32) * LOG2E
        o_ref[:, r, :] = b[first : first + HEADS].astype(BF16)


def pair_bias(x, gain, bw, first):
    rows, res, chan = x.shape
    return pl.pallas_call(
        functools.partial(bias_kernel, first),
        out_shape=[
            jax.ShapeDtypeStruct((HEADS, rows, res), BF16),
            jax.ShapeDtypeStruct(x.shape, BF16),
        ],
        in_specs=[VMEM] * 3,
        out_specs=[VMEM] * 2,
    )(x, gain, bw)


ORDERS = (
    ("xyz", "yzx", "zxy", "xyz", "yzx"),
    ("yzx", "zxy", "xyz", "yzx", "xyz"),
)


def place():
    gx, gy = lax.axis_index("gx"), lax.axis_index("gy")
    return {
        "x": lax.rem(gx // 2, 4),
        "y": gy // 2,
        "z": 2 * lax.rem(gy, 2) + gx // 8,
        "c": lax.rem(gx, 2),
    }


def device(at):
    z_lo, z_hi = lax.rem(at["z"], 2), at["z"] // 2
    return {"gx": (z_lo * 4 + at["x"]) * 2 + at["c"], "gy": at["y"] * 2 + z_hi}


def shift(at, dim, by):
    return {**at, dim: lax.rem(at[dim] + by + 4, 4)}


def part(ref, lead, at, free, tail=()):
    z = "z" in free
    pick = lambda d: slice(None) if d in free else at[d]
    z_lo = slice(None) if z else lax.rem(at["z"], 2)
    z_hi = slice(None) if z else at["z"] // 2
    return ref.at[lead + (z_lo, pick("x"), at["c"], pick("y"), z_hi) + tail]


def gather_kernel(n_out, *refs):
    ins, outs = refs[:n_out], refs[n_out : 2 * n_out]
    ring_send, ring_recv, pair_send, pair_recv, own_sem = refs[2 * n_out :]
    me = place()
    barrier = pltpu.get_barrier_semaphore()
    sib = {**me, "c": 1 - me["c"]}
    partners = [shift(me, d, by) for d in "xyz" for by in (1, -1, 2)] + [sib]
    for at in partners:
        pl.semaphore_signal(barrier, inc=1, device_id=device(at), device_id_type=pl.DeviceIdType.MESH)
    pl.semaphore_wait(barrier, len(partners))

    def items(core):
        half = outs[0].shape[-1] // 2
        got = []
        for h in range(HEADS):
            got.append((h, ins[0].at[h], functools.partial(part, outs[0], (h,)), half))
        if n_out == 2:
            got.append((HEADS, ins[1], functools.partial(part, outs[1], ()), 0))
        return got

    def copy(src, dst, sems, idx, to):
        return pltpu.make_async_remote_copy(
            src_ref=src, dst_ref=dst, send_sem=sems[0].at[idx], recv_sem=sems[1].at[idx],
            device_id=device(to), device_id_type=pl.DeviceIdType.MESH,
        )

    ring, pair = (ring_send, ring_recv), (pair_send, pair_recv)

    def run(core):
        at = {**me, "c": core}
        other = {**me, "c": 1 - core}
        todo = items(core)
        sends = []

        def step0(p, idx, own, sets, half):
            d, free = ORDERS[core][idx][p], ORDERS[core][idx][:p]
            src = sets(at, free)
            for k, by in enumerate((1, -1)):
                c = copy(own if p == 0 else src, src, ring, (idx, p, k), shift(at, d, by))
                c.start()
                sends.append(c)
            if p == 0:
                c = copy(own, src, ring, (idx, p, 2), shift(at, d, 2))
                c.start()
                sends.append(c)

        def step1(p, idx, own, sets, half):
            d, free = ORDERS[core][idx][p], ORDERS[core][idx][:p]
            for k, by in enumerate((1, -1)):
                got = sets(shift(at, d, -by), free)
                copy(got, got, ring, (idx, p, k), shift(at, d, by)).wait_recv()
                if p == 0:
                    continue
                if half:
                    tail = (slice(None), pl.ds(k * half, half))
                    piece = sets(shift(at, d, -by), free, tail)
                elif k == 0:
                    piece = got
                else:
                    continue
                c = copy(piece, piece, ring, (idx, p, 2 + k), shift(at, d, by))
                c.start()
                sends.append(c)

        def step2(p, idx, own, sets, half):
            d, free = ORDERS[core][idx][p], ORDERS[core][idx][:p]
            for k, by in enumerate((1, -1)):
                if half and p > 0:
                    tail = (slice(None), pl.ds(k * half, half))
                    piece = sets(shift(at, d, 2), free, tail)
                elif k == 0:
                    piece = sets(shift(at, d, 2), free)
                else:
                    continue
                copy(piece, piece, ring, (idx, p, 2 + k), shift(at, d, by)).wait_recv()

        def across(idx, sets, hop):
            d, free = ORDERS[core][idx][2], ORDERS[core][idx][:2]
            piece = sets(shift(at, d, hop), free)
            c = copy(piece, piece, pair, (idx, hop), other)
            c.start()
            sends.append(c)

        own_copies = []
        for idx, own, sets, half in todo:
            step0(0, idx, own, sets, half)
            mine = pltpu.make_async_copy(own, sets(at, ""), own_sem.at[idx])
            mine.start()
            own_copies.append(mine)
        for p in range(3):
            for t in todo:
                step1(p, *t)
                if p == 2:
                    for hop in (1, 3):
                        across(t[0], t[2], hop)
            for i, t in enumerate(todo):
                if p == 0:
                    own_copies[i].wait()
                step2(p, *t)
                if p < 2:
                    step0(p + 1, *t)
                if p == 1:
                    across(t[0], t[2], 0)
                if p == 2:
                    across(t[0], t[2], 2)
        for idx, own, sets, half in todo:
            d, free = ORDERS[1 - core][idx][2], ORDERS[1 - core][idx][:2]
            for hop in range(4):
                piece = sets(shift(other, d, hop), free)
                copy(piece, piece, pair, (idx, hop), other).wait_recv()
        for c in sends:
            c.wait_send()

    for core in range(2):
        pl.when(me["c"] == core)(functools.partial(run, core))


def gather(cid, bias, *mask):
    heads, rows, res = bias.shape
    grid = (2, 4, 2, 4, 2)
    outs = [jax.ShapeDtypeStruct((heads,) + grid + (rows, res), BF16)]
    if mask:
        outs.append(jax.ShapeDtypeStruct(grid + mask[0].shape, F32))
    n = len(outs)
    got = pl.pallas_call(
        functools.partial(gather_kernel, n),
        out_shape=outs,
        in_specs=[VMEM] * n,
        out_specs=[pl.BlockSpec(memory_space=pl.ANY)] * n,
        scratch_shapes=[
            pltpu.SemaphoreType.DMA((5, 3, 4)),
            pltpu.SemaphoreType.DMA((5, 3, 4)),
            pltpu.SemaphoreType.DMA((5, 4)),
            pltpu.SemaphoreType.DMA((5, 4)),
            pltpu.SemaphoreType.DMA((5,)),
        ],
        compiler_params=pltpu.CompilerParams(collective_id=cid, has_side_effects=True),
    )(bias, *mask)
    full = got[0].reshape(heads, -1, res)
    return (full, got[1].reshape((-1,) + mask[0].shape)) if mask else full


def stage_tools(trans, m):
    rows, res, chan = m.x.shape
    groups = rows // 4
    nk = res // KB
    tasks = groups * HEADS
    t = types.SimpleNamespace()

    def eye():
        i = lax.broadcasted_iota(jnp.int32, (KB, KB), 0)
        j = lax.broadcasted_iota(jnp.int32, (KB, KB), 1)
        return (i == j).astype(F32).astype(BF16)

    def project_all():
        w = m.w[...].astype(F32)
        wqt = w[:, :chan].T
        for s in range(4):
            cut = chan - 32 * s
            wk = w[:, chan : 2 * chan]
            m.wk[s] = (pltpu.roll(wk, 32 * s, 1) if s else wk).astype(BF16)
            m.wq[s] = (jnp.concatenate([wqt[cut:], wqt[:cut]], axis=0) if s else wqt).astype(BF16)
        wvt = w[:, 2 * chan : 3 * chan].T.astype(BF16)
        wgt = w[:, 3 * chan :].T.astype(BF16)
        gb = m.gb[...].T
        mrow = m.mrow[...]
        lane = lax.broadcasted_iota(jnp.int32, (1, chan), 1) // HEAD_DIM

        def project(r, carry):
            s = lax.rem(r, 4)
            grp = r // 4
            a = m.a[r]
            kk = jnp.dot(a, m.wk[s], preferred_element_type=F32).astype(BF16)
            qt = (
                lax.dot_general(m.wq[s], a, NT, preferred_element_type=F32)
                * (HEAD_DIM**-0.5 * LOG2E)
            ).astype(BF16)
            vt = lax.dot_general(wvt, a, NT, preferred_element_type=F32) * mrow
            m.gt[r] = jax.nn.sigmoid(lax.dot_general(wgt, a, NT, preferred_element_type=F32) + gb)
            for h in range(HEADS):
                slot = lax.rem(h + s, 4)
                m.km[r, h] = kk * (lane == slot).astype(F32).astype(BF16)
                m.vx[r, h, :HEAD_DIM] = vt[HEAD_DIM * h : HEAD_DIM * (h + 1)].astype(BF16)
                m.vx[r, h, HEAD_DIM:] = jnp.broadcast_to(mrow, (16, res)).astype(BF16)
            for u in range(4):
                hh = lax.rem(u - s + 4, 4)
                m.qs[grp, hh, pl.ds(32 * u, 32)] = qt[32 * u : 32 * (u + 1)]
            return carry

        lax.fori_loop(0, rows, project, 0)

    def turn_bias(b_ref):
        for h in range(HEADS):
            for kb in range(nk):
                sl = slice(KB * kb, KB * (kb + 1))
                m.bt[h, sl] = b_ref[h, :, sl].T

    def head_slice(h):
        return pl.ds(pl.multiple_of(HEAD_DIM * h, HEAD_DIM), HEAD_DIM)

    def fast_heads(joff):
        one = eye()

        def of(k):
            return k // HEADS, lax.rem(k, HEADS)

        def weights_step(k, kb, pp):
            grp, h = of(k)
            sl = slice(KB * kb, KB * (kb + 1))
            rhs = jnp.concatenate([m.bt[h, sl], m.qs[grp, h, :, pl.ds(joff, JB)]], axis=0)
            lhs = jnp.concatenate(
                [jnp.concatenate([one, m.km[grp * 4 + r, h, sl]], axis=1) for r in range(4)], axis=0
            )
            p4 = jnp.exp2(jnp.dot(lhs, rhs, preferred_element_type=F32)).astype(BF16)
            for r in range(4):
                pp[r, sl] = p4[KB * r : KB * (r + 1)]

        def mix_step(k, r, pp):
            grp, h = of(k)
            oe = jnp.dot(m.vx[grp * 4 + r, h], pp[r], preferred_element_type=F32)
            den = oe[HEAD_DIM : HEAD_DIM + 1]
            m.gd[...] = jnp.where((den > 2.0**-60) & (den < 2.0**100), m.gd[...], 0.0)
            m.ot[grp * 4 + r, head_slice(h)] = oe[:HEAD_DIM] / den

        def both(k, new, old):
            for kb in range(nk):
                weights_step(k, kb, new)
                if kb % 2:
                    mix_step(k - 1, kb // 2, old)

        for kb in range(nk):
            weights_step(0, kb, m.pa)

        def pair(i, carry):
            both(2 * i + 1, m.pb, m.pa)
            both(2 * i + 2, m.pa, m.pb)
            return carry

        lax.fori_loop(0, tasks // 2 - 1, pair, 0)
        both(tasks - 1, m.pb, m.pa)
        for r in range(4):
            mix_step(tasks - 1, r, m.pb)

    def safe_heads(joff):
        one = eye()

        def row_head(it, carry):
            row, h = it // HEADS, lax.rem(it, HEADS)
            q = m.qs[row // 4, h, :, pl.ds(joff, JB)]

            def scores(kb, carry):
                ks = pl.ds(pl.multiple_of(kb * KB, KB), KB)
                rhs = jnp.concatenate([m.bt[h, ks], q], axis=0)
                lhs = jnp.concatenate([one, m.km[row, h, ks]], axis=1)
                s1 = jnp.dot(lhs, rhs, preferred_element_type=F32)
                s1 = jnp.where(m.mcol[ks] > 0.5, s1, -1e30)
                m.ss[ks] = s1
                return jnp.maximum(carry, jnp.max(s1, axis=0, keepdims=True))

            top = lax.fori_loop(0, nk, scores, jnp.full((1, JB), -1e30, F32))

            def weights(kb, carry):
                ks = pl.ds(pl.multiple_of(kb * KB, KB), KB)
                m.pa[0, ks] = jnp.exp2(m.ss[ks] - top).astype(BF16)
                return carry

            lax.fori_loop(0, nk, weights, 0)
            oe = jnp.dot(m.vx[row, h], m.pa[0], preferred_element_type=F32)
            m.ot[row, head_slice(h)] = oe[:HEAD_DIM] / oe[HEAD_DIM : HEAD_DIM + 1]
            return carry

        lax.fori_loop(0, rows * HEADS, row_head, 0)

    def finish(joff, store):
        def row(r):
            gated = (m.ot[r] * m.gt[r, :, pl.ds(joff, JB)]).T.astype(BF16)
            z = m.x[r, pl.ds(joff, JB)].astype(F32) + jnp.dot(
                gated, m.ow[...], preferred_element_type=F32
            )
            z = z.astype(BF16)
            if trans:
                zf = z.astype(F32)
                a = layer_norm(z, m.ng[...])
                hid = jnp.dot(a, m.ti[...], preferred_element_type=F32) + m.tb[...]
                hid = jnp.maximum(hid, 0.0).astype(BF16)
                z = (zf + jnp.dot(hid, m.to[...], preferred_element_type=F32)).astype(BF16)
            m.zz[r] = z

        def some(i, carry):
            for r in range(UNROLL):
                row(UNROLL * i + r)
            return carry

        lax.fori_loop(0, rows // UNROLL, some, 0)
        span = JB // rows
        out_row = lax.broadcasted_iota(jnp.int32, (JB, JB), 0)
        in_row = lax.broadcasted_iota(jnp.int32, (JB, JB), 1)
        perm = (in_row == lax.rem(out_row, rows) * span + out_row // rows).astype(F32).astype(BF16)
        for q in range(rows // 2):
            cols = [
                jnp.concatenate([m.zz[r, span * n : span * (n + 1)] for r in range(rows)], axis=0)
                for n in (2 * q, 2 * q + 1)
            ]
            moved = jnp.dot(perm, jnp.concatenate(cols, axis=1), preferred_element_type=F32)
            for n in range(2):
                part = moved[:, chan * n : chan * (n + 1)]
                store(span * (2 * q + n), part.reshape(span, rows, chan).astype(BF16))

    return types.SimpleNamespace(
        project_all=project_all, turn_bias=turn_bias, fast_heads=fast_heads,
        safe_heads=safe_heads, finish=finish,
    )


def stage_names(trans):
    names = ["x", "a", "w", "gb", "ow", "mrow"]
    return names + (["ng", "ti", "tb", "to"] if trans else [])


def stage_scratch(rows, res, chan):
    return {
        "km": pltpu.VMEM((rows, HEADS, res, chan), BF16),
        "qs": pltpu.VMEM((rows // 4, HEADS, chan, res), BF16),
        "vx": pltpu.VMEM((rows, HEADS, HEAD_DIM + 16, res), BF16),
        "gt": pltpu.VMEM((rows, chan, res), F32),
        "bt": pltpu.VMEM((HEADS, res, JB), BF16),
        "pa": pltpu.VMEM((4, res, JB), BF16),
        "pb": pltpu.VMEM((4, res, JB), BF16),
        "ot": pltpu.VMEM((rows, chan, JB), F32),
        "wk": pltpu.VMEM((4, chan, chan), BF16),
        "wq": pltpu.VMEM((4, chan, chan), BF16),
        "gd": pltpu.VMEM((1, JB), F32),
        "zz": pltpu.VMEM((rows, JB, chan), BF16),
        "bs": pltpu.VMEM((HEADS, JB, res), BF16),
        "ss": pltpu.VMEM((res, JB), F32),
    }


def safe_kernel(trans, names, *refs):
    m = types.SimpleNamespace(**dict(zip(names, refs)))
    tools = stage_tools(trans, m)

    @pl.when(pl.program_id(0) == 0)
    def _():
        tools.project_all()

    joff = pl.multiple_of(pl.program_id(0) * JB, JB)
    tools.turn_bias(m.b)
    tools.safe_heads(joff)

    def store(at, part):
        m.o[at : at + part.shape[0]] = part

    tools.finish(joff, store)


def safe_attention(ins, bias, trans):
    rows, res, chan = ins[0].shape
    scratch = stage_scratch(rows, res, chan)
    names = stage_names(trans) + ["mcol", "b", "o"] + list(scratch)
    full = lambda a: pl.BlockSpec(a.shape, lambda j, n=a.ndim: (0,) * n)
    return pl.pallas_call(
        functools.partial(safe_kernel, trans, names),
        grid=(res // JB,),
        out_shape=jax.ShapeDtypeStruct((res, rows, chan), BF16),
        in_specs=[full(a) for a in ins] + [pl.BlockSpec((HEADS, JB, res), lambda j: (0, j, 0))],
        out_specs=pl.BlockSpec((JB, rows, chan), lambda j: (j, 0, 0)),
        scratch_shapes=list(scratch.values()),
        compiler_params=pltpu.CompilerParams(
            dimension_semantics=("arbitrary",), vmem_limit_bytes=60 * 1024 * 1024
        ),
    )(*ins, bias)


def fused_kernel(trans, n, names, *refs):
    m = types.SimpleNamespace(**dict(zip(names, refs)))
    tools = stage_tools(trans, m)
    rows, res, chan = m.x.shape
    nj = res // JB
    per = JB // rows
    gy = n // 16
    gx_me, gy_me = lax.axis_index("gx"), lax.axis_index("gy")
    me = gx_me * gy + gy_me
    at = lambda d: {"gx": d // gy, "gy": lax.rem(d, gy)}
    barrier = pltpu.get_barrier_semaphore()
    cols = [lax.rem(gy_me + b, gy) for b in range(gy)]

    def everyone(act):
        def ring(a, carry):
            for col in cols:
                act({"gx": lax.rem(gx_me + a, n // gy), "gy": col})
            return carry

        for col in cols[1:]:
            act({"gx": gx_me, "gy": col})
        lax.fori_loop(1, n // gy, ring, 0)

    def greet(to):
        pl.semaphore_signal(barrier, inc=1, device_id=to, device_id_type=pl.DeviceIdType.MESH)

    everyone(greet)

    def block_of(t):
        return lax.rem(t + me, nj)

    def fetch(t):
        return pltpu.make_async_copy(
            m.b.at[:, pl.ds(pl.multiple_of(block_of(t) * JB, JB), JB)], m.bs, m.fetch_sem
        )

    mine = pl.ds(pl.multiple_of(rows * me, rows), rows)

    def send_block(t):
        def send(k, carry):
            i = lax.rem(k + me // nj, per)
            to = block_of(t) * per + i
            src = m.zs.at[lax.rem(t, 2), pl.ds(pl.multiple_of(i * rows, rows), rows)]

            @pl.when(to != me)
            def _():
                pltpu.make_async_remote_copy(
                    src_ref=src, dst_ref=m.o.at[:, mine],
                    send_sem=m.send_sem.at[lax.rem(t, 2)], recv_sem=m.recv_sem,
                    device_id=at(to), device_id_type=pl.DeviceIdType.MESH,
                ).start()

            @pl.when(to == me)
            def _():
                pltpu.make_async_copy(src, m.o.at[:, mine], m.own_sem).start()

            return carry

        lax.fori_loop(0, per, send, 0)

    def sent_block(t):
        here = block_of(t) == me // per
        slot = lax.rem(t, 2)

        def sent(count):
            piece = m.zs.at[slot, pl.ds(0, count * rows)]
            pltpu.make_async_copy(piece, piece, m.send_sem.at[slot]).wait()

        @pl.when(here)
        def _():
            sent(per - 1)
            pltpu.make_async_copy(m.zs.at[slot, pl.ds(0, rows)], m.o.at[:, mine], m.own_sem).wait()

        @pl.when(jnp.logical_not(here))
        def _():
            sent(per)

    fetch(0).start()
    tools.project_all()
    m.gd[...] = jnp.ones_like(m.gd)
    pl.semaphore_wait(barrier, n - 1)

    def block(t, carry):
        joff = pl.multiple_of(block_of(t) * JB, JB)
        fetch(t).wait()
        tools.turn_bias(m.bs)

        @pl.when(t > 0)
        def _():
            send_block(t - 1)

        @pl.when(t < nj - 1)
        def _():
            fetch(t + 1).start()

        tools.fast_heads(joff)

        @pl.when(t > 1)
        def _():
            sent_block(t - 2)

        def store(at, part):
            m.zs[lax.rem(t, 2), at : at + part.shape[0]] = part

        tools.finish(joff, store)
        return carry

    lax.fori_loop(0, nj, block, 0)
    good = jnp.min(m.gd[...], axis=1, keepdims=True)
    if trans:
        m.good[...] = jnp.minimum(m.before[...], good)
    else:
        m.good[...] = jnp.broadcast_to(good, m.good.shape)
    send_block(nj - 1)
    if trans:
        def flag(to):
            pltpu.make_async_remote_copy(
                src_ref=m.good.at[pl.ds(0, 1)], dst_ref=m.flags.at[me, pl.ds(0, 1)],
                send_sem=m.fsend, recv_sem=m.frecv,
                device_id=to, device_id_type=pl.DeviceIdType.MESH,
            ).start()

        everyone(flag)
        own_flag = pltpu.make_async_copy(m.good, m.flags.at[me], m.flag_sem)
        own_flag.start()
        own_flag.wait()
    sent_block(nj - 2)
    sent_block(nj - 1)
    others = m.o.at[:, pl.ds(0, rows * (n - 1))]
    pltpu.make_async_copy(others, others, m.recv_sem).wait()
    if trans:
        others = m.flags.at[pl.ds(0, n - 1), pl.ds(0, 1)]
        pltpu.make_async_copy(others, others, m.fsend).wait()
        pltpu.make_async_copy(others, others, m.frecv).wait()


def fused_attention(cid, n, ins, bias, before):
    trans = before is not None
    rows, res, chan = ins[0].shape
    scratch = stage_scratch(rows, res, chan)
    del scratch["ss"]
    scratch |= {
        "zs": pltpu.VMEM((2, JB, rows, chan), BF16),
        "send_sem": pltpu.SemaphoreType.DMA((2,)),
        "recv_sem": pltpu.SemaphoreType.DMA,
        "fetch_sem": pltpu.SemaphoreType.DMA,
        "own_sem": pltpu.SemaphoreType.DMA,
    }
    anywhere = pl.BlockSpec(memory_space=pl.ANY)
    outs = {"o": jax.ShapeDtypeStruct((rows, res, chan), BF16)}
    out_specs = [anywhere]
    names = stage_names(trans) + ["b"]
    args = list(ins) + [bias]
    in_specs = [VMEM] * len(ins) + [anywhere]
    if trans:
        names.append("before")
        args.append(before)
        in_specs.append(VMEM)
        outs["flags"] = jax.ShapeDtypeStruct((n, 8, 128), F32)
        out_specs.append(anywhere)
        scratch |= {
            "good": pltpu.VMEM((8, 128), F32),
            "fsend": pltpu.SemaphoreType.DMA,
            "frecv": pltpu.SemaphoreType.DMA,
            "flag_sem": pltpu.SemaphoreType.DMA,
        }
    else:
        outs["good"] = jax.ShapeDtypeStruct((8, 128), F32)
        out_specs.append(VMEM)
    return pl.pallas_call(
        functools.partial(fused_kernel, trans, n, names + list(outs) + list(scratch)),
        out_shape=list(outs.values()),
        in_specs=in_specs,
        out_specs=out_specs,
        scratch_shapes=list(scratch.values()),
        compiler_params=pltpu.CompilerParams(
            collective_id=cid, has_side_effects=True, vmem_limit_bytes=60 * 1024 * 1024
        ),
    )(*args)


def exchange_kernel(n, whole, z_ref, o_ref, send_sem, recv_sem, own_sem):
    rows = z_ref.shape[1]
    cut = lambda d: z_ref if whole else z_ref.at[pl.ds(pl.multiple_of(rows * d, rows), rows)]
    gy = n // 16
    me = lax.axis_index("gx") * gy + lax.axis_index("gy")
    at = lambda d: {"gx": d // gy, "gy": lax.rem(d, gy)}
    barrier = pltpu.get_barrier_semaphore()

    def greet(t, carry):
        pl.semaphore_signal(
            barrier, inc=1, device_id=at(lax.rem(me + t, n)), device_id_type=pl.DeviceIdType.MESH
        )
        return carry

    lax.fori_loop(1, n, greet, 0)
    mine = pl.ds(pl.multiple_of(rows * me, rows), rows)
    own = pltpu.make_async_copy(cut(me), o_ref.at[:, mine], own_sem)
    own.start()
    pl.semaphore_wait(barrier, n - 1)

    def copy(t, to, frm):
        return pltpu.make_async_remote_copy(
            src_ref=cut(to),
            dst_ref=o_ref.at[:, pl.ds(pl.multiple_of(rows * frm, rows), rows)],
            send_sem=send_sem.at[t], recv_sem=recv_sem.at[t],
            device_id=at(to), device_id_type=pl.DeviceIdType.MESH,
        )

    def send(t, carry):
        copy(t, lax.rem(me + t, n), me).start()
        return carry

    lax.fori_loop(1, n, send, 0)
    own.wait()

    def land(t, carry):
        copy(t, lax.rem(me + t, n), lax.rem(me + n - t, n)).wait_recv()
        copy(t, lax.rem(me + t, n), me).wait_send()
        return carry

    lax.fori_loop(1, n, land, 0)


def exchange(cid, n, z, whole=False):
    lead, rows, width = z.shape
    shape = (lead, n * rows, width) if whole else (rows, lead, width)
    return pl.pallas_call(
        functools.partial(exchange_kernel, n, whole),
        out_shape=jax.ShapeDtypeStruct(shape, BF16),
        in_specs=[pl.BlockSpec(memory_space=pl.ANY)],
        out_specs=pl.BlockSpec(memory_space=pl.ANY),
        scratch_shapes=[
            pltpu.SemaphoreType.DMA((n,)),
            pltpu.SemaphoreType.DMA((n,)),
            pltpu.SemaphoreType.DMA,
        ],
        compiler_params=pltpu.CompilerParams(collective_id=cid, has_side_effects=True),
    )(z)


def local(
    pair_in,
    residue_mask,
    norm_start,
    proj_start,
    gate_bias_start,
    bias_w_start,
    out_w_start,
    norm_end,
    proj_end,
    gate_bias_end,
    bias_w_end,
    out_w_end,
    norm_trans,
    trans_in,
    trans_bias,
    trans_out,
):
    rows, res, chan = pair_in.shape
    n = lax.axis_size(("gx", "gy"))
    row = lambda v: v.reshape(1, -1)
    mine = jnp.pad(residue_mask.astype(F32).reshape(1, rows), ((0, 7), (0, 128 - rows)))
    bias_w = jnp.concatenate([bias_w_start, bias_w_end], axis=1)
    bias_w = jnp.pad(bias_w, ((0, 0), (0, 128 - 2 * HEADS)))
    bias, normed = pair_bias(pair_in, row(norm_start), bias_w, 0)
    bias, mask = gather(0, bias, mine)
    mask = mask[:, 0, :rows].reshape(res)
    mask = jnp.where(jnp.max(mask) > 0.5, mask, 1.0)
    mrow = mask.reshape(1, res)
    start = [pair_in, normed, proj_start, row(gate_bias_start), out_w_start, mrow]
    ends = [proj_end, row(gate_bias_end), out_w_end, mrow]
    ends += [row(norm_trans), trans_in, row(trans_bias), trans_out]

    def end_inputs(cols):
        bias, normed = pair_bias(cols, row(norm_end), bias_w, HEADS)
        return [cols, normed] + ends, bias

    def safe(bias):
        mcol = [mask.reshape(res, 1)]
        cols = exchange(4, n, safe_attention(start + mcol, bias, False))
        ins, bias = end_inputs(cols)
        return exchange(5, n, safe_attention(ins + mcol, exchange(6, n, bias, True), True))

    cols, good = fused_attention(2, n, start, bias, None)
    ins, end_bias = end_inputs(cols)
    out, flags = fused_attention(3, n, ins, gather(1, end_bias), good)
    return lax.cond(jnp.min(flags[:, 0]) > 0.5, lambda b: out, safe, bias)


def solution(mesh):
    spec = P(("gx", "gy"), None, None)
    placed = (spec, P(("gx", "gy"))) + (P(),) * 14
    return jax.shard_map(local, mesh=mesh, in_specs=placed, out_specs=spec, check_vma=False)
```

```python
import functools
import types

import jax
import jax.numpy as jnp
from jax import lax
from jax.experimental import pallas as pl
from jax.experimental.pallas import tpu as pltpu
from jax.sharding import PartitionSpec as P

HEADS = 4
HEAD_DIM = 32
LOG2E = 1.4426950408889634
JB = 256
KB = 128
UNROLL = 8
F32 = jnp.float32
BF16 = jnp.bfloat16
NT = (((1,), (1,)), ((), ()))
TN = (((0,), (0,)), ((), ()))
VMEM = pl.BlockSpec(memory_space=pltpu.VMEM)


def layer_norm(t, gain):
    chan = t.shape[1]
    mean = jnp.dot(t, jnp.full((chan, chan), 1.0 / chan, BF16), preferred_element_type=F32)
    cent = t.astype(F32) - mean
    var = jnp.mean(cent * cent, axis=-1, keepdims=True)
    return (cent * lax.rsqrt(var + 1e-05) * gain).astype(BF16)


def bias_kernel(first, x_ref, g_ref, bw_ref, o_ref, a_ref):
    bwt = bw_ref[...].astype(F32).T.astype(BF16)
    gain = g_ref[...]
    for r in range(x_ref.shape[0]):
        a = layer_norm(x_ref[r], gain)
        a_ref[r] = a
        b = lax.dot_general(bwt, a, NT, preferred_element_type=F32) * LOG2E
        o_ref[:, r, :] = b[first : first + HEADS].astype(BF16)


def pair_bias(x, gain, bw, first):
    rows, res, chan = x.shape
    return pl.pallas_call(
        functools.partial(bias_kernel, first),
        out_shape=[
            jax.ShapeDtypeStruct((HEADS, rows, res), BF16),
            jax.ShapeDtypeStruct(x.shape, BF16),
        ],
        in_specs=[VMEM] * 3,
        out_specs=[VMEM] * 2,
    )(x, gain, bw)


ORDERS = (
    ("xyz", "yzx", "zxy", "xyz", "yzx"),
    ("yzx", "zxy", "xyz", "yzx", "xyz"),
)


def place():
    gx, gy = lax.axis_index("gx"), lax.axis_index("gy")
    return {
        "x": lax.rem(gx // 2, 4),
        "y": gy // 2,
        "z": 2 * lax.rem(gy, 2) + gx // 8,
        "c": lax.rem(gx, 2),
    }


def device(at):
    z_lo, z_hi = lax.rem(at["z"], 2), at["z"] // 2
    return {"gx": (z_lo * 4 + at["x"]) * 2 + at["c"], "gy": at["y"] * 2 + z_hi}


def shift(at, dim, by):
    return {**at, dim: lax.rem(at[dim] + by + 4, 4)}


def part(ref, lead, at, free, tail=()):
    z = "z" in free
    pick = lambda d: slice(None) if d in free else at[d]
    z_lo = slice(None) if z else lax.rem(at["z"], 2)
    z_hi = slice(None) if z else at["z"] // 2
    return ref.at[lead + (z_lo, pick("x"), at["c"], pick("y"), z_hi) + tail]


def gather_kernel(n_out, *refs):
    ins, outs = refs[:n_out], refs[n_out : 2 * n_out]
    ring_send, ring_recv, pair_send, pair_recv, own_sem = refs[2 * n_out :]
    me = place()
    barrier = pltpu.get_barrier_semaphore()
    sib = {**me, "c": 1 - me["c"]}
    partners = [shift(me, d, by) for d in "xyz" for by in (1, -1, 2)] + [sib]
    for at in partners:
        pl.semaphore_signal(barrier, inc=1, device_id=device(at), device_id_type=pl.DeviceIdType.MESH)
    pl.semaphore_wait(barrier, len(partners))

    def items(core):
        half = outs[0].shape[-1] // 2
        got = []
        for h in range(HEADS):
            got.append((h, ins[0].at[h], functools.partial(part, outs[0], (h,)), half))
        if n_out == 2:
            got.append((HEADS, ins[1], functools.partial(part, outs[1], ()), 0))
        return got

    def copy(src, dst, sems, idx, to):
        return pltpu.make_async_remote_copy(
            src_ref=src, dst_ref=dst, send_sem=sems[0].at[idx], recv_sem=sems[1].at[idx],
            device_id=device(to), device_id_type=pl.DeviceIdType.MESH,
        )

    ring, pair = (ring_send, ring_recv), (pair_send, pair_recv)

    def run(core):
        at = {**me, "c": core}
        other = {**me, "c": 1 - core}
        todo = items(core)
        sends = []

        def step0(p, idx, own, sets, half):
            d, free = ORDERS[core][idx][p], ORDERS[core][idx][:p]
            src = sets(at, free)
            for k, by in enumerate((1, -1)):
                c = copy(own if p == 0 else src, src, ring, (idx, p, k), shift(at, d, by))
                c.start()
                sends.append(c)
            if p == 0:
                c = copy(own, src, ring, (idx, p, 2), shift(at, d, 2))
                c.start()
                sends.append(c)

        def step1(p, idx, own, sets, half):
            d, free = ORDERS[core][idx][p], ORDERS[core][idx][:p]
            for k, by in enumerate((1, -1)):
                got = sets(shift(at, d, -by), free)
                copy(got, got, ring, (idx, p, k), shift(at, d, by)).wait_recv()
                if p == 0:
                    continue
                if half:
                    tail = (slice(None), pl.ds(k * half, half))
                    piece = sets(shift(at, d, -by), free, tail)
                elif k == 0:
                    piece = got
                else:
                    continue
                c = copy(piece, piece, ring, (idx, p, 2 + k), shift(at, d, by))
                c.start()
                sends.append(c)

        def step2(p, idx, own, sets, half):
            d, free = ORDERS[core][idx][p], ORDERS[core][idx][:p]
            for k, by in enumerate((1, -1)):
                if half and p > 0:
                    tail = (slice(None), pl.ds(k * half, half))
                    piece = sets(shift(at, d, 2), free, tail)
                elif k == 0:
                    piece = sets(shift(at, d, 2), free)
                else:
                    continue
                copy(piece, piece, ring, (idx, p, 2 + k), shift(at, d, by)).wait_recv()

        def across(idx, sets, hop):
            d, free = ORDERS[core][idx][2], ORDERS[core][idx][:2]
            piece = sets(shift(at, d, hop), free)
            c = copy(piece, piece, pair, (idx, hop), other)
            c.start()
            sends.append(c)

        own_copies = []
        for idx, own, sets, half in todo:
            step0(0, idx, own, sets, half)
            mine = pltpu.make_async_copy(own, sets(at, ""), own_sem.at[idx])
            mine.start()
            own_copies.append(mine)
        for p in range(3):
            for t in todo:
                step1(p, *t)
                if p == 2:
                    for hop in (1, 3):
                        across(t[0], t[2], hop)
            for i, t in enumerate(todo):
                if p == 0:
                    own_copies[i].wait()
                step2(p, *t)
                if p < 2:
                    step0(p + 1, *t)
                if p == 1:
                    across(t[0], t[2], 0)
                if p == 2:
                    across(t[0], t[2], 2)
        for idx, own, sets, half in todo:
            d, free = ORDERS[1 - core][idx][2], ORDERS[1 - core][idx][:2]
            for hop in range(4):
                piece = sets(shift(other, d, hop), free)
                copy(piece, piece, pair, (idx, hop), other).wait_recv()
        for c in sends:
            c.wait_send()

    for core in range(2):
        pl.when(me["c"] == core)(functools.partial(run, core))


def gather(cid, bias, *mask):
    heads, rows, res = bias.shape
    grid = (2, 4, 2, 4, 2)
    outs = [jax.ShapeDtypeStruct((heads,) + grid + (rows, res), BF16)]
    if mask:
        outs.append(jax.ShapeDtypeStruct(grid + mask[0].shape, F32))
    n = len(outs)
    got = pl.pallas_call(
        functools.partial(gather_kernel, n),
        out_shape=outs,
        in_specs=[VMEM] * n,
        out_specs=[pl.BlockSpec(memory_space=pl.ANY)] * n,
        scratch_shapes=[
            pltpu.SemaphoreType.DMA((5, 3, 4)),
            pltpu.SemaphoreType.DMA((5, 3, 4)),
            pltpu.SemaphoreType.DMA((5, 4)),
            pltpu.SemaphoreType.DMA((5, 4)),
            pltpu.SemaphoreType.DMA((5,)),
        ],
        compiler_params=pltpu.CompilerParams(collective_id=cid, has_side_effects=True),
    )(bias, *mask)
    full = got[0].reshape(heads, -1, res)
    return (full, got[1].reshape((-1,) + mask[0].shape)) if mask else full


def stage_tools(trans, m):
    rows, res, chan = m.x.shape
    groups = rows // 4
    nk = res // KB
    tasks = groups * HEADS
    t = types.SimpleNamespace()

    def eye():
        i = lax.broadcasted_iota(jnp.int32, (KB, KB), 0)
        j = lax.broadcasted_iota(jnp.int32, (KB, KB), 1)
        return (i == j).astype(F32).astype(BF16)

    def project_all():
        w = m.w[...].astype(F32)
        wqt = w[:, :chan].T
        for s in range(4):
            cut = chan - 32 * s
            wk = w[:, chan : 2 * chan]
            m.wk[s] = (pltpu.roll(wk, 32 * s, 1) if s else wk).astype(BF16)
            m.wq[s] = (jnp.concatenate([wqt[cut:], wqt[:cut]], axis=0) if s else wqt).astype(BF16)
        wvt = w[:, 2 * chan : 3 * chan].T.astype(BF16)
        wgt = w[:, 3 * chan :].T.astype(BF16)
        gb = m.gb[...].T
        mrow = m.mrow[...]
        lane = lax.broadcasted_iota(jnp.int32, (1, chan), 1) // HEAD_DIM

        def project(r, carry):
            s = lax.rem(r, 4)
            grp = r // 4
            a = m.a[r]
            kk = jnp.dot(a, m.wk[s], preferred_element_type=F32).astype(BF16)
            qt = (
                lax.dot_general(m.wq[s], a, NT, preferred_element_type=F32)
                * (HEAD_DIM**-0.5 * LOG2E)
            ).astype(BF16)
            vt = lax.dot_general(wvt, a, NT, preferred_element_type=F32) * mrow
            m.gt[r] = jax.nn.sigmoid(lax.dot_general(wgt, a, NT, preferred_element_type=F32) + gb)
            for h in range(HEADS):
                slot = lax.rem(h + s, 4)
                m.km[r, h] = kk * (lane == slot).astype(F32).astype(BF16)
                m.vx[r, h, :HEAD_DIM] = vt[HEAD_DIM * h : HEAD_DIM * (h + 1)].astype(BF16)
                m.vx[r, h, HEAD_DIM:] = jnp.broadcast_to(mrow, (16, res)).astype(BF16)
            for u in range(4):
                hh = lax.rem(u - s + 4, 4)
                m.qs[grp, hh, pl.ds(32 * u, 32)] = qt[32 * u : 32 * (u + 1)]
            return carry

        lax.fori_loop(0, rows, project, 0)

    def turn_bias(b_ref):
        for h in range(HEADS):
            for kb in range(nk):
                sl = slice(KB * kb, KB * (kb + 1))
                m.bt[h, sl] = b_ref[h, :, sl].T

    def head_slice(h):
        return pl.ds(pl.multiple_of(HEAD_DIM * h, HEAD_DIM), HEAD_DIM)

    def fast_heads(joff):
        one = eye()

        def of(k):
            return k // HEADS, lax.rem(k, HEADS)

        def weights_step(k, kb, pp):
            grp, h = of(k)
            sl = slice(KB * kb, KB * (kb + 1))
            rhs = jnp.concatenate([m.bt[h, sl], m.qs[grp, h, :, pl.ds(joff, JB)]], axis=0)
            lhs = jnp.concatenate(
                [jnp.concatenate([one, m.km[grp * 4 + r, h, sl]], axis=1) for r in range(4)], axis=0
            )
            p4 = jnp.exp2(jnp.dot(lhs, rhs, preferred_element_type=F32)).astype(BF16)
            for r in range(4):
                pp[r, sl] = p4[KB * r : KB * (r + 1)]

        def mix_step(k, r, pp):
            grp, h = of(k)
            oe = jnp.dot(m.vx[grp * 4 + r, h], pp[r], preferred_element_type=F32)
            den = oe[HEAD_DIM : HEAD_DIM + 1]
            m.gd[...] = jnp.where((den > 2.0**-60) & (den < 2.0**100), m.gd[...], 0.0)
            m.ot[grp * 4 + r, head_slice(h)] = oe[:HEAD_DIM] / den

        def both(k, new, old):
            for kb in range(nk):
                weights_step(k, kb, new)
                if kb % 2:
                    mix_step(k - 1, kb // 2, old)

        for kb in range(nk):
            weights_step(0, kb, m.pa)

        def pair(i, carry):
            both(2 * i + 1, m.pb, m.pa)
            both(2 * i + 2, m.pa, m.pb)
            return carry

        lax.fori_loop(0, tasks // 2 - 1, pair, 0)
        both(tasks - 1, m.pb, m.pa)
        for r in range(4):
            mix_step(tasks - 1, r, m.pb)

    def safe_heads(joff):
        one = eye()

        def row_head(it, carry):
            row, h = it // HEADS, lax.rem(it, HEADS)
            q = m.qs[row // 4, h, :, pl.ds(joff, JB)]

            def scores(kb, carry):
                ks = pl.ds(pl.multiple_of(kb * KB, KB), KB)
                rhs = jnp.concatenate([m.bt[h, ks], q], axis=0)
                lhs = jnp.concatenate([one, m.km[row, h, ks]], axis=1)
                s1 = jnp.dot(lhs, rhs, preferred_element_type=F32)
                s1 = jnp.where(m.mcol[ks] > 0.5, s1, -1e30)
                m.ss[ks] = s1
                return jnp.maximum(carry, jnp.max(s1, axis=0, keepdims=True))

            top = lax.fori_loop(0, nk, scores, jnp.full((1, JB), -1e30, F32))

            def weights(kb, carry):
                ks = pl.ds(pl.multiple_of(kb * KB, KB), KB)
                m.pa[0, ks] = jnp.exp2(m.ss[ks] - top).astype(BF16)
                return carry

            lax.fori_loop(0, nk, weights, 0)
            oe = jnp.dot(m.vx[row, h], m.pa[0], preferred_element_type=F32)
            m.ot[row, head_slice(h)] = oe[:HEAD_DIM] / oe[HEAD_DIM : HEAD_DIM + 1]
            return carry

        lax.fori_loop(0, rows * HEADS, row_head, 0)

    def finish(joff, store):
        def row(r):
            gated = (m.ot[r] * m.gt[r, :, pl.ds(joff, JB)]).T.astype(BF16)
            z = m.x[r, pl.ds(joff, JB)].astype(F32) + jnp.dot(
                gated, m.ow[...], preferred_element_type=F32
            )
            z = z.astype(BF16)
            if trans:
                zf = z.astype(F32)
                a = layer_norm(z, m.ng[...])
                hid = jnp.dot(a, m.ti[...], preferred_element_type=F32) + m.tb[...]
                hid = jnp.maximum(hid, 0.0).astype(BF16)
                z = (zf + jnp.dot(hid, m.to[...], preferred_element_type=F32)).astype(BF16)
            m.zz[r] = z

        def some(i, carry):
            for r in range(UNROLL):
                row(UNROLL * i + r)
            return carry

        lax.fori_loop(0, rows // UNROLL, some, 0)
        span = JB // rows
        out_row = lax.broadcasted_iota(jnp.int32, (JB, JB), 0)
        in_row = lax.broadcasted_iota(jnp.int32, (JB, JB), 1)
        perm = (in_row == lax.rem(out_row, rows) * span + out_row // rows).astype(F32).astype(BF16)
        for q in range(rows // 2):
            cols = [
                jnp.concatenate([m.zz[r, span * n : span * (n + 1)] for r in range(rows)], axis=0)
                for n in (2 * q, 2 * q + 1)
            ]
            moved = jnp.dot(perm, jnp.concatenate(cols, axis=1), preferred_element_type=F32)
            for n in range(2):
                part = moved[:, chan * n : chan * (n + 1)]
                store(span * (2 * q + n), part.reshape(span, rows, chan).astype(BF16))

    return types.SimpleNamespace(
        project_all=project_all, turn_bias=turn_bias, fast_heads=fast_heads,
        safe_heads=safe_heads, finish=finish,
    )


def stage_names(trans):
    names = ["x", "a", "w", "gb", "ow", "mrow"]
    return names + (["ng", "ti", "tb", "to"] if trans else [])


def stage_scratch(rows, res, chan):
    return {
        "km": pltpu.VMEM((rows, HEADS, res, chan), BF16),
        "qs": pltpu.VMEM((rows // 4, HEADS, chan, res), BF16),
        "vx": pltpu.VMEM((rows, HEADS, HEAD_DIM + 16, res), BF16),
        "gt": pltpu.VMEM((rows, chan, res), F32),
        "bt": pltpu.VMEM((HEADS, res, JB), BF16),
        "pa": pltpu.VMEM((4, res, JB), BF16),
        "pb": pltpu.VMEM((4, res, JB), BF16),
        "ot": pltpu.VMEM((rows, chan, JB), F32),
        "wk": pltpu.VMEM((4, chan, chan), BF16),
        "wq": pltpu.VMEM((4, chan, chan), BF16),
        "gd": pltpu.VMEM((1, JB), F32),
        "zz": pltpu.VMEM((rows, JB, chan), BF16),
        "bs": pltpu.VMEM((HEADS, JB, res), BF16),
        "ss": pltpu.VMEM((res, JB), F32),
    }


def safe_kernel(trans, names, *refs):
    m = types.SimpleNamespace(**dict(zip(names, refs)))
    tools = stage_tools(trans, m)

    @pl.when(pl.program_id(0) == 0)
    def _():
        tools.project_all()

    joff = pl.multiple_of(pl.program_id(0) * JB, JB)
    tools.turn_bias(m.b)
    tools.safe_heads(joff)

    def store(at, part):
        m.o[at : at + part.shape[0]] = part

    tools.finish(joff, store)


def safe_attention(ins, bias, trans):
    rows, res, chan = ins[0].shape
    scratch = stage_scratch(rows, res, chan)
    names = stage_names(trans) + ["mcol", "b", "o"] + list(scratch)
    full = lambda a: pl.BlockSpec(a.shape, lambda j, n=a.ndim: (0,) * n)
    return pl.pallas_call(
        functools.partial(safe_kernel, trans, names),
        grid=(res // JB,),
        out_shape=jax.ShapeDtypeStruct((res, rows, chan), BF16),
        in_specs=[full(a) for a in ins] + [pl.BlockSpec((HEADS, JB, res), lambda j: (0, j, 0))],
        out_specs=pl.BlockSpec((JB, rows, chan), lambda j: (j, 0, 0)),
        scratch_shapes=list(scratch.values()),
        compiler_params=pltpu.CompilerParams(
            dimension_semantics=("arbitrary",), vmem_limit_bytes=60 * 1024 * 1024
        ),
    )(*ins, bias)


def fused_kernel(trans, n, names, *refs):
    m = types.SimpleNamespace(**dict(zip(names, refs)))
    tools = stage_tools(trans, m)
    rows, res, chan = m.x.shape
    nj = res // JB
    per = JB // rows
    gy = n // 16
    gx_me, gy_me = lax.axis_index("gx"), lax.axis_index("gy")
    me = gx_me * gy + gy_me
    at = lambda d: {"gx": d // gy, "gy": lax.rem(d, gy)}
    barrier = pltpu.get_barrier_semaphore()
    cols = [lax.rem(gy_me + b, gy) for b in range(gy)]

    def everyone(act):
        def ring(a, carry):
            for col in cols:
                act({"gx": lax.rem(gx_me + a, n // gy), "gy": col})
            return carry

        for col in cols[1:]:
            act({"gx": gx_me, "gy": col})
        lax.fori_loop(1, n // gy, ring, 0)

    def greet(to):
        pl.semaphore_signal(barrier, inc=1, device_id=to, device_id_type=pl.DeviceIdType.MESH)

    everyone(greet)

    def block_of(t):
        return lax.rem(t + me, nj)

    def fetch(t):
        return pltpu.make_async_copy(
            m.b.at[:, pl.ds(pl.multiple_of(block_of(t) * JB, JB), JB)], m.bs, m.fetch_sem
        )

    mine = pl.ds(pl.multiple_of(rows * me, rows), rows)

    def send_block(t):
        def send(k, carry):
            i = lax.rem(k + me // nj, per)
            to = block_of(t) * per + i
            src = m.zs.at[lax.rem(t, 2), pl.ds(pl.multiple_of(i * rows, rows), rows)]

            @pl.when(to != me)
            def _():
                pltpu.make_async_remote_copy(
                    src_ref=src, dst_ref=m.o.at[:, mine],
                    send_sem=m.send_sem.at[lax.rem(t, 2)], recv_sem=m.recv_sem,
                    device_id=at(to), device_id_type=pl.DeviceIdType.MESH,
                ).start()

            @pl.when(to == me)
            def _():
                pltpu.make_async_copy(src, m.o.at[:, mine], m.own_sem).start()

            return carry

        lax.fori_loop(0, per, send, 0)

    def sent_block(t):
        here = block_of(t) == me // per
        slot = lax.rem(t, 2)

        def sent(count):
            piece = m.zs.at[slot, pl.ds(0, count * rows)]
            pltpu.make_async_copy(piece, piece, m.send_sem.at[slot]).wait()

        @pl.when(here)
        def _():
            sent(per - 1)
            pltpu.make_async_copy(m.zs.at[slot, pl.ds(0, rows)], m.o.at[:, mine], m.own_sem).wait()

        @pl.when(jnp.logical_not(here))
        def _():
            sent(per)

    fetch(0).start()
    tools.project_all()
    m.gd[...] = jnp.ones_like(m.gd)
    pl.semaphore_wait(barrier, n - 1)

    def block(t, carry):
        joff = pl.multiple_of(block_of(t) * JB, JB)
        fetch(t).wait()
        tools.turn_bias(m.bs)

        @pl.when(t > 0)
        def _():
            send_block(t - 1)

        @pl.when(t < nj - 1)
        def _():
            fetch(t + 1).start()

        tools.fast_heads(joff)

        @pl.when(t > 1)
        def _():
            sent_block(t - 2)

        def store(at, part):
            m.zs[lax.rem(t, 2), at : at + part.shape[0]] = part

        tools.finish(joff, store)
        return carry

    lax.fori_loop(0, nj, block, 0)
    good = jnp.min(m.gd[...], axis=1, keepdims=True)
    if trans:
        m.good[...] = jnp.minimum(m.before[...], good)
    else:
        m.good[...] = jnp.broadcast_to(good, m.good.shape)
    send_block(nj - 1)
    if trans:
        def flag(to):
            pltpu.make_async_remote_copy(
                src_ref=m.good.at[pl.ds(0, 1)], dst_ref=m.flags.at[me, pl.ds(0, 1)],
                send_sem=m.fsend, recv_sem=m.frecv,
                device_id=to, device_id_type=pl.DeviceIdType.MESH,
            ).start()

        everyone(flag)
        own_flag = pltpu.make_async_copy(m.good, m.flags.at[me], m.flag_sem)
        own_flag.start()
        own_flag.wait()
    sent_block(nj - 2)
    sent_block(nj - 1)
    others = m.o.at[:, pl.ds(0, rows * (n - 1))]
    pltpu.make_async_copy(others, others, m.recv_sem).wait()
    if trans:
        others = m.flags.at[pl.ds(0, n - 1), pl.ds(0, 1)]
        pltpu.make_async_copy(others, others, m.fsend).wait()
        pltpu.make_async_copy(others, others, m.frecv).wait()


def fused_attention(cid, n, ins, bias, before):
    trans = before is not None
    rows, res, chan = ins[0].shape
    scratch = stage_scratch(rows, res, chan)
    del scratch["ss"]
    scratch |= {
        "zs": pltpu.VMEM((2, JB, rows, chan), BF16),
        "send_sem": pltpu.SemaphoreType.DMA((2,)),
        "recv_sem": pltpu.SemaphoreType.DMA,
        "fetch_sem": pltpu.SemaphoreType.DMA,
        "own_sem": pltpu.SemaphoreType.DMA,
    }
    anywhere = pl.BlockSpec(memory_space=pl.ANY)
    outs = {"o": jax.ShapeDtypeStruct((rows, res, chan), BF16)}
    out_specs = [anywhere]
    names = stage_names(trans) + ["b"]
    args = list(ins) + [bias]
    in_specs = [VMEM] * len(ins) + [anywhere]
    if trans:
        names.append("before")
        args.append(before)
        in_specs.append(VMEM)
        outs["flags"] = jax.ShapeDtypeStruct((n, 8, 128), F32)
        out_specs.append(anywhere)
        scratch |= {
            "good": pltpu.VMEM((8, 128), F32),
            "fsend": pltpu.SemaphoreType.DMA,
            "frecv": pltpu.SemaphoreType.DMA,
            "flag_sem": pltpu.SemaphoreType.DMA,
        }
    else:
        outs["good"] = jax.ShapeDtypeStruct((8, 128), F32)
        out_specs.append(VMEM)
    return pl.pallas_call(
        functools.partial(fused_kernel, trans, n, names + list(outs) + list(scratch)),
        out_shape=list(outs.values()),
        in_specs=in_specs,
        out_specs=out_specs,
        scratch_shapes=list(scratch.values()),
        compiler_params=pltpu.CompilerParams(
            collective_id=cid, has_side_effects=True, vmem_limit_bytes=60 * 1024 * 1024
        ),
    )(*args)


def exchange_kernel(n, whole, z_ref, o_ref, send_sem, recv_sem, own_sem):
    rows = z_ref.shape[1]
    cut = lambda d: z_ref if whole else z_ref.at[pl.ds(pl.multiple_of(rows * d, rows), rows)]
    gy = n // 16
    me = lax.axis_index("gx") * gy + lax.axis_index("gy")
    at = lambda d: {"gx": d // gy, "gy": lax.rem(d, gy)}
    barrier = pltpu.get_barrier_semaphore()

    def greet(t, carry):
        pl.semaphore_signal(
            barrier, inc=1, device_id=at(lax.rem(me + t, n)), device_id_type=pl.DeviceIdType.MESH
        )
        return carry

    lax.fori_loop(1, n, greet, 0)
    mine = pl.ds(pl.multiple_of(rows * me, rows), rows)
    own = pltpu.make_async_copy(cut(me), o_ref.at[:, mine], own_sem)
    own.start()
    pl.semaphore_wait(barrier, n - 1)

    def copy(t, to, frm):
        return pltpu.make_async_remote_copy(
            src_ref=cut(to),
            dst_ref=o_ref.at[:, pl.ds(pl.multiple_of(rows * frm, rows), rows)],
            send_sem=send_sem.at[t], recv_sem=recv_sem.at[t],
            device_id=at(to), device_id_type=pl.DeviceIdType.MESH,
        )

    def send(t, carry):
        copy(t, lax.rem(me + t, n), me).start()
        return carry

    lax.fori_loop(1, n, send, 0)
    own.wait()

    def land(t, carry):
        copy(t, lax.rem(me + t, n), lax.rem(me + n - t, n)).wait_recv()
        copy(t, lax.rem(me + t, n), me).wait_send()
        return carry

    lax.fori_loop(1, n, land, 0)


def exchange(cid, n, z, whole=False):
    lead, rows, width = z.shape
    shape = (lead, n * rows, width) if whole else (rows, lead, width)
    return pl.pallas_call(
        functools.partial(exchange_kernel, n, whole),
        out_shape=jax.ShapeDtypeStruct(shape, BF16),
        in_specs=[pl.BlockSpec(memory_space=pl.ANY)],
        out_specs=pl.BlockSpec(memory_space=pl.ANY),
        scratch_shapes=[
            pltpu.SemaphoreType.DMA((n,)),
            pltpu.SemaphoreType.DMA((n,)),
            pltpu.SemaphoreType.DMA,
        ],
        compiler_params=pltpu.CompilerParams(collective_id=cid, has_side_effects=True),
    )(z)


def local(
    pair_in,
    residue_mask,
    norm_start,
    proj_start,
    gate_bias_start,
    bias_w_start,
    out_w_start,
    norm_end,
    proj_end,
    gate_bias_end,
    bias_w_end,
    out_w_end,
    norm_trans,
    trans_in,
    trans_bias,
    trans_out,
):
    rows, res, chan = pair_in.shape
    n = lax.axis_size(("gx", "gy"))
    row = lambda v: v.reshape(1, -1)
    mine = jnp.pad(residue_mask.astype(F32).reshape(1, rows), ((0, 7), (0, 128 - rows)))
    bias_w = jnp.concatenate([bias_w_start, bias_w_end], axis=1)
    bias_w = jnp.pad(bias_w, ((0, 0), (0, 128 - 2 * HEADS)))
    bias, normed = pair_bias(pair_in, row(norm_start), bias_w, 0)
    bias, mask = gather(0, bias, mine)
    mask = mask[:, 0, :rows].reshape(res)
    mask = jnp.where(jnp.max(mask) > 0.5, mask, 1.0)
    mrow = mask.reshape(1, res)
    start = [pair_in, normed, proj_start, row(gate_bias_start), out_w_start, mrow]
    ends = [proj_end, row(gate_bias_end), out_w_end, mrow]
    ends += [row(norm_trans), trans_in, row(trans_bias), trans_out]

    def end_inputs(cols):
        bias, normed = pair_bias(cols, row(norm_end), bias_w, HEADS)
        return [cols, normed] + ends, bias

    def safe(bias):
        mcol = [mask.reshape(res, 1)]
        cols = exchange(4, n, safe_attention(start + mcol, bias, False))
        ins, bias = end_inputs(cols)
        return exchange(5, n, safe_attention(ins + mcol, exchange(6, n, bias, True), True))

    cols, good = fused_attention(2, n, start, bias, None)
    ins, end_bias = end_inputs(cols)
    out, flags = fused_attention(3, n, ins, gather(1, end_bias), good)
    return lax.cond(jnp.min(flags[:, 0]) > 0.5, lambda b: out, safe, bias)


def solution(mesh):
    spec = P(("gx", "gy"), None, None)
    placed = (spec, P(("gx", "gy"))) + (P(),) * 14
    return jax.shard_map(local, mesh=mesh, in_specs=placed, out_specs=spec, check_vma=False)
```
